32 devices in a mesh: fsdp: 8 (over z, y), seq: 4 (over x, core).
Axes of the slice: x: 2, y: 2, z: 4, core: 2. Of those that a mesh axis runs over, the one named last changes fastest.
Arguments:
- tokens: bfloat16 [8, 1024, 768], P('fsdp', 'seq'), may hold values from -6 to 6
- condition: bfloat16 [8, 768], P('fsdp'), may hold values from -6 to 6
- ada_weight: bfloat16 [2, 768, 4608], P(None, 'fsdp'), may hold values from -0.21875 to 0.21875
- ada_bias: bfloat16 [2, 4608], P(None, 'fsdp'), may hold values from -3 to 3
- qkv_weight: bfloat16 [2, 768, 2304], P(None, 'fsdp'), may hold values from -0.21875 to 0.21875
- qv_bias: bfloat16 [2, 1536], P(None, 'fsdp'), may hold values from -3 to 3
- out_weight: bfloat16 [2, 768, 768], P(None, 'fsdp'), may hold values from -1.25 to 1.25
- out_bias: bfloat16 [2, 768], P(None, 'fsdp'), may hold values from -3 to 3
- up_weight: bfloat16 [2, 768, 3072], P(None, 'fsdp'), may hold values from -0.21875 to 0.21875
- up_bias: bfloat16 [2, 3072], P(None, 'fsdp'), may hold values from -3 to 3
- down_weight: bfloat16 [2, 3072, 768], P(None, 'fsdp'), may hold values from -0.109375 to 0.109375
- down_bias: bfloat16 [2, 768], P(None, 'fsdp'), may hold values from -3 to 3
- cotangent: bfloat16 [8, 1024, 768], P('fsdp', 'seq'), may hold values from -6 to 6
Outputs:
- block_out: bfloat16 [8, 1024, 768], P('fsdp', 'seq')
- grad_tokens: float32 [8, 1024, 768], P('fsdp', 'seq')
- grad_condition: float32 [8, 768], P('fsdp')
- grad_ada_weight: float32 [2, 768, 4608], P(None, 'fsdp')
- grad_ada_bias: float32 [2, 4608], P(None, 'fsdp')
- grad_qkv_weight: float32 [2, 768, 2304], P(None, 'fsdp')
- grad_qv_bias: float32 [2, 1536], P(None, 'fsdp')
- grad_out_weight: float32 [2, 768, 768], P(None, 'fsdp')
- grad_out_bias: float32 [2, 768], P(None, 'fsdp')
- grad_up_weight: float32 [2, 768, 3072], P(None, 'fsdp')
- grad_up_bias: float32 [2, 3072], P(None, 'fsdp')
- grad_down_weight: float32 [2, 3072, 768], P(None, 'fsdp')
- grad_down_bias: float32 [2, 768], P(None, 'fsdp')
The draws below stay inside these ranges and needn't reach their ends.
All inputs are finite; a program needn't handle non-finite values.
Results may differ from the reference program's by a relative error of at most 0.017.
The reference program's roundings to bfloat16 on the way count: a program that leaves them out, or rounds other values in their place, can miss the bound.
Values may be sent and summed in bfloat16 or wider, within the bound.
A program may use at most 256 MiB of HBM per device.

```python
import jax
import jax.numpy as jnp
from jax import lax

D = 768
HEADS = 12
HEAD_DIM = 64
FF = 3072
SEQ_LEN = 1024
LAYERS = 2
LAT_DEV = 1
LATENTS = 8


def level_of(own_key, extent, cuts, smallest, largest):
    gain = 1.0
    for axis_at, shards_of in cuts:
        heights = jax.random.uniform(jax.random.fold_in(jax.random.fold_in(own_key, 6), axis_at), (shards_of,), jnp.float32, smallest / len(cuts), largest / len(cuts))
        gain = gain * jnp.repeat(jnp.exp(heights), extent[axis_at] // shards_of).reshape((-1,) + (1,) * (len(extent) - 1 - axis_at))
    return gain


def normal_values(key, dims, scale, reach, shards=(), held_as=jnp.bfloat16):
    values = scale * jax.random.normal(key, dims, jnp.float32)
    if shards:
        values = values * level_of(key, dims, shards, -0.22, 0.18)
    return jnp.clip(values, -reach, reach).astype(held_as)


def setup_inputs(seed: int = 0) -> dict:
    key_list = jax.random.split(jax.random.key(seed), 14)
    tokens = normal_values(key_list[0], (LATENTS, SEQ_LEN, D), 1.0, 6.0, ((0, 8), (1, 4)))
    condition = normal_values(key_list[1], (LATENTS, D), 1.0, 6.0, ((0, 8),))
    ada_weight = normal_values(key_list[2], (LAYERS, D, 6 * D), D ** -0.5, 0.21875, ((1, 8),))
    ada_bias = normal_values(key_list[3], (LAYERS, 6 * D), 0.5, 3.0, ((1, 8),))
    qkv_weight = normal_values(key_list[4], (LAYERS, D, 3 * D), D ** -0.5, 0.21875, ((1, 8),))
    qv_bias = normal_values(key_list[5], (LAYERS, 2 * D), 0.5, 3.0, ((1, 8),))
    out_weight = normal_values(key_list[6], (LAYERS, D, D), (D // 32) ** -0.5, 1.25, ((1, 8),))
    out_bias = normal_values(key_list[7], (LAYERS, D), 0.5, 3.0, ((1, 8),))
    up_weight = normal_values(key_list[8], (LAYERS, D, FF), D ** -0.5, 0.21875, ((1, 8),))
    up_bias = normal_values(key_list[9], (LAYERS, FF), 0.5, 3.0, ((1, 8),))
    down_weight = normal_values(key_list[10], (LAYERS, FF, D), FF ** -0.5, 0.109375, ((1, 8),))
    down_bias = normal_values(key_list[11], (LAYERS, D), 0.5, 3.0, ((1, 8),))
    cotangent = normal_values(key_list[12], (LATENTS, SEQ_LEN, D), 1.0, 6.0, ((0, 8), (1, 4)))
    return {"tokens": tokens, "condition": condition, "ada_weight": ada_weight, "ada_bias": ada_bias, "qkv_weight": qkv_weight, "qv_bias": qv_bias, "out_weight": out_weight, "out_bias": out_bias, "up_weight": up_weight, "up_bias": up_bias, "down_weight": down_weight, "down_bias": down_bias, "cotangent": cotangent}


@jax.custom_vjp
def low(v):
    return lax.optimization_barrier(v.astype(jnp.bfloat16)).astype(jnp.float32)

@jax.custom_vjp
def low_back(v):
    return v

def low_keep(v):
    return (low(v), None)

def low_pass(kept, grad):
    return (grad,)

def back_keep(v):
    return (v, None)

def back_low(kept, grad):
    return (low(grad),)
low.defvjp(low_keep, low_pass)
low_back.defvjp(back_keep, back_low)
highest = lax.Precision.HIGHEST
epsilon = 1e-06

def normalize(values):
    centred = values - lax.optimization_barrier(jnp.mean(values, axis=-1, keepdims=True))
    spread = lax.optimization_barrier(jnp.mean(centred * centred, axis=-1, keepdims=True))
    return centred * lax.rsqrt(spread + epsilon)

def project(values, matrix, offset):
    return jnp.einsum('lsd,dn->lsn', values, matrix, precision=highest) + offset

def attend_latent(operands):
    queries, key_rows, value_rows = operands
    queries = queries.reshape(SEQ_LEN, HEADS, HEAD_DIM)
    key_rows = key_rows.reshape(SEQ_LEN, HEADS, HEAD_DIM)
    value_rows = value_rows.reshape(SEQ_LEN, HEADS, HEAD_DIM)
    scores = low_back(jnp.einsum('qhd,khd->hqk', queries, key_rows, precision=highest) * HEAD_DIM ** (-0.5))
    logsum = jnp.log(lax.optimization_barrier(jnp.sum(jnp.exp(scores), axis=-1, keepdims=True)))
    probability = low(jnp.exp(scores - logsum))
    output = jnp.einsum('hqk,khd->qhd', probability, value_rows, precision=highest)
    return low(low_back(output.reshape(SEQ_LEN, D)))

def block_layer(hidden, scaled, weights):
    ada_matrix, ada_offset, qkv_matrix, qv_offset, out_matrix, out_offset, up_matrix, up_offset, down_matrix, down_offset = weights
    modulation = jnp.dot(scaled, ada_matrix, precision=highest) + ada_offset
    pieces = [portion[:, None, :] for portion in jnp.split(modulation, 6, axis=-1)]
    shift_attn, scale_attn, gate_attn, shift_mlp, scale_mlp, gate_mlp = pieces
    attn_in = low(normalize(hidden) * (1.0 + scale_attn) + shift_attn)
    qkv_offset = jnp.concatenate([qv_offset[:D], jnp.zeros((D,), jnp.float32), qv_offset[D:]])
    projected = low(low_back(project(attn_in, qkv_matrix, qkv_offset)))
    queries, key_rows, value_rows = jnp.split(projected, 3, axis=-1)
    attended = lax.map(jax.checkpoint(attend_latent), (queries, key_rows, value_rows))
    branch = low_back(project(attended, out_matrix, out_offset))
    middle = hidden + gate_attn * branch
    mlp_in = low(normalize(middle) * (1.0 + scale_mlp) + shift_mlp)
    upward = low_back(project(mlp_in, up_matrix, up_offset))
    activated = low(jax.nn.gelu(upward, approximate=True))
    feed_out = low_back(project(activated, down_matrix, down_offset))
    return middle + gate_mlp * feed_out

def reference(tokens, condition, ada_weight, ada_bias, qkv_weight, qv_bias, out_weight, out_bias, up_weight, up_bias, down_weight, down_bias, cotangent):
    params = tuple((member.astype(jnp.float32) for member in (ada_weight, ada_bias, qkv_weight, qv_bias, out_weight, out_bias, up_weight, up_bias, down_weight, down_bias)))
    groups = LATENTS // LAT_DEV
    token_groups = tokens.astype(jnp.float32).reshape(groups, LAT_DEV, SEQ_LEN, D)
    cond_groups = condition.astype(jnp.float32).reshape(groups, LAT_DEV, D)
    grad_groups = cotangent.astype(jnp.float32).reshape(groups, LAT_DEV, SEQ_LEN, D)

    def forward(hidden, cond_rows, weights):
        scaled = low(jax.nn.silu(cond_rows))
        for layer_index in range(LAYERS):
            hidden = block_layer(hidden, scaled, tuple((member[layer_index] for member in weights)))
        return hidden

    def group_step(totals, operands):
        hidden, cond_rows, gradient = operands
        result, backward = jax.vjp(forward, hidden, cond_rows, params)
        grad_hidden, grad_cond, grad_params = backward(gradient)
        summed = tuple((running + addend for running, addend in zip(totals, grad_params)))
        return (summed, (result.astype(jnp.bfloat16), grad_hidden, grad_cond))
    starting = tuple((jnp.zeros_like(member) for member in params))
    totals, (outputs, grad_hidden, grad_cond) = lax.scan(group_step, starting, (token_groups, cond_groups, grad_groups))
    return (outputs.reshape(LATENTS, SEQ_LEN, D), grad_hidden.reshape(LATENTS, SEQ_LEN, D), grad_cond.reshape(LATENTS, D), totals[0], totals[1], totals[2], totals[3], totals[4], totals[5], totals[6], totals[7], totals[8], totals[9])
```

```python
import jax
import jax.numpy as jnp
from jax import lax
from jax.sharding import PartitionSpec as P

HEAD_DIM = 64
SCORE_SCALE = HEAD_DIM ** (-0.5)
EPSILON = 1e-06
HIGHEST = lax.Precision.HIGHEST
F32 = jnp.float32
BF16 = jnp.bfloat16


def normalize(values):
    centred = values - jnp.mean(values, axis=-1, keepdims=True)
    inverse = lax.rsqrt(jnp.mean(centred * centred, axis=-1, keepdims=True) + EPSILON)
    return centred * inverse, inverse


def norm_back(gradient, normed, inverse):
    return inverse * (
        gradient
        - jnp.mean(gradient, axis=-1, keepdims=True)
        - normed * jnp.mean(gradient * normed, axis=-1, keepdims=True)
    )


def mm(a, b):
    return lax.dot_general(a, b, (((1,), (0,)), ((), ())), preferred_element_type=F32)


def mm_nt(a, b):
    return lax.dot_general(a, b, (((1,), (1,)), ((), ())), preferred_element_type=F32)


def mm_tn(a, b):
    return lax.dot_general(a, b, (((0,), (0,)), ((), ())), preferred_element_type=F32)


def split_heads(rows):
    return rows.reshape(rows.shape[0], -1, HEAD_DIM).transpose(1, 0, 2)


def join_heads(heads):
    return heads.transpose(1, 0, 2).reshape(heads.shape[1], -1)


def attend(q, k, v):
    q, k, v = split_heads(q), split_heads(k), split_heads(v)
    scores = jnp.einsum("hqd,hkd->hqk", q, k, preferred_element_type=F32) * SCORE_SCALE
    logsum = jnp.log(jnp.sum(jnp.exp(scores), axis=-1, keepdims=True))
    prob = jnp.exp(scores - logsum).astype(BF16)
    out = jnp.einsum("hqk,hkd->hqd", prob, v, preferred_element_type=F32)
    return join_heads(out).astype(BF16), logsum


def attend_back(q, k, v, logsum, out_grad):
    q, k, v, out_grad = split_heads(q), split_heads(k), split_heads(v), split_heads(out_grad)
    scores = jnp.einsum("hqd,hkd->hqk", q, k, preferred_element_type=F32) * SCORE_SCALE
    prob = jnp.exp(scores - logsum)
    dv = jnp.einsum("hqk,hqd->hkd", prob.astype(BF16), out_grad, preferred_element_type=F32)
    dp = jnp.einsum("hqd,hkd->hqk", out_grad, v, preferred_element_type=F32)
    inner = jnp.sum(prob * dp, axis=-1, keepdims=True)
    ds = (prob * (dp - inner)).astype(BF16)
    dq = jnp.einsum("hqk,hkd->hqd", ds, k, preferred_element_type=F32) * SCORE_SCALE
    dk = jnp.einsum("hqk,hqd->hkd", ds, q, preferred_element_type=F32) * SCORE_SCALE
    return [join_heads(t).astype(BF16) for t in (dq, dk, dv)]


def gelu_parts(u):
    c = 0.7978845608028654
    inner = c * (u + 0.044715 * (u * u * u))
    t = jnp.tanh(inner)
    value = 0.5 * u * (1.0 + t)
    slope = 0.5 * (1.0 + t) + 0.5 * u * (1.0 - t * t) * (c * (1.0 + 3.0 * 0.044715 * u * u))
    return value, slope


def per_device(
    tokens, condition, ada_weight, ada_bias, qkv_weight, qv_bias, out_weight, out_bias,
    up_weight, up_bias, down_weight, down_bias, cotangent,
):
    n = lax.axis_size("fsdp")
    ns = lax.axis_size("seq")
    f = lax.axis_index("fsdp")
    s = lax.axis_index("seq")
    layers, rows, width6 = ada_weight.shape
    width = rows * n
    ff = up_weight.shape[2]
    hc = width // ns
    fc = ff // (ns * n)

    def take(x, axis):
        return lax.dynamic_index_in_dim(x, s, axis, keepdims=False)

    def own(x, axis, size):
        return lax.dynamic_slice_in_dim(x, f * size, size, axis)

    w_qkv, w_rest = [], []
    for l in range(layers):
        q_part = take(qkv_weight[l].reshape(rows, 3, ns, hc), 2).reshape(rows, 3 * hc)
        u_part = take(up_weight[l].reshape(rows, n, ns, fc), 2).reshape(rows, n * fc)
        d_part = take(down_weight[l].reshape(ns, fc, width), 0)
        w_qkv.append(lax.all_gather(q_part, "fsdp", axis=0, tiled=True))
        rest = jnp.concatenate([u_part, d_part, out_weight[l]], axis=1)
        w_rest.append(lax.all_gather(rest, "fsdp", axis=0, tiled=True))
    fw = n * fc

    cond_float = condition.astype(F32)
    cond_act = jax.nn.silu(cond_float).astype(BF16)
    small = jnp.concatenate(
        [ada_bias.reshape(-1), qv_bias.reshape(-1), out_bias.reshape(-1), up_bias.reshape(-1),
         down_bias.reshape(-1), cond_act.reshape(-1)]
    )
    small = lax.all_gather(small, "fsdp", axis=0, tiled=False)
    pos = 0

    def unpack(per_layer):
        nonlocal pos
        part = small[:, pos: pos + layers * per_layer].reshape(n, layers, per_layer)
        pos += layers * per_layer
        return part.transpose(1, 0, 2).reshape(layers, n * per_layer)

    ada_b = unpack(ada_bias.shape[1]).astype(F32)
    qv_b = unpack(qv_bias.shape[1]).astype(F32)
    out_b = unpack(out_bias.shape[1]).astype(F32)
    up_b = unpack(up_bias.shape[1]).astype(F32)
    down_b = unpack(down_bias.shape[1]).astype(F32)
    cond_all = small[:, pos:]
    cond_rows = own(cond_all, 1, rows)
    q_b = take(qv_b[:, :width].reshape(layers, ns, hc), 1)
    v_b = take(qv_b[:, width:].reshape(layers, ns, hc), 1)
    qkv_b = jnp.concatenate([q_b, jnp.zeros_like(q_b), v_b], axis=1)
    up_bs = take(up_b.reshape(layers, n, ns, fc), 2).reshape(layers, fw)

    mod_partial = jnp.stack([mm(cond_rows, ada_weight[l]) for l in range(layers)], axis=1)
    mod = lax.psum_scatter(mod_partial, "fsdp", scatter_dimension=0, tiled=True)[0] + ada_b

    hidden = tokens[0].astype(F32)
    saved = []
    for l in range(layers):
        shift_a, scale_a, gate_a, shift_m, scale_m, gate_m = jnp.split(mod[l], 6)
        n_a, r_a = normalize(hidden)
        attn_in = (n_a * (1.0 + scale_a) + shift_a).astype(BF16)
        attn_all = lax.all_gather(attn_in, "seq", axis=0, tiled=True)
        qkv = (mm(attn_all, w_qkv[l]) + qkv_b[l]).astype(BF16)
        q, k, v = qkv[:, :hc], qkv[:, hc: 2 * hc], qkv[:, 2 * hc:]
        head_out, logsum = attend(q, k, v)
        tok_out = lax.all_to_all(head_out, "seq", split_axis=0, concat_axis=1, tiled=True)
        branch = mm(tok_out, w_rest[l][:, fw + width:]) + out_b[l]
        middle = hidden + gate_a * branch
        n_m, r_m = normalize(middle)
        mlp_in = (n_m * (1.0 + scale_m) + shift_m).astype(BF16)
        mlp_all = lax.all_gather(mlp_in, "seq", axis=0, tiled=True)
        up = mm(mlp_all, w_rest[l][:, :fw]) + up_bs[l]
        act = gelu_parts(up)[0].astype(BF16)
        feed = mm(act, w_rest[l][:, fw: fw + width])
        feed = lax.psum_scatter(feed, "seq", scatter_dimension=0, tiled=True) + down_b[l]
        saved.append((n_a, r_a, attn_all, q, k, v, logsum, tok_out, branch, n_m, r_m, mlp_all, up, act, feed))
        hidden = middle + gate_m * feed
    block_out = hidden.astype(BF16)

    g = cotangent[0].astype(F32)
    d_mods = [None] * layers
    reduced = [None] * layers
    bias_grads = [None] * layers
    for l in reversed(range(layers)):
        shift_a, scale_a, gate_a, shift_m, scale_m, gate_m = jnp.split(mod[l], 6)
        n_a, r_a, attn_all, q, k, v, logsum, tok_out, branch, n_m, r_m, mlp_all, up, act, feed = saved[l]
        g_feed = (gate_m * g).astype(BF16)
        d_gate_m = jnp.sum(g * feed, axis=0)
        g_feed_all = lax.all_gather(g_feed, "seq", axis=0, tiled=True)
        grad_down = mm_tn(act, g_feed_all)
        g_up = (mm_nt(g_feed_all, w_rest[l][:, fw: fw + width]) * gelu_parts(up)[1]).astype(BF16)
        grad_up = mm_tn(mlp_all, g_up)
        g_min = lax.psum_scatter(mm_nt(g_up, w_rest[l][:, :fw]), "seq", scatter_dimension=0, tiled=True)
        d_scale_m = jnp.sum(g_min * n_m, axis=0)
        d_shift_m = jnp.sum(g_min, axis=0)
        g_mid = g + norm_back(g_min * (1.0 + scale_m), n_m, r_m)
        g_branch = (gate_a * g_mid).astype(BF16)
        d_gate_a = jnp.sum(g_mid * branch, axis=0)
        grad_out = mm_tn(tok_out, g_branch)
        g_o = mm_nt(g_branch, w_rest[l][:, fw + width:]).astype(BF16)
        g_o_heads = lax.all_to_all(g_o, "seq", split_axis=1, concat_axis=0, tiled=True)
        dq, dk, dv = attend_back(q, k, v, logsum, g_o_heads)
        g_qkv = jnp.concatenate([dq, dk, dv], axis=1)
        grad_qkv = mm_tn(attn_all, g_qkv)
        g_ain = lax.psum_scatter(mm_nt(g_qkv, w_qkv[l]), "seq", scatter_dimension=0, tiled=True)
        d_scale_a = jnp.sum(g_ain * n_a, axis=0)
        d_shift_a = jnp.sum(g_ain, axis=0)
        g = g_mid + norm_back(g_ain * (1.0 + scale_a), n_a, r_a)
        d_mods[l] = jnp.concatenate([d_shift_a, d_scale_a, d_gate_a, d_shift_m, d_scale_m, d_gate_m])
        packed = jnp.concatenate([grad_up, grad_down, grad_out, grad_qkv], axis=1).astype(BF16)
        reduced[l] = lax.psum_scatter(packed, "fsdp", scatter_dimension=0, tiled=True)

        def place(x, axis):
            zeros = jnp.zeros(x.shape[:axis] + (ns,) + x.shape[axis + 1:], F32)
            return lax.dynamic_update_slice_in_dim(zeros, x, s, axis)

        qv_g = place(jnp.stack([jnp.sum(dq.astype(F32), axis=0), jnp.sum(dv.astype(F32), axis=0)])[:, None, :], 1)
        up_g = place(jnp.sum(g_up.astype(F32), axis=0).reshape(n, 1, fc), 1)
        bias_grads[l] = jnp.concatenate([
            qv_g.reshape(n, -1), jnp.sum(g_branch.astype(F32), axis=0).reshape(n, -1),
            up_g.reshape(n, -1), jnp.sum(g_feed.astype(F32), axis=0).reshape(n, -1)], axis=1)

    red = jnp.stack(reduced)
    shared = jnp.concatenate([red[:, :, : fw + width], red[:, :, fw + 2 * width:]], axis=2)
    shared = lax.all_gather(shared, "seq", axis=0, tiled=False).astype(F32)
    grad_up = shared[..., :fw].reshape(ns, layers, rows, n, fc).transpose(1, 2, 3, 0, 4).reshape(layers, rows, ff)
    grad_down = shared[..., fw: fw + width].transpose(1, 0, 2, 3).reshape(layers, ns * fc, width)
    grad_qkv = shared[..., fw + width:].reshape(ns, layers, rows, 3, hc).transpose(1, 2, 3, 0, 4)
    grad_qkv = grad_qkv.reshape(layers, rows, 3 * width)
    grad_out = lax.psum(red[:, :, fw + width: fw + 2 * width], "seq").astype(F32)

    bias = lax.psum(jnp.stack(bias_grads), ("fsdp", "seq"))
    bias = lax.dynamic_index_in_dim(bias, f, 1, keepdims=False)
    cuts = [qv_bias.shape[1], out_bias.shape[1], up_bias.shape[1], down_bias.shape[1]]
    grad_bias, at = [], 0
    for size in cuts:
        grad_bias.append(bias[:, at: at + size])
        at += size

    d_mod = lax.psum(jnp.stack(d_mods), "seq")
    d_mod_all = lax.all_gather(d_mod, "fsdp", axis=0, tiled=False)
    cond_rows32 = cond_rows.astype(F32)
    grad_ada = jnp.stack([
        lax.dot_general(cond_rows32, d_mod_all[:, l], (((0,), (0,)), ((), ())), precision=HIGHEST,
                        preferred_element_type=F32) for l in range(layers)])
    grad_ada_bias = own(jnp.sum(d_mod_all, axis=0), 1, width6 // n)
    g_cond = sum(
        lax.dot_general(d_mod_all[:, l], ada_weight[l].astype(F32), (((1,), (1,)), ((), ())),
                        precision=HIGHEST, preferred_element_type=F32) for l in range(layers))
    g_cond = lax.all_to_all(g_cond, "fsdp", split_axis=0, concat_axis=1, tiled=True)
    _, silu_back = jax.vjp(jax.nn.silu, cond_float)
    grad_condition = silu_back(g_cond)[0]
    return (
        block_out[None], g[None], grad_condition, grad_ada, grad_ada_bias, grad_qkv, grad_bias[0],
        grad_out, grad_bias[1], grad_up, grad_bias[2], grad_down, grad_bias[3],
    )


def solution(mesh):
    token = P("fsdp", "seq", None)
    matrix = P(None, "fsdp", None)
    vector = P(None, "fsdp")
    return jax.shard_map(
        per_device,
        mesh=mesh,
        in_specs=(token, P("fsdp", None)) + (matrix, vector) * 5 + (token,),
        out_specs=(token, token, P("fsdp", None)) + (matrix, vector) * 5,
        check_vma=False,
    )
```

```python
import functools

import jax
import jax.numpy as jnp
from jax import lax
from jax.experimental import pallas as pl
from jax.experimental.pallas import tpu as pltpu
from jax.sharding import PartitionSpec as P

HEAD_DIM = 64
SCORE_SCALE = HEAD_DIM ** (-0.5)
EPSILON = 1e-06
HIGHEST = lax.Precision.HIGHEST
F32 = jnp.float32
BF16 = jnp.bfloat16


def normalize(values):
    centred = values - jnp.mean(values, axis=-1, keepdims=True)
    inverse = lax.rsqrt(jnp.mean(centred * centred, axis=-1, keepdims=True) + EPSILON)
    return centred * inverse, inverse


def norm_back(gradient, normed, inverse):
    return inverse * (
        gradient
        - jnp.mean(gradient, axis=-1, keepdims=True)
        - normed * jnp.mean(gradient * normed, axis=-1, keepdims=True)
    )


def mm(a, b):
    return lax.dot_general(a, b, (((1,), (0,)), ((), ())), preferred_element_type=F32)


def mm_nt(a, b):
    return lax.dot_general(a, b, (((1,), (1,)), ((), ())), preferred_element_type=F32)


def mm_tn(a, b):
    return lax.dot_general(a, b, (((0,), (0,)), ((), ())), preferred_element_type=F32)


def split_heads(rows):
    return rows.reshape(rows.shape[0], -1, HEAD_DIM).transpose(1, 0, 2)


def join_heads(heads):
    return heads.transpose(1, 0, 2).reshape(heads.shape[1], -1)


def attend(q, k, v):
    q, k, v = split_heads(q), split_heads(k), split_heads(v)
    scores = jnp.einsum("hqd,hkd->hqk", q, k, preferred_element_type=F32) * SCORE_SCALE
    logsum = jnp.log(jnp.sum(jnp.exp(scores), axis=-1, keepdims=True))
    prob = jnp.exp(scores - logsum).astype(BF16)
    out = jnp.einsum("hqk,hkd->hqd", prob, v, preferred_element_type=F32)
    return join_heads(out).astype(BF16), logsum


def attend_back(q, k, v, logsum, out_grad):
    q, k, v, out_grad = split_heads(q), split_heads(k), split_heads(v), split_heads(out_grad)
    scores = jnp.einsum("hqd,hkd->hqk", q, k, preferred_element_type=F32) * SCORE_SCALE
    prob = jnp.exp(scores - logsum)
    dv = jnp.einsum("hqk,hqd->hkd", prob.astype(BF16), out_grad, preferred_element_type=F32)
    dp = jnp.einsum("hqd,hkd->hqk", out_grad, v, preferred_element_type=F32)
    inner = jnp.sum(prob * dp, axis=-1, keepdims=True)
    ds = (prob * (dp - inner)).astype(BF16)
    dq = jnp.einsum("hqk,hkd->hqd", ds, k, preferred_element_type=F32) * SCORE_SCALE
    dk = jnp.einsum("hqk,hqd->hkd", ds, q, preferred_element_type=F32) * SCORE_SCALE
    return [join_heads(t).astype(BF16) for t in (dq, dk, dv)]


def gelu_parts(u):
    c = 0.7978845608028654
    inner = c * (u + 0.044715 * (u * u * u))
    t = jnp.tanh(inner)
    value = 0.5 * u * (1.0 + t)
    slope = 0.5 * (1.0 + t) + 0.5 * u * (1.0 - t * t) * (c * (1.0 + 3.0 * 0.044715 * u * u))
    return value, slope


def plain_device(
    tokens, condition, ada_weight, ada_bias, qkv_weight, qv_bias, out_weight, out_bias,
    up_weight, up_bias, down_weight, down_bias, cotangent,
):
    n = lax.axis_size("fsdp")
    ns = lax.axis_size("seq")
    f = lax.axis_index("fsdp")
    s = lax.axis_index("seq")
    layers, rows, width6 = ada_weight.shape
    width = rows * n
    ff = up_weight.shape[2]
    hc = width // ns
    fc = ff // (ns * n)

    def take(x, axis):
        return lax.dynamic_index_in_dim(x, s, axis, keepdims=False)

    def own(x, axis, size):
        return lax.dynamic_slice_in_dim(x, f * size, size, axis)

    w_qkv, w_rest = [], []
    for l in range(layers):
        q_part = take(qkv_weight[l].reshape(rows, 3, ns, hc), 2).reshape(rows, 3 * hc)
        u_part = take(up_weight[l].reshape(rows, n, ns, fc), 2).reshape(rows, n * fc)
        d_part = take(down_weight[l].reshape(ns, fc, width), 0)
        w_qkv.append(lax.all_gather(q_part, "fsdp", axis=0, tiled=True))
        rest = jnp.concatenate([u_part, d_part, out_weight[l]], axis=1)
        w_rest.append(lax.all_gather(rest, "fsdp", axis=0, tiled=True))
    fw = n * fc

    cond_float = condition.astype(F32)
    cond_act = jax.nn.silu(cond_float).astype(BF16)
    small = jnp.concatenate(
        [ada_bias.reshape(-1), qv_bias.reshape(-1), out_bias.reshape(-1), up_bias.reshape(-1),
         down_bias.reshape(-1), cond_act.reshape(-1)]
    )
    small = lax.all_gather(small, "fsdp", axis=0, tiled=False)
    pos = 0

    def unpack(per_layer):
        nonlocal pos
        part = small[:, pos: pos + layers * per_layer].reshape(n, layers, per_layer)
        pos += layers * per_layer
        return part.transpose(1, 0, 2).reshape(layers, n * per_layer)

    ada_b = unpack(ada_bias.shape[1]).astype(F32)
    qv_b = unpack(qv_bias.shape[1]).astype(F32)
    out_b = unpack(out_bias.shape[1]).astype(F32)
    up_b = unpack(up_bias.shape[1]).astype(F32)
    down_b = unpack(down_bias.shape[1]).astype(F32)
    cond_all = small[:, pos:]
    cond_rows = own(cond_all, 1, rows)
    q_b = take(qv_b[:, :width].reshape(layers, ns, hc), 1)
    v_b = take(qv_b[:, width:].reshape(layers, ns, hc), 1)
    qkv_b = jnp.concatenate([q_b, jnp.zeros_like(q_b), v_b], axis=1)
    up_bs = take(up_b.reshape(layers, n, ns, fc), 2).reshape(layers, fw)

    mod_partial = jnp.stack([mm(cond_rows, ada_weight[l]) for l in range(layers)], axis=1)
    mod = lax.psum_scatter(mod_partial, "fsdp", scatter_dimension=0, tiled=True)[0] + ada_b

    hidden = tokens[0].astype(F32)
    saved = []
    for l in range(layers):
        shift_a, scale_a, gate_a, shift_m, scale_m, gate_m = jnp.split(mod[l], 6)
        n_a, r_a = normalize(hidden)
        attn_in = (n_a * (1.0 + scale_a) + shift_a).astype(BF16)
        attn_all = lax.all_gather(attn_in, "seq", axis=0, tiled=True)
        qkv = (mm(attn_all, w_qkv[l]) + qkv_b[l]).astype(BF16)
        q, k, v = qkv[:, :hc], qkv[:, hc: 2 * hc], qkv[:, 2 * hc:]
        head_out, logsum = attend(q, k, v)
        tok_out = lax.all_to_all(head_out, "seq", split_axis=0, concat_axis=1, tiled=True)
        branch = mm(tok_out, w_rest[l][:, fw + width:]) + out_b[l]
        middle = hidden + gate_a * branch
        n_m, r_m = normalize(middle)
        mlp_in = (n_m * (1.0 + scale_m) + shift_m).astype(BF16)
        mlp_all = lax.all_gather(mlp_in, "seq", axis=0, tiled=True)
        up = mm(mlp_all, w_rest[l][:, :fw]) + up_bs[l]
        act = gelu_parts(up)[0].astype(BF16)
        feed = mm(act, w_rest[l][:, fw: fw + width])
        feed = lax.psum_scatter(feed, "seq", scatter_dimension=0, tiled=True) + down_b[l]
        saved.append((n_a, r_a, attn_all, q, k, v, logsum, tok_out, branch, n_m, r_m, mlp_all, up, act, feed))
        hidden = middle + gate_m * feed
    block_out = hidden.astype(BF16)

    g = cotangent[0].astype(F32)
    d_mods = [None] * layers
    reduced = [None] * layers
    bias_grads = [None] * layers
    for l in reversed(range(layers)):
        shift_a, scale_a, gate_a, shift_m, scale_m, gate_m = jnp.split(mod[l], 6)
        n_a, r_a, attn_all, q, k, v, logsum, tok_out, branch, n_m, r_m, mlp_all, up, act, feed = saved[l]
        g_feed = (gate_m * g).astype(BF16)
        d_gate_m = jnp.sum(g * feed, axis=0)
        g_feed_all = lax.all_gather(g_feed, "seq", axis=0, tiled=True)
        grad_down = mm_tn(act, g_feed_all)
        g_up = (mm_nt(g_feed_all, w_rest[l][:, fw: fw + width]) * gelu_parts(up)[1]).astype(BF16)
        grad_up = mm_tn(mlp_all, g_up)
        g_min = lax.psum_scatter(mm_nt(g_up, w_rest[l][:, :fw]), "seq", scatter_dimension=0, tiled=True)
        d_scale_m = jnp.sum(g_min * n_m, axis=0)
        d_shift_m = jnp.sum(g_min, axis=0)
        g_mid = g + norm_back(g_min * (1.0 + scale_m), n_m, r_m)
        g_branch = (gate_a * g_mid).astype(BF16)
        d_gate_a = jnp.sum(g_mid * branch, axis=0)
        grad_out = mm_tn(tok_out, g_branch)
        g_o = mm_nt(g_branch, w_rest[l][:, fw + width:]).astype(BF16)
        g_o_heads = lax.all_to_all(g_o, "seq", split_axis=1, concat_axis=0, tiled=True)
        dq, dk, dv = attend_back(q, k, v, logsum, g_o_heads)
        g_qkv = jnp.concatenate([dq, dk, dv], axis=1)
        grad_qkv = mm_tn(attn_all, g_qkv)
        g_ain = lax.psum_scatter(mm_nt(g_qkv, w_qkv[l]), "seq", scatter_dimension=0, tiled=True)
        d_scale_a = jnp.sum(g_ain * n_a, axis=0)
        d_shift_a = jnp.sum(g_ain, axis=0)
        g = g_mid + norm_back(g_ain * (1.0 + scale_a), n_a, r_a)
        d_mods[l] = jnp.concatenate([d_shift_a, d_scale_a, d_gate_a, d_shift_m, d_scale_m, d_gate_m])
        packed = jnp.concatenate([grad_up, grad_down, grad_out, grad_qkv], axis=1).astype(BF16)
        reduced[l] = lax.psum_scatter(packed, "fsdp", scatter_dimension=0, tiled=True)

        def place(x, axis):
            zeros = jnp.zeros(x.shape[:axis] + (ns,) + x.shape[axis + 1:], F32)
            return lax.dynamic_update_slice_in_dim(zeros, x, s, axis)

        qv_g = place(jnp.stack([jnp.sum(dq.astype(F32), axis=0), jnp.sum(dv.astype(F32), axis=0)])[:, None, :], 1)
        up_g = place(jnp.sum(g_up.astype(F32), axis=0).reshape(n, 1, fc), 1)
        bias_grads[l] = jnp.concatenate([
            qv_g.reshape(n, -1), jnp.sum(g_branch.astype(F32), axis=0).reshape(n, -1),
            up_g.reshape(n, -1), jnp.sum(g_feed.astype(F32), axis=0).reshape(n, -1)], axis=1)

    red = jnp.stack(reduced)
    shared = jnp.concatenate([red[:, :, : fw + width], red[:, :, fw + 2 * width:]], axis=2)
    shared = lax.all_gather(shared, "seq", axis=0, tiled=False).astype(F32)
    grad_up = shared[..., :fw].reshape(ns, layers, rows, n, fc).transpose(1, 2, 3, 0, 4).reshape(layers, rows, ff)
    grad_down = shared[..., fw: fw + width].transpose(1, 0, 2, 3).reshape(layers, ns * fc, width)
    grad_qkv = shared[..., fw + width:].reshape(ns, layers, rows, 3, hc).transpose(1, 2, 3, 0, 4)
    grad_qkv = grad_qkv.reshape(layers, rows, 3 * width)
    grad_out = lax.psum(red[:, :, fw + width: fw + 2 * width], "seq").astype(F32)

    bias = lax.psum(jnp.stack(bias_grads), ("fsdp", "seq"))
    bias = lax.dynamic_index_in_dim(bias, f, 1, keepdims=False)
    cuts = [qv_bias.shape[1], out_bias.shape[1], up_bias.shape[1], down_bias.shape[1]]
    grad_bias, at = [], 0
    for size in cuts:
        grad_bias.append(bias[:, at: at + size])
        at += size

    d_mod = lax.psum(jnp.stack(d_mods), "seq")
    d_mod_all = lax.all_gather(d_mod, "fsdp", axis=0, tiled=False)
    cond_rows32 = cond_rows.astype(F32)
    grad_ada = jnp.stack([
        lax.dot_general(cond_rows32, d_mod_all[:, l], (((0,), (0,)), ((), ())), precision=HIGHEST,
                        preferred_element_type=F32) for l in range(layers)])
    grad_ada_bias = own(jnp.sum(d_mod_all, axis=0), 1, width6 // n)
    g_cond = sum(
        lax.dot_general(d_mod_all[:, l], ada_weight[l].astype(F32), (((1,), (1,)), ((), ())),
                        precision=HIGHEST, preferred_element_type=F32) for l in range(layers))
    g_cond = lax.all_to_all(g_cond, "fsdp", split_axis=0, concat_axis=1, tiled=True)
    _, silu_back = jax.vjp(jax.nn.silu, cond_float)
    grad_condition = silu_back(g_cond)[0]
    return (
        block_out[None], g[None], grad_condition, grad_ada, grad_ada_bias, grad_qkv, grad_bias[0],
        grad_out, grad_bias[1], grad_up, grad_bias[2], grad_down, grad_bias[3],
    )


MESH = pl.DeviceIdType.MESH
FAST = 2
VMEM_LIMIT = 66_000_000


def rcopy(src, dst, send, recv, device):
    return pltpu.make_async_remote_copy(
        src_ref=src, dst_ref=dst, send_sem=send, recv_sem=recv, device_id=device, device_id_type=MESH
    )


def vmem_specs(count):
    return [pl.BlockSpec(memory_space=pltpu.VMEM)] * count


def entry_barrier(devices):
    barrier = pltpu.get_barrier_semaphore()
    for device in devices:
        pl.semaphore_signal(barrier, inc=1, device_id=device, device_id_type=MESH)
    pl.semaphore_wait(barrier, len(devices))


def relative(s, j):
    half = j // 2
    return ((s // 2 + 1 - half) % 2) * 2 + (s % 2 + half + j) % 2


def prep_kernel(n, cond_ref, small_ref, ada_ref, rows_ref, small_all, mod_ref,
                crecv, msend, mrecv, c_s, c_r, b_s, b_r, m_s, m_r):
    f = lax.axis_index("fsdp")
    layers, rows, _ = ada_ref.shape
    others = [{"fsdp": (f + k) % n} for k in range(1, n)]
    entry_barrier(others)
    first, second = [], []
    for k in range(1, n):
        to = (f + k) % n
        first.append(rcopy(cond_ref.at[to], crecv.at[f], c_s.at[k], c_r.at[k], {"fsdp": to}))
        first[-1].start()
    for k in range(1, n):
        to = (f + k) % n
        second.append(rcopy(small_ref, small_all.at[f], b_s.at[k], b_r.at[k], {"fsdp": to}))
        second[-1].start()
    crecv[f] = cond_ref[f]
    small_all[f] = small_ref[...]
    for k in range(1, n):
        at = (f - k + n) % n
        rcopy(cond_ref.at[at], crecv.at[at], c_s.at[k], c_r.at[k], {"fsdp": at}).wait_recv()
    cond_rows = jnp.sum(crecv[...], axis=1)
    rows_ref[...] = cond_rows
    cond_rows = cond_rows[:, :rows].astype(BF16)
    for l in range(layers):
        part = mm(cond_rows, ada_ref[l])
        for i in range(n):
            msend[i, l: l + 1, :] = part[i: i + 1, :]
    third = []
    for k in range(1, n):
        to = (f + k) % n
        third.append(rcopy(msend.at[to], mrecv.at[f], m_s.at[k], m_r.at[k], {"fsdp": to}))
        third[-1].start()
    mrecv[f] = msend[f]
    for k in range(1, n):
        at = (f - k + n) % n
        rcopy(msend.at[at], mrecv.at[at], m_s.at[k], m_r.at[k], {"fsdp": at}).wait_recv()
    mod_ref[...] = jnp.sum(mrecv[...], axis=0)
    for k in range(1, n):
        at = (f - k + n) % n
        rcopy(small_ref, small_all.at[at], b_s.at[k], b_r.at[k], {"fsdp": at}).wait_recv()
    for copy in first + second + third:
        copy.wait_send()


def prep(n, cond_blocks, small, ada_weight):
    layers, rows, width6 = ada_weight.shape
    lanes = cond_blocks.shape[-1]
    return pl.pallas_call(
        functools.partial(prep_kernel, n),
        out_shape=(
            jax.ShapeDtypeStruct((n, lanes), F32),
            jax.ShapeDtypeStruct((n,) + small.shape, F32),
            jax.ShapeDtypeStruct((layers, width6), F32),
        ),
        in_specs=vmem_specs(3),
        out_specs=tuple(vmem_specs(3)),
        scratch_shapes=[
            pltpu.VMEM((n, 8, lanes), F32),
            pltpu.VMEM((n, layers, width6), F32),
            pltpu.VMEM((n, layers, width6), F32),
        ] + [pltpu.SemaphoreType.DMA((n,))] * 6,
        compiler_params=pltpu.CompilerParams(collective_id=0, has_side_effects=True),
    )(cond_blocks, small, ada_weight)


def forward_kernel(n, *refs):
    (x_ref, mod_ref, bq_ref, bo_ref, bu_ref, bd_ref, sq_ref, so_ref, su_ref, sd_ref,
     out_ref, wq_ref, wo_ref, wu_ref, wd_ref, xs_ref, attn_ref, qh_ref, tok_ref, branch_ref,
     mid_ref, mlp_ref, up_ref, feed_ref,
     osend, psend, precv, xsend, xrecv, own_feed,
     z_s, z_r, y_s, y_r, a_s, a_r, t_s, t_r, g_s, g_r, r_s, r_r) = refs
    f = lax.axis_index("fsdp")
    s = lax.axis_index("seq")
    slow = n // FAST
    a, b = f // FAST, f % FAST
    layers, rows = sq_ref.shape[0], sq_ref.shape[1]
    block = x_ref.shape[0]
    width = x_ref.shape[1]
    hc = sq_ref.shape[2] // 3
    heads = hc // HEAD_DIM
    shards = (sq_ref, so_ref, su_ref, sd_ref)
    full = (wq_ref, wo_ref, wu_ref, wd_ref)
    across, diagonal, partner = relative(s, 0), relative(s, 1), relative(s, 2)
    y_dev = {"fsdp": a * FAST + (1 - b)}

    entry_barrier(
        [{"fsdp": ((a + k) % slow) * FAST + b} for k in range(1, slow)] + [y_dev]
        + [{"seq": across}, {"seq": diagonal}, {"seq": partner}]
    )

    def z_copy(l, p, k, to):
        return rcopy(shards[p].at[l], full[p].at[l, f], z_s.at[l, p, k], z_r.at[l, p, k], {"fsdp": to})

    def y_copy(l, p, k):
        at = ((a - k + slow) % slow) * FAST + b
        src = shards[p].at[l] if k == 0 else full[p].at[l, at]
        return rcopy(src, full[p].at[l, at], y_s.at[l, p, k], y_r.at[l, p, k], y_dev)

    for l in range(layers):
        for p in range(4):
            y_copy(l, p, 0).start()
            for k in range(1, slow):
                z_copy(l, p, k, ((a + k) % slow) * FAST + b).start()

    def forward_weights(l, p):
        for k in range(1, slow):
            at = ((a - k + slow) % slow) * FAST + b
            rcopy(shards[p].at[l], full[p].at[l, at], z_s.at[l, p, k], z_r.at[l, p, k], {"fsdp": at}).wait_recv()
            y_copy(l, p, k).start()

    def ready(l, p):
        for k in range(slow):
            at = ((a - k + slow) % slow) * FAST + 1 - b
            rcopy(shards[p].at[l], full[p].at[l, at], y_s.at[l, p, k], y_r.at[l, p, k], y_dev).wait_recv()

    xs_ref[0] = x_ref[...].astype(F32)
    for l in range(layers):
        for p in range(4):
            full[p][l, f] = shards[p][l]

    def matrix(ref, l):
        return ref[l].reshape(n * rows, ref.shape[3])

    def gather(buf, l, send, recv, visit):
        mine = buf.at[l, s]
        to_partner = rcopy(mine, mine, send.at[0], recv.at[0], {"seq": partner})
        to_across = rcopy(mine, mine, send.at[1], recv.at[1], {"seq": across})
        to_across.start()
        to_partner.start()
        theirs = buf.at[l, across]
        relay = rcopy(theirs, theirs, send.at[2], recv.at[2], {"seq": partner})

        def step(i, carry):
            @pl.when(i == 1)
            def _():
                ref = buf.at[l, partner]
                rcopy(ref, ref, send.at[0], recv.at[0], {"seq": partner}).wait_recv()

            @pl.when(i == 2)
            def _():
                rcopy(theirs, theirs, send.at[1], recv.at[1], {"seq": across}).wait_recv()
                relay.start()

            @pl.when(i == 3)
            def _():
                ref = buf.at[l, diagonal]
                rcopy(ref, ref, send.at[2], recv.at[2], {"seq": partner}).wait_recv()

            visit(i, relative(s, pick(i)))
            return carry

        lax.fori_loop(0, 4, step, 0)
        for copy in (to_partner, to_across, relay):
            copy.wait_send()

    def pick(i):
        return (3 - i) * (1 - i // 2) + (i - 2) * (i // 2)

    def layer(l, carry):
        row = lambda i: mod_ref[l, i: i + 1, :]
        x = xs_ref[l]
        normed, _ = normalize(x)
        attn_ref[l, s] = (normed * (1.0 + row(1)) + row(0)).astype(BF16)

        @pl.when(l == 0)
        def _():
            forward_weights(0, 0)

        def qkv_block(i, t):
            @pl.when(i == 0)
            def _():
                ready(l, 0)

            val = (mm(attn_ref[l, t], matrix(wq_ref, l)) + bq_ref[l]).astype(BF16)
            for h in range(3 * heads):
                qh_ref[l, h, pl.ds(pl.multiple_of(t * block, block), block), :] = (
                    val[:, h * HEAD_DIM: (h + 1) * HEAD_DIM]
                )

        gather(attn_ref, l, a_s, a_r, qkv_block)
        forward_weights(l, 1)

        def attend_block(j, carry):
            t = relative(s, j)
            outs = []
            for h in range(heads):
                q = qh_ref[l, h, pl.ds(pl.multiple_of(t * block, block), block), :]
                scores = mm_nt(q, qh_ref[l, heads + h]) * SCORE_SCALE
                e = jnp.exp(scores)
                inverse = 1.0 / jnp.sum(e, axis=-1, keepdims=True)
                prob = (e * inverse).astype(BF16)
                outs.append(mm(prob, qh_ref[l, 2 * heads + h]))
            osend[j] = jnp.concatenate(outs, axis=1).astype(BF16)

            @pl.when(j < 3)
            def _():
                rcopy(osend.at[j], tok_ref.at[l, s], t_s.at[j], t_r.at[j], {"seq": t}).start()

            @pl.when(j == 1)
            def _():
                forward_weights(l, 2)

            return carry

        lax.fori_loop(0, 4, attend_block, 0)
        tok_ref[l, s] = osend[3]
        forward_weights(l, 3)
        ready(l, 1)
        for j in range(3):
            t = relative(s, j)
            rcopy(osend.at[j], tok_ref.at[l, t], t_s.at[j], t_r.at[j], {"seq": t}).wait_recv()
        tokens_out = jnp.concatenate([tok_ref[l, t] for t in range(4)], axis=1)
        branch = mm(tokens_out, matrix(wo_ref, l)) + bo_ref[l]
        branch_ref[l] = branch
        middle = xs_ref[l] + row(2) * branch
        mid_ref[l] = middle
        normed, _ = normalize(middle)
        mlp_ref[l, s] = (normed * (1.0 + row(4)) + row(3)).astype(BF16)

        def mlp_block(i, t):
            @pl.when(i == 0)
            def _():
                ready(l, 2)
                ready(l, 3)

            up = mm(mlp_ref[l, t], matrix(wu_ref, l)) + bu_ref[l]
            up_ref[l, t] = up
            act = gelu_parts(up)[0].astype(BF16)
            part = mm(act, matrix(wd_ref, l))

            @pl.when(i == 0)
            def _():
                own_feed[...] = part

            @pl.when(i == 1)
            def _():
                psend[0] = part
                rcopy(psend.at[0], precv.at[0], r_s.at[0], r_r.at[0], {"seq": partner}).start()

            @pl.when(i == 2)
            def _():
                xsend[...] = part

            @pl.when(i == 3)
            def _():
                psend[1] = part
                rcopy(psend.at[1], precv.at[1], r_s.at[1], r_r.at[1], {"seq": partner}).start()

            @pl.when((i == 1) & (l + 1 < layers))
            def _():
                forward_weights(1, 0)

        gather(mlp_ref, l, g_s, g_r, mlp_block)
        rcopy(psend.at[1], precv.at[1], r_s.at[1], r_r.at[1], {"seq": partner}).wait_recv()
        xsend[...] = xsend[...] + precv[1]
        over = rcopy(xsend, xrecv, r_s.at[2], r_r.at[2], {"seq": across})
        over.start()
        rcopy(psend.at[0], precv.at[0], r_s.at[0], r_r.at[0], {"seq": partner}).wait_recv()
        own_feed[...] = own_feed[...] + precv[0] + bd_ref[l]
        over.wait_recv()
        feed = own_feed[...] + xrecv[...]
        feed_ref[l] = feed
        nxt = mid_ref[l] + row(5) * feed

        @pl.when(l + 1 < layers)
        def _():
            xs_ref[1] = nxt

        @pl.when(l + 1 == layers)
        def _():
            out_ref[...] = nxt.astype(BF16)

        over.wait_send()
        for i in range(2):
            rcopy(psend.at[i], precv.at[i], r_s.at[i], r_r.at[i], {"seq": partner}).wait_send()
        for j in range(3):
            rcopy(osend.at[j], tok_ref.at[l, s], t_s.at[j], t_r.at[j], {"seq": relative(s, j)}).wait_send()
        return carry

    lax.fori_loop(0, layers, layer, 0)
    for l in range(layers):
        for p in range(4):
            y_copy(l, p, 0).wait_send()
            for k in range(1, slow):
                z_copy(l, p, k, ((a + k) % slow) * FAST + b).wait_send()
                y_copy(l, p, k).wait_send()


def forward(n, x, mod, bq, bo, bu, bd, sq, so, su, sd):
    layers, rows, qc = sq.shape
    block, width = x.shape
    hc = qc // 3
    nh = qc // HEAD_DIM
    uc = su.shape[2]
    total = 4 * block
    sds = jax.ShapeDtypeStruct
    outs = (
        sds((block, width), BF16),
        sds((layers, n, rows, qc), BF16),
        sds((layers, n, rows, width), BF16),
        sds((layers, n, rows, uc), BF16),
        sds((layers, n, rows, width), BF16),
        sds((layers, block, width), F32),
        sds((layers, 4, block, width), BF16),
        sds((layers, nh, total, HEAD_DIM), BF16),
        sds((layers, 4, block, hc), BF16),
        sds((layers, block, width), F32),
        sds((layers, block, width), F32),
        sds((layers, 4, block, width), BF16),
        sds((layers, 4, block, uc), F32),
        sds((layers, block, width), F32),
    )
    slow = n // FAST
    dma = pltpu.SemaphoreType.DMA
    scratch = [
        pltpu.VMEM((4, block, hc), BF16),
        pltpu.VMEM((2, block, width), F32),
        pltpu.VMEM((2, block, width), F32),
        pltpu.VMEM((block, width), F32),
        pltpu.VMEM((block, width), F32),
        pltpu.VMEM((block, width), F32),
    ] + [dma((layers, 4, slow))] * 4 + [dma((3,))] * 8
    return pl.pallas_call(
        functools.partial(forward_kernel, n),
        out_shape=outs,
        in_specs=vmem_specs(10),
        out_specs=tuple(vmem_specs(len(outs))),
        scratch_shapes=scratch,
        compiler_params=pltpu.CompilerParams(
            collective_id=1, has_side_effects=True, vmem_limit_bytes=VMEM_LIMIT
        ),
    )(x, mod, bq, bo, bu, bd, sq, so, su, sd)


def fused_device(
    tokens, condition, ada_weight, ada_bias, qkv_weight, qv_bias, out_weight, out_bias,
    up_weight, up_bias, down_weight, down_bias, cotangent,
):
    n = lax.axis_size("fsdp")
    ns = lax.axis_size("seq")
    f = lax.axis_index("fsdp")
    s = lax.axis_index("seq")
    layers, rows, width6 = ada_weight.shape
    width = rows * n
    ff = up_weight.shape[2]
    hc = width // ns
    fc = ff // (ns * n)

    def take(x, axis):
        return lax.dynamic_index_in_dim(x, s, axis, keepdims=False)

    def own(x, axis, size):
        return lax.dynamic_slice_in_dim(x, f * size, size, axis)

    fw = n * fc
    s_q = take(qkv_weight.reshape(layers, rows, 3, ns, hc), 3).reshape(layers, rows, 3 * hc)
    s_u = take(up_weight.reshape(layers, rows, n, ns, fc), 3).reshape(layers, rows, fw)
    s_d = take(down_weight.reshape(layers, ns, fc, width), 1)

    cond_float = condition.astype(F32)
    cond_act = jax.nn.silu(cond_float).astype(BF16)
    cond_blocks = jnp.pad(cond_act.astype(F32).reshape(n, 1, rows), ((0, 0), (0, 7), (0, -rows % 128)))
    small = jnp.concatenate(
        [ada_bias.reshape(-1), qv_bias.reshape(-1), out_bias.reshape(-1), up_bias.reshape(-1),
         down_bias.reshape(-1)]
    ).astype(F32).reshape(8, -1)
    cond_rows, small, mod = prep(n, cond_blocks, small, ada_weight)
    cond_rows = cond_rows[:, :rows]
    small = small.reshape(n, -1)
    pos = 0

    def unpack(per_layer):
        nonlocal pos
        part = small[:, pos: pos + layers * per_layer].reshape(n, layers, per_layer)
        pos += layers * per_layer
        return part.transpose(1, 0, 2).reshape(layers, n * per_layer)

    ada_b = unpack(ada_bias.shape[1])
    qv_b = unpack(qv_bias.shape[1])
    out_b = unpack(out_bias.shape[1])
    up_b = unpack(up_bias.shape[1])
    down_b = unpack(down_bias.shape[1])
    q_b = take(qv_b[:, :width].reshape(layers, ns, hc), 1)
    v_b = take(qv_b[:, width:].reshape(layers, ns, hc), 1)
    qkv_b = jnp.concatenate([q_b, jnp.zeros_like(q_b), v_b], axis=1)
    up_bs = take(up_b.reshape(layers, n, ns, fc), 2).reshape(layers, fw)
    mod = mod + ada_b

    (block_out, w_q, w_o, w_u, w_d, xs, attn, qh, tok, branches, mids, mlp, ups, feeds) = forward(
        n, tokens[0], mod.reshape(layers, 6, width), qkv_b[:, None], out_b[:, None], up_bs[:, None],
        down_b[:, None], s_q, out_weight, s_u, s_d)
    saved, w_qkv, w_rest = [], [], []
    nh = hc // HEAD_DIM
    for l in range(layers):
        n_a, r_a = normalize(xs[l])
        n_m, r_m = normalize(mids[l])
        q, k, v = [join_heads(qh[l, i * nh: (i + 1) * nh]) for i in range(3)]
        scores = jnp.einsum("hqd,hkd->hqk", split_heads(q), split_heads(k), preferred_element_type=F32) * SCORE_SCALE
        logsum = jnp.log(jnp.sum(jnp.exp(scores), axis=-1, keepdims=True))
        up = ups[l].reshape(-1, fw)
        saved.append((n_a, r_a, attn[l].reshape(-1, width), q, k, v, logsum,
                      tok[l].transpose(1, 0, 2).reshape(-1, width), branches[l], n_m, r_m,
                      mlp[l].reshape(-1, width), up, gelu_parts(up)[0].astype(BF16), feeds[l]))
        w_qkv.append(w_q[l].reshape(width, -1))
        w_rest.append(jnp.concatenate([w.reshape(width, -1) for w in (w_u[l], w_d[l], w_o[l])], axis=1))

    g = cotangent[0].astype(F32)
    d_mods = [None] * layers
    reduced = [None] * layers
    bias_grads = [None] * layers
    for l in reversed(range(layers)):
        shift_a, scale_a, gate_a, shift_m, scale_m, gate_m = jnp.split(mod[l], 6)
        n_a, r_a, attn_all, q, k, v, logsum, tok_out, branch, n_m, r_m, mlp_all, up, act, feed = saved[l]
        g_feed = (gate_m * g).astype(BF16)
        d_gate_m = jnp.sum(g * feed, axis=0)
        g_feed_all = lax.all_gather(g_feed, "seq", axis=0, tiled=True)
        grad_down = mm_tn(act, g_feed_all)
        g_up = (mm_nt(g_feed_all, w_rest[l][:, fw: fw + width]) * gelu_parts(up)[1]).astype(BF16)
        grad_up = mm_tn(mlp_all, g_up)
        g_min = lax.psum_scatter(mm_nt(g_up, w_rest[l][:, :fw]), "seq", scatter_dimension=0, tiled=True)
        d_scale_m = jnp.sum(g_min * n_m, axis=0)
        d_shift_m = jnp.sum(g_min, axis=0)
        g_mid = g + norm_back(g_min * (1.0 + scale_m), n_m, r_m)
        g_branch = (gate_a * g_mid).astype(BF16)
        d_gate_a = jnp.sum(g_mid * branch, axis=0)
        grad_out = mm_tn(tok_out, g_branch)
        g_o = mm_nt(g_branch, w_rest[l][:, fw + width:]).astype(BF16)
        g_o_heads = lax.all_to_all(g_o, "seq", split_axis=1, concat_axis=0, tiled=True)
        dq, dk, dv = attend_back(q, k, v, logsum, g_o_heads)
        g_qkv = jnp.concatenate([dq, dk, dv], axis=1)
        grad_qkv = mm_tn(attn_all, g_qkv)
        g_ain = lax.psum_scatter(mm_nt(g_qkv, w_qkv[l]), "seq", scatter_dimension=0, tiled=True)
        d_scale_a = jnp.sum(g_ain * n_a, axis=0)
        d_shift_a = jnp.sum(g_ain, axis=0)
        g = g_mid + norm_back(g_ain * (1.0 + scale_a), n_a, r_a)
        d_mods[l] = jnp.concatenate([d_shift_a, d_scale_a, d_gate_a, d_shift_m, d_scale_m, d_gate_m])
        packed = jnp.concatenate([grad_up, grad_down, grad_out, grad_qkv], axis=1).astype(BF16)
        reduced[l] = lax.psum_scatter(packed, "fsdp", scatter_dimension=0, tiled=True)

        def place(x, axis):
            zeros = jnp.zeros(x.shape[:axis] + (ns,) + x.shape[axis + 1:], F32)
            return lax.dynamic_update_slice_in_dim(zeros, x, s, axis)

        qv_g = place(jnp.stack([jnp.sum(dq.astype(F32), axis=0), jnp.sum(dv.astype(F32), axis=0)])[:, None, :], 1)
        up_g = place(jnp.sum(g_up.astype(F32), axis=0).reshape(n, 1, fc), 1)
        bias_grads[l] = jnp.concatenate([
            qv_g.reshape(n, -1), jnp.sum(g_branch.astype(F32), axis=0).reshape(n, -1),
            up_g.reshape(n, -1), jnp.sum(g_feed.astype(F32), axis=0).reshape(n, -1)], axis=1)

    red = jnp.stack(reduced)
    shared = jnp.concatenate([red[:, :, : fw + width], red[:, :, fw + 2 * width:]], axis=2)
    shared = lax.all_gather(shared, "seq", axis=0, tiled=False).astype(F32)
    grad_up = shared[..., :fw].reshape(ns, layers, rows, n, fc).transpose(1, 2, 3, 0, 4).reshape(layers, rows, ff)
    grad_down = shared[..., fw: fw + width].transpose(1, 0, 2, 3).reshape(layers, ns * fc, width)
    grad_qkv = shared[..., fw + width:].reshape(ns, layers, rows, 3, hc).transpose(1, 2, 3, 0, 4)
    grad_qkv = grad_qkv.reshape(layers, rows, 3 * width)
    grad_out = lax.psum(red[:, :, fw + width: fw + 2 * width], "seq").astype(F32)

    bias = lax.psum(jnp.stack(bias_grads), ("fsdp", "seq"))
    bias = lax.dynamic_index_in_dim(bias, f, 1, keepdims=False)
    cuts = [qv_bias.shape[1], out_bias.shape[1], up_bias.shape[1], down_bias.shape[1]]
    grad_bias, at = [], 0
    for size in cuts:
        grad_bias.append(bias[:, at: at + size])
        at += size

    d_mod = lax.psum(jnp.stack(d_mods), "seq")
    d_mod_all = lax.all_gather(d_mod, "fsdp", axis=0, tiled=False)
    cond_rows32 = cond_rows.astype(F32)
    grad_ada = jnp.stack([
        lax.dot_general(cond_rows32, d_mod_all[:, l], (((0,), (0,)), ((), ())), precision=HIGHEST,
                        preferred_element_type=F32) for l in range(layers)])
    grad_ada_bias = own(jnp.sum(d_mod_all, axis=0), 1, width6 // n)
    g_cond = sum(
        lax.dot_general(d_mod_all[:, l], ada_weight[l].astype(F32), (((1,), (1,)), ((), ())),
                        precision=HIGHEST, preferred_element_type=F32) for l in range(layers))
    g_cond = lax.all_to_all(g_cond, "fsdp", split_axis=0, concat_axis=1, tiled=True)
    _, silu_back = jax.vjp(jax.nn.silu, cond_float)
    grad_condition = silu_back(g_cond)[0]
    return (
        block_out[None], g[None], grad_condition, grad_ada, grad_ada_bias, grad_qkv, grad_bias[0],
        grad_out, grad_bias[1], grad_up, grad_bias[2], grad_down, grad_bias[3],
    )


def solution(mesh):
    token = P("fsdp", "seq", None)
    matrix = P(None, "fsdp", None)
    vector = P(None, "fsdp")

    def per_device(*args):
        rows = args[2].shape[1]
        fits = rows % 32 == 0 and mesh.shape["seq"] == 4 and args[0].shape[0] == 1
        return (fused_device if fits else plain_device)(*args)

    return jax.shard_map(
        per_device,
        mesh=mesh,
        in_specs=(token, P("fsdp", None)) + (matrix, vector) * 5 + (token,),
        out_specs=(token, token, P("fsdp", None)) + (matrix, vector) * 5,
        check_vma=False,
    )
```

```python
import functools

import jax
import jax.numpy as jnp
from jax import lax
from jax.experimental import pallas as pl
from jax.experimental.pallas import tpu as pltpu
from jax.sharding import PartitionSpec as P

HEAD_DIM = 64
SCORE_SCALE = HEAD_DIM ** (-0.5)
EPSILON = 1e-06
HIGHEST = lax.Precision.HIGHEST
F32 = jnp.float32
BF16 = jnp.bfloat16


def normalize(values):
    centred = values - jnp.mean(values, axis=-1, keepdims=True)
    inverse = lax.rsqrt(jnp.mean(centred * centred, axis=-1, keepdims=True) + EPSILON)
    return centred * inverse, inverse


def norm_back(gradient, normed, inverse):
    return inverse * (
        gradient
        - jnp.mean(gradient, axis=-1, keepdims=True)
        - normed * jnp.mean(gradient * normed, axis=-1, keepdims=True)
    )


def mm(a, b):
    return lax.dot_general(a, b, (((1,), (0,)), ((), ())), preferred_element_type=F32)


def mm_nt(a, b):
    return lax.dot_general(a, b, (((1,), (1,)), ((), ())), preferred_element_type=F32)


def mm_tn(a, b):
    return lax.dot_general(a, b, (((0,), (0,)), ((), ())), preferred_element_type=F32)


def split_heads(rows):
    return rows.reshape(rows.shape[0], -1, HEAD_DIM).transpose(1, 0, 2)


def join_heads(heads):
    return heads.transpose(1, 0, 2).reshape(heads.shape[1], -1)


def attend(q, k, v):
    q, k, v = split_heads(q), split_heads(k), split_heads(v)
    scores = jnp.einsum("hqd,hkd->hqk", q, k, preferred_element_type=F32) * SCORE_SCALE
    logsum = jnp.log(jnp.sum(jnp.exp(scores), axis=-1, keepdims=True))
    prob = jnp.exp(scores - logsum).astype(BF16)
    out = jnp.einsum("hqk,hkd->hqd", prob, v, preferred_element_type=F32)
    return join_heads(out).astype(BF16), logsum


def attend_back(q, k, v, logsum, out_grad):
    q, k, v, out_grad = split_heads(q), split_heads(k), split_heads(v), split_heads(out_grad)
    scores = jnp.einsum("hqd,hkd->hqk", q, k, preferred_element_type=F32) * SCORE_SCALE
    prob = jnp.exp(scores - logsum)
    dv = jnp.einsum("hqk,hqd->hkd", prob.astype(BF16), out_grad, preferred_element_type=F32)
    dp = jnp.einsum("hqd,hkd->hqk", out_grad, v, preferred_element_type=F32)
    inner = jnp.sum(prob * dp, axis=-1, keepdims=True)
    ds = (prob * (dp - inner)).astype(BF16)
    dq = jnp.einsum("hqk,hkd->hqd", ds, k, preferred_element_type=F32) * SCORE_SCALE
    dk = jnp.einsum("hqk,hqd->hkd", ds, q, preferred_element_type=F32) * SCORE_SCALE
    return [join_heads(t).astype(BF16) for t in (dq, dk, dv)]


def gelu_parts(u):
    c = 0.7978845608028654
    inner = c * (u + 0.044715 * (u * u * u))
    t = jnp.tanh(inner)
    value = 0.5 * u * (1.0 + t)
    slope = 0.5 * (1.0 + t) + 0.5 * u * (1.0 - t * t) * (c * (1.0 + 3.0 * 0.044715 * u * u))
    return value, slope


def plain_device(
    tokens, condition, ada_weight, ada_bias, qkv_weight, qv_bias, out_weight, out_bias,
    up_weight, up_bias, down_weight, down_bias, cotangent,
):
    n = lax.axis_size("fsdp")
    ns = lax.axis_size("seq")
    f = lax.axis_index("fsdp")
    s = lax.axis_index("seq")
    layers, rows, width6 = ada_weight.shape
    width = rows * n
    ff = up_weight.shape[2]
    hc = width // ns
    fc = ff // (ns * n)

    def take(x, axis):
        return lax.dynamic_index_in_dim(x, s, axis, keepdims=False)

    def own(x, axis, size):
        return lax.dynamic_slice_in_dim(x, f * size, size, axis)

    w_qkv, w_rest = [], []
    for l in range(layers):
        q_part = take(qkv_weight[l].reshape(rows, 3, ns, hc), 2).reshape(rows, 3 * hc)
        u_part = take(up_weight[l].reshape(rows, n, ns, fc), 2).reshape(rows, n * fc)
        d_part = take(down_weight[l].reshape(ns, fc, width), 0)
        w_qkv.append(lax.all_gather(q_part, "fsdp", axis=0, tiled=True))
        rest = jnp.concatenate([u_part, d_part, out_weight[l]], axis=1)
        w_rest.append(lax.all_gather(rest, "fsdp", axis=0, tiled=True))
    fw = n * fc

    cond_float = condition.astype(F32)
    cond_act = jax.nn.silu(cond_float).astype(BF16)
    small = jnp.concatenate(
        [ada_bias.reshape(-1), qv_bias.reshape(-1), out_bias.reshape(-1), up_bias.reshape(-1),
         down_bias.reshape(-1), cond_act.reshape(-1)]
    )
    small = lax.all_gather(small, "fsdp", axis=0, tiled=False)
    pos = 0

    def unpack(per_layer):
        nonlocal pos
        part = small[:, pos: pos + layers * per_layer].reshape(n, layers, per_layer)
        pos += layers * per_layer
        return part.transpose(1, 0, 2).reshape(layers, n * per_layer)

    ada_b = unpack(ada_bias.shape[1]).astype(F32)
    qv_b = unpack(qv_bias.shape[1]).astype(F32)
    out_b = unpack(out_bias.shape[1]).astype(F32)
    up_b = unpack(up_bias.shape[1]).astype(F32)
    down_b = unpack(down_bias.shape[1]).astype(F32)
    cond_all = small[:, pos:]
    cond_rows = own(cond_all, 1, rows)
    q_b = take(qv_b[:, :width].reshape(layers, ns, hc), 1)
    v_b = take(qv_b[:, width:].reshape(layers, ns, hc), 1)
    qkv_b = jnp.concatenate([q_b, jnp.zeros_like(q_b), v_b], axis=1)
    up_bs = take(up_b.reshape(layers, n, ns, fc), 2).reshape(layers, fw)

    mod_partial = jnp.stack([mm(cond_rows, ada_weight[l]) for l in range(layers)], axis=1)
    mod = lax.psum_scatter(mod_partial, "fsdp", scatter_dimension=0, tiled=True)[0] + ada_b

    hidden = tokens[0].astype(F32)
    saved = []
    for l in range(layers):
        shift_a, scale_a, gate_a, shift_m, scale_m, gate_m = jnp.split(mod[l], 6)
        n_a, r_a = normalize(hidden)
        attn_in = (n_a * (1.0 + scale_a) + shift_a).astype(BF16)
        attn_all = lax.all_gather(attn_in, "seq", axis=0, tiled=True)
        qkv = (mm(attn_all, w_qkv[l]) + qkv_b[l]).astype(BF16)
        q, k, v = qkv[:, :hc], qkv[:, hc: 2 * hc], qkv[:, 2 * hc:]
        head_out, logsum = attend(q, k, v)
        tok_out = lax.all_to_all(head_out, "seq", split_axis=0, concat_axis=1, tiled=True)
        branch = mm(tok_out, w_rest[l][:, fw + width:]) + out_b[l]
        middle = hidden + gate_a * branch
        n_m, r_m = normalize(middle)
        mlp_in = (n_m * (1.0 + scale_m) + shift_m).astype(BF16)
        mlp_all = lax.all_gather(mlp_in, "seq", axis=0, tiled=True)
        up = mm(mlp_all, w_rest[l][:, :fw]) + up_bs[l]
        act = gelu_parts(up)[0].astype(BF16)
        feed = mm(act, w_rest[l][:, fw: fw + width])
        feed = lax.psum_scatter(feed, "seq", scatter_dimension=0, tiled=True) + down_b[l]
        saved.append((n_a, r_a, attn_all, q, k, v, logsum, tok_out, branch, n_m, r_m, mlp_all, up, act, feed))
        hidden = middle + gate_m * feed
    block_out = hidden.astype(BF16)

    g = cotangent[0].astype(F32)
    d_mods = [None] * layers
    reduced = [None] * layers
    bias_grads = [None] * layers
    for l in reversed(range(layers)):
        shift_a, scale_a, gate_a, shift_m, scale_m, gate_m = jnp.split(mod[l], 6)
        n_a, r_a, attn_all, q, k, v, logsum, tok_out, branch, n_m, r_m, mlp_all, up, act, feed = saved[l]
        g_feed = (gate_m * g).astype(BF16)
        d_gate_m = jnp.sum(g * feed, axis=0)
        g_feed_all = lax.all_gather(g_feed, "seq", axis=0, tiled=True)
        grad_down = mm_tn(act, g_feed_all)
        g_up = (mm_nt(g_feed_all, w_rest[l][:, fw: fw + width]) * gelu_parts(up)[1]).astype(BF16)
        grad_up = mm_tn(mlp_all, g_up)
        g_min = lax.psum_scatter(mm_nt(g_up, w_rest[l][:, :fw]), "seq", scatter_dimension=0, tiled=True)
        d_scale_m = jnp.sum(g_min * n_m, axis=0)
        d_shift_m = jnp.sum(g_min, axis=0)
        g_mid = g + norm_back(g_min * (1.0 + scale_m), n_m, r_m)
        g_branch = (gate_a * g_mid).astype(BF16)
        d_gate_a = jnp.sum(g_mid * branch, axis=0)
        grad_out = mm_tn(tok_out, g_branch)
        g_o = mm_nt(g_branch, w_rest[l][:, fw + width:]).astype(BF16)
        g_o_heads = lax.all_to_all(g_o, "seq", split_axis=1, concat_axis=0, tiled=True)
        dq, dk, dv = attend_back(q, k, v, logsum, g_o_heads)
        g_qkv = jnp.concatenate([dq, dk, dv], axis=1)
        grad_qkv = mm_tn(attn_all, g_qkv)
        g_ain = lax.psum_scatter(mm_nt(g_qkv, w_qkv[l]), "seq", scatter_dimension=0, tiled=True)
        d_scale_a = jnp.sum(g_ain * n_a, axis=0)
        d_shift_a = jnp.sum(g_ain, axis=0)
        g = g_mid + norm_back(g_ain * (1.0 + scale_a), n_a, r_a)
        d_mods[l] = jnp.concatenate([d_shift_a, d_scale_a, d_gate_a, d_shift_m, d_scale_m, d_gate_m])
        packed = jnp.concatenate([grad_up, grad_down, grad_out, grad_qkv], axis=1).astype(BF16)
        reduced[l] = lax.psum_scatter(packed, "fsdp", scatter_dimension=0, tiled=True)

        def place(x, axis):
            zeros = jnp.zeros(x.shape[:axis] + (ns,) + x.shape[axis + 1:], F32)
            return lax.dynamic_update_slice_in_dim(zeros, x, s, axis)

        qv_g = place(jnp.stack([jnp.sum(dq.astype(F32), axis=0), jnp.sum(dv.astype(F32), axis=0)])[:, None, :], 1)
        up_g = place(jnp.sum(g_up.astype(F32), axis=0).reshape(n, 1, fc), 1)
        bias_grads[l] = jnp.concatenate([
            qv_g.reshape(n, -1), jnp.sum(g_branch.astype(F32), axis=0).reshape(n, -1),
            up_g.reshape(n, -1), jnp.sum(g_feed.astype(F32), axis=0).reshape(n, -1)], axis=1)

    red = jnp.stack(reduced)
    shared = jnp.concatenate([red[:, :, : fw + width], red[:, :, fw + 2 * width:]], axis=2)
    shared = lax.all_gather(shared, "seq", axis=0, tiled=False).astype(F32)
    grad_up = shared[..., :fw].reshape(ns, layers, rows, n, fc).transpose(1, 2, 3, 0, 4).reshape(layers, rows, ff)
    grad_down = shared[..., fw: fw + width].transpose(1, 0, 2, 3).reshape(layers, ns * fc, width)
    grad_qkv = shared[..., fw + width:].reshape(ns, layers, rows, 3, hc).transpose(1, 2, 3, 0, 4)
    grad_qkv = grad_qkv.reshape(layers, rows, 3 * width)
    grad_out = lax.psum(red[:, :, fw + width: fw + 2 * width], "seq").astype(F32)

    bias = lax.psum(jnp.stack(bias_grads), ("fsdp", "seq"))
    bias = lax.dynamic_index_in_dim(bias, f, 1, keepdims=False)
    cuts = [qv_bias.shape[1], out_bias.shape[1], up_bias.shape[1], down_bias.shape[1]]
    grad_bias, at = [], 0
    for size in cuts:
        grad_bias.append(bias[:, at: at + size])
        at += size

    d_mod = lax.psum(jnp.stack(d_mods), "seq")
    d_mod_all = lax.all_gather(d_mod, "fsdp", axis=0, tiled=False)
    cond_rows32 = cond_rows.astype(F32)
    grad_ada = jnp.stack([
        lax.dot_general(cond_rows32, d_mod_all[:, l], (((0,), (0,)), ((), ())), precision=HIGHEST,
                        preferred_element_type=F32) for l in range(layers)])
    grad_ada_bias = own(jnp.sum(d_mod_all, axis=0), 1, width6 // n)
    g_cond = sum(
        lax.dot_general(d_mod_all[:, l], ada_weight[l].astype(F32), (((1,), (1,)), ((), ())),
                        precision=HIGHEST, preferred_element_type=F32) for l in range(layers))
    g_cond = lax.all_to_all(g_cond, "fsdp", split_axis=0, concat_axis=1, tiled=True)
    _, silu_back = jax.vjp(jax.nn.silu, cond_float)
    grad_condition = silu_back(g_cond)[0]
    return (
        block_out[None], g[None], grad_condition, grad_ada, grad_ada_bias, grad_qkv, grad_bias[0],
        grad_out, grad_bias[1], grad_up, grad_bias[2], grad_down, grad_bias[3],
    )


MESH = pl.DeviceIdType.MESH
FAST = 2
VMEM_LIMIT = 66_000_000


def rcopy(src, dst, send, recv, device):
    return pltpu.make_async_remote_copy(
        src_ref=src, dst_ref=dst, send_sem=send, recv_sem=recv, device_id=device, device_id_type=MESH
    )


def vmem_specs(count):
    return [pl.BlockSpec(memory_space=pltpu.VMEM)] * count


def entry_barrier(devices):
    barrier = pltpu.get_barrier_semaphore()
    for device in devices:
        pl.semaphore_signal(barrier, inc=1, device_id=device, device_id_type=MESH)
    pl.semaphore_wait(barrier, len(devices))


def relative(s, j):
    half = j // 2
    return ((s // 2 + 1 - half) % 2) * 2 + (s % 2 + half + j) % 2


def prep_kernel(n, cond_ref, small_ref, ada_ref, rows_ref, small_all, mod_ref,
                crecv, msend, mrecv, c_s, c_r, b_s, b_r, m_s, m_r):
    f = lax.axis_index("fsdp")
    layers, rows, _ = ada_ref.shape
    others = [{"fsdp": (f + k) % n} for k in range(1, n)]
    entry_barrier(others)
    first, second = [], []
    for k in range(1, n):
        to = (f + k) % n
        first.append(rcopy(cond_ref.at[to], crecv.at[f], c_s.at[k], c_r.at[k], {"fsdp": to}))
        first[-1].start()
    for k in range(1, n):
        to = (f + k) % n
        second.append(rcopy(small_ref, small_all.at[f], b_s.at[k], b_r.at[k], {"fsdp": to}))
        second[-1].start()
    crecv[f] = cond_ref[f]
    small_all[f] = small_ref[...]
    for k in range(1, n):
        at = (f - k + n) % n
        rcopy(cond_ref.at[at], crecv.at[at], c_s.at[k], c_r.at[k], {"fsdp": at}).wait_recv()
    cond_rows = jnp.sum(crecv[...], axis=1)
    rows_ref[...] = cond_rows
    cond_rows = cond_rows[:, :rows].astype(BF16)
    for l in range(layers):
        part = mm(cond_rows, ada_ref[l])
        for i in range(n):
            msend[i, l: l + 1, :] = part[i: i + 1, :]
    third = []
    for k in range(1, n):
        to = (f + k) % n
        third.append(rcopy(msend.at[to], mrecv.at[f], m_s.at[k], m_r.at[k], {"fsdp": to}))
        third[-1].start()
    mrecv[f] = msend[f]
    for k in range(1, n):
        at = (f - k + n) % n
        rcopy(msend.at[at], mrecv.at[at], m_s.at[k], m_r.at[k], {"fsdp": at}).wait_recv()
    mod_ref[...] = jnp.sum(mrecv[...], axis=0)
    for k in range(1, n):
        at = (f - k + n) % n
        rcopy(small_ref, small_all.at[at], b_s.at[k], b_r.at[k], {"fsdp": at}).wait_recv()
    for copy in first + second + third:
        copy.wait_send()


def prep(n, cond_blocks, small, ada_weight):
    layers, rows, width6 = ada_weight.shape
    lanes = cond_blocks.shape[-1]
    return pl.pallas_call(
        functools.partial(prep_kernel, n),
        out_shape=(
            jax.ShapeDtypeStruct((n, lanes), F32),
            jax.ShapeDtypeStruct((n,) + small.shape, F32),
            jax.ShapeDtypeStruct((layers, width6), F32),
        ),
        in_specs=vmem_specs(3),
        out_specs=tuple(vmem_specs(3)),
        scratch_shapes=[
            pltpu.VMEM((n, 8, lanes), F32),
            pltpu.VMEM((n, layers, width6), F32),
            pltpu.VMEM((n, layers, width6), F32),
        ] + [pltpu.SemaphoreType.DMA((n,))] * 6,
        compiler_params=pltpu.CompilerParams(collective_id=0, has_side_effects=True),
    )(cond_blocks, small, ada_weight)


def forward_kernel(n, *refs):
    (x_ref, mod_ref, bq_ref, bo_ref, bu_ref, bd_ref, sq_ref, so_ref, su_ref, sd_ref,
     out_ref, wq_ref, wo_ref, wu_ref, wd_ref, xs_ref, attn_ref, qh_ref, tok_ref, branch_ref,
     mid_ref, mlp_ref, up_ref, feed_ref,
     osend, psend, precv, xsend, xrecv, own_feed,
     z_s, z_r, y_s, y_r, a_s, a_r, t_s, t_r, g_s, g_r, r_s, r_r) = refs
    f = lax.axis_index("fsdp")
    s = lax.axis_index("seq")
    slow = n // FAST
    a, b = f // FAST, f % FAST
    layers, rows = sq_ref.shape[0], sq_ref.shape[1]
    block = x_ref.shape[0]
    width = x_ref.shape[1]
    hc = sq_ref.shape[2] // 3
    heads = hc // HEAD_DIM
    shards = (sq_ref, so_ref, su_ref, sd_ref)
    full = (wq_ref, wo_ref, wu_ref, wd_ref)
    across, diagonal, partner = relative(s, 0), relative(s, 1), relative(s, 2)
    y_dev = {"fsdp": a * FAST + (1 - b)}

    entry_barrier(
        [{"fsdp": ((a + k) % slow) * FAST + b} for k in range(1, slow)] + [y_dev]
        + [{"seq": across}, {"seq": diagonal}, {"seq": partner}]
    )

    def z_copy(l, p, k, to):
        return rcopy(shards[p].at[l], full[p].at[l, f], z_s.at[l, p, k], z_r.at[l, p, k], {"fsdp": to})

    def y_copy(l, p, k):
        at = ((a - k + slow) % slow) * FAST + b
        src = shards[p].at[l] if k == 0 else full[p].at[l, at]
        return rcopy(src, full[p].at[l, at], y_s.at[l, p, k], y_r.at[l, p, k], y_dev)

    for l in range(layers):
        for p in range(4):
            y_copy(l, p, 0).start()
            for k in range(1, slow):
                z_copy(l, p, k, ((a + k) % slow) * FAST + b).start()

    def forward_weights(l, p):
        for k in range(1, slow):
            at = ((a - k + slow) % slow) * FAST + b
            rcopy(shards[p].at[l], full[p].at[l, at], z_s.at[l, p, k], z_r.at[l, p, k], {"fsdp": at}).wait_recv()
            y_copy(l, p, k).start()

    def ready(l, p):
        for k in range(slow):
            at = ((a - k + slow) % slow) * FAST + 1 - b
            rcopy(shards[p].at[l], full[p].at[l, at], y_s.at[l, p, k], y_r.at[l, p, k], y_dev).wait_recv()

    xs_ref[0] = x_ref[...].astype(F32)
    for l in range(layers):
        for p in range(4):
            full[p][l, f] = shards[p][l]

    def matrix(ref, l):
        return ref[l].reshape(n * rows, ref.shape[3])

    def gather(buf, l, send, recv, visit):
        mine = buf.at[l, s]
        to_partner = rcopy(mine, mine, send.at[0], recv.at[0], {"seq": partner})
        to_across = rcopy(mine, mine, send.at[1], recv.at[1], {"seq": across})
        to_across.start()
        to_partner.start()
        theirs = buf.at[l, across]
        relay = rcopy(theirs, theirs, send.at[2], recv.at[2], {"seq": partner})

        def step(i, carry):
            @pl.when(i == 1)
            def _():
                ref = buf.at[l, partner]
                rcopy(ref, ref, send.at[0], recv.at[0], {"seq": partner}).wait_recv()

            @pl.when(i == 2)
            def _():
                rcopy(theirs, theirs, send.at[1], recv.at[1], {"seq": across}).wait_recv()
                relay.start()

            @pl.when(i == 3)
            def _():
                ref = buf.at[l, diagonal]
                rcopy(ref, ref, send.at[2], recv.at[2], {"seq": partner}).wait_recv()

            visit(i, relative(s, pick(i)))
            return carry

        lax.fori_loop(0, 4, step, 0)
        for copy in (to_partner, to_across, relay):
            copy.wait_send()

    def pick(i):
        return (3 - i) * (1 - i // 2) + (i - 2) * (i // 2)

    def layer(l, carry):
        row = lambda i: mod_ref[l, i: i + 1, :]
        x = xs_ref[l]
        normed, _ = normalize(x)
        attn_ref[l, s] = (normed * (1.0 + row(1)) + row(0)).astype(BF16)

        @pl.when(l == 0)
        def _():
            forward_weights(0, 0)

        def qkv_block(i, t):
            @pl.when(i == 0)
            def _():
                ready(l, 0)

            val = (mm(attn_ref[l, t], matrix(wq_ref, l)) + bq_ref[l]).astype(BF16)
            for h in range(3 * heads):
                qh_ref[l, h, pl.ds(pl.multiple_of(t * block, block), block), :] = (
                    val[:, h * HEAD_DIM: (h + 1) * HEAD_DIM]
                )

        gather(attn_ref, l, a_s, a_r, qkv_block)
        forward_weights(l, 1)

        def attend_block(j, carry):
            t = relative(s, j)
            outs = []
            for h in range(heads):
                q = qh_ref[l, h, pl.ds(pl.multiple_of(t * block, block), block), :]
                scores = mm_nt(q, qh_ref[l, heads + h]) * SCORE_SCALE
                e = jnp.exp(scores)
                inverse = 1.0 / jnp.sum(e, axis=-1, keepdims=True)
                prob = (e * inverse).astype(BF16)
                outs.append(mm(prob, qh_ref[l, 2 * heads + h]))
            osend[j] = jnp.concatenate(outs, axis=1).astype(BF16)

            @pl.when(j < 3)
            def _():
                rcopy(osend.at[j], tok_ref.at[l, s], t_s.at[j], t_r.at[j], {"seq": t}).start()

            @pl.when(j == 1)
            def _():
                forward_weights(l, 2)

            return carry

        lax.fori_loop(0, 4, attend_block, 0)
        tok_ref[l, s] = osend[3]
        forward_weights(l, 3)
        ready(l, 1)
        for j in range(3):
            t = relative(s, j)
            rcopy(osend.at[j], tok_ref.at[l, t], t_s.at[j], t_r.at[j], {"seq": t}).wait_recv()
        tokens_out = jnp.concatenate([tok_ref[l, t] for t in range(4)], axis=1)
        branch = mm(tokens_out, matrix(wo_ref, l)) + bo_ref[l]
        branch_ref[l] = branch
        middle = xs_ref[l] + row(2) * branch
        mid_ref[l] = middle
        normed, _ = normalize(middle)
        mlp_ref[l, s] = (normed * (1.0 + row(4)) + row(3)).astype(BF16)

        def mlp_block(i, t):
            @pl.when(i == 0)
            def _():
                ready(l, 2)
                ready(l, 3)

            up = mm(mlp_ref[l, t], matrix(wu_ref, l)) + bu_ref[l]
            up_ref[l, t] = up
            act = gelu_parts(up)[0].astype(BF16)
            part = mm(act, matrix(wd_ref, l))

            @pl.when(i == 0)
            def _():
                own_feed[...] = part

            @pl.when(i == 1)
            def _():
                psend[0] = part
                rcopy(psend.at[0], precv.at[0], r_s.at[0], r_r.at[0], {"seq": partner}).start()

            @pl.when(i == 2)
            def _():
                xsend[...] = part

            @pl.when(i == 3)
            def _():
                psend[1] = part
                rcopy(psend.at[1], precv.at[1], r_s.at[1], r_r.at[1], {"seq": partner}).start()

            @pl.when((i == 1) & (l + 1 < layers))
            def _():
                forward_weights(1, 0)

        gather(mlp_ref, l, g_s, g_r, mlp_block)
        rcopy(psend.at[1], precv.at[1], r_s.at[1], r_r.at[1], {"seq": partner}).wait_recv()
        xsend[...] = xsend[...] + precv[1]
        over = rcopy(xsend, xrecv, r_s.at[2], r_r.at[2], {"seq": across})
        over.start()
        rcopy(psend.at[0], precv.at[0], r_s.at[0], r_r.at[0], {"seq": partner}).wait_recv()
        own_feed[...] = own_feed[...] + precv[0] + bd_ref[l]
        over.wait_recv()
        feed = own_feed[...] + xrecv[...]
        feed_ref[l] = feed
        nxt = mid_ref[l] + row(5) * feed

        @pl.when(l + 1 < layers)
        def _():
            xs_ref[1] = nxt

        @pl.when(l + 1 == layers)
        def _():
            out_ref[...] = nxt.astype(BF16)

        over.wait_send()
        for i in range(2):
            rcopy(psend.at[i], precv.at[i], r_s.at[i], r_r.at[i], {"seq": partner}).wait_send()
        for j in range(3):
            rcopy(osend.at[j], tok_ref.at[l, s], t_s.at[j], t_r.at[j], {"seq": relative(s, j)}).wait_send()
        return carry

    lax.fori_loop(0, layers, layer, 0)
    for l in range(layers):
        for p in range(4):
            y_copy(l, p, 0).wait_send()
            for k in range(1, slow):
                z_copy(l, p, k, ((a + k) % slow) * FAST + b).wait_send()
                y_copy(l, p, k).wait_send()


def forward(n, x, mod, bq, bo, bu, bd, sq, so, su, sd):
    layers, rows, qc = sq.shape
    block, width = x.shape
    hc = qc // 3
    nh = qc // HEAD_DIM
    uc = su.shape[2]
    total = 4 * block
    sds = jax.ShapeDtypeStruct
    outs = (
        sds((block, width), BF16),
        sds((layers, n, rows, qc), BF16),
        sds((layers, n, rows, width), BF16),
        sds((layers, n, rows, uc), BF16),
        sds((layers, n, rows, width), BF16),
        sds((layers, block, width), F32),
        sds((layers, 4, block, width), BF16),
        sds((layers, nh, total, HEAD_DIM), BF16),
        sds((layers, 4, block, hc), BF16),
        sds((layers, block, width), F32),
        sds((layers, block, width), F32),
        sds((layers, 4, block, width), BF16),
        sds((layers, 4, block, uc), F32),
        sds((layers, block, width), F32),
    )
    slow = n // FAST
    dma = pltpu.SemaphoreType.DMA
    scratch = [
        pltpu.VMEM((4, block, hc), BF16),
        pltpu.VMEM((2, block, width), F32),
        pltpu.VMEM((2, block, width), F32),
        pltpu.VMEM((block, width), F32),
        pltpu.VMEM((block, width), F32),
        pltpu.VMEM((block, width), F32),
    ] + [dma((layers, 4, slow))] * 4 + [dma((3,))] * 8
    return pl.pallas_call(
        functools.partial(forward_kernel, n),
        out_shape=outs,
        in_specs=vmem_specs(10),
        out_specs=tuple(vmem_specs(len(outs))),
        scratch_shapes=scratch,
        compiler_params=pltpu.CompilerParams(
            collective_id=1, has_side_effects=True, vmem_limit_bytes=VMEM_LIMIT
        ),
    )(x, mod, bq, bo, bu, bd, sq, so, su, sd)


def backward_kernel(n, *refs):
    (cot_ref, mod_ref), rest = refs[:2], refs[2:]
    stored, rest = rest[:13], rest[13:]
    (g_ref, dmod_ref, gob_ref, gdb_ref, gub_ref, gqb_ref), rest = rest[:6], rest[6:]
    fin, rest = rest[:4], rest[4:]
    loaded, rest = rest[:13], rest[13:]
    grads, rest = rest[:4], rest[4:]
    y_in, rest = rest[:4], rest[4:]
    z_out, rest = rest[:4], rest[4:]
    z_in, rest = rest[:4], rest[4:]
    kept, rest = rest[:4], rest[4:]
    (gf_ref, act_ref, gup_ref, gosend, go_ref, goh_ref, gqh_ref, gqkv_ref, psend, precv, xsend, xrecv,
     own_part, gmid_ref, dk_acc, dv_acc,
     l_s, y_s, y_r, z_s, z_r, f_s, f_r, g_s, g_r, t_s, t_r, r_s, r_r) = rest
    wq, wo, wu, wd, xs, attn, qh, tok, branch, mid, mlp, up, feed = range(13)
    down, upw, outw, qkvw = range(4)
    f = lax.axis_index("fsdp")
    s = lax.axis_index("seq")
    slow = n // FAST
    a, b = f // FAST, f % FAST
    layers = mod_ref.shape[0]
    block, width = cot_ref.shape
    rows = width // n
    hc = gosend.shape[2]
    heads = hc // HEAD_DIM
    across, diagonal, partner = relative(s, 0), relative(s, 1), relative(s, 2)
    y_dev = {"fsdp": a * FAST + (1 - b)}

    def load(i, l):
        return pltpu.make_async_copy(stored[i].at[l], loaded[i], l_s.at[i])

    for i in (feed, wd, up, wu, mlp, mid, branch, wo, tok, qh, wq, attn, xs):
        load(i, layers - 1).start()

    entry_barrier(
        [{"fsdp": ((a + k) % slow) * FAST + b} for k in range(1, slow)] + [y_dev]
        + [{"seq": across}, {"seq": diagonal}, {"seq": partner}]
    )

    def y_copy(l, p):
        return rcopy(grads[p].at[:, 1 - b], y_in[p].at[l], y_s.at[p], y_r.at[l, p], y_dev)

    def z_copy(l, p, k):
        to = (a + k) % slow
        return rcopy(z_out[p].at[to], z_in[p].at[l, k - 1], z_s.at[p, k], z_r.at[l, p, k], {"fsdp": to * FAST + b})

    def z_start(l, p):
        y_copy(l, p).wait_recv()
        for i in range(slow):
            z_out[p][i] = (grads[p][i, b].astype(F32) + y_in[p][l, i].astype(F32)).astype(BF16)
        kept[p][...] = grads[p][a, b].astype(F32) + y_in[p][l, a].astype(F32)
        for k in range(1, slow):
            z_copy(l, p, k).start()
        y_copy(l, p).wait_send()

    def fin_copy(l, p, i):
        mine, theirs = fin[p].at[l, s], fin[p].at[l, across]
        ref = theirs if i == 2 else mine
        return rcopy(ref, ref, f_s.at[l, p, i], f_r.at[l, p, i], {"seq": across if i == 1 else partner})

    def z_finish(l, p):
        total = kept[p][...]
        for k in range(1, slow):
            z_copy(l, p, k).wait_recv()
            total = total + z_in[p][l, k - 1].astype(F32)
        fin[p][l, s] = total.astype(BF16)
        fin_copy(l, p, 1).start()
        fin_copy(l, p, 0).start()
        for k in range(1, slow):
            z_copy(l, p, k).wait_send()

    def fin_arrived(l, p, i):
        ref = fin[p].at[l, (partner, across, diagonal)[i]]
        rcopy(ref, ref, f_s.at[l, p, i], f_r.at[l, p, i], {"seq": partner}).wait_recv()

    def matrix(i):
        return loaded[i][...].reshape(width, loaded[i].shape[2])

    def part_copy(i):
        return rcopy(psend.at[i], precv.at[i], r_s.at[i], r_r.at[i], {"seq": partner})

    over = rcopy(xsend, xrecv, r_s.at[2], r_r.at[2], {"seq": across})

    def place(j, part):
        @pl.when(j == 3)
        def _():
            own_part[...] = part

        @pl.when(j == 2)
        def _():
            psend[0] = part
            part_copy(0).start()

        @pl.when(j == 0)
        def _():
            xsend[...] = part

        @pl.when(j == 1)
        def _():
            psend[1] = part
            part_copy(1).start()

    def send_across():
        part_copy(1).wait_recv()
        xsend[...] = xsend[...] + precv[1]
        over.start()

    def collect():
        part_copy(0).wait_recv()
        own_part[...] = own_part[...] + precv[0]
        over.wait_recv()
        own_part[...] = own_part[...] + xrecv[...]
        over.wait_send()
        part_copy(0).wait_send()
        part_copy(1).wait_send()

    def sums(value):
        return jnp.sum(value, axis=0, keepdims=True)

    def layer(step, carry):
        l = layers - 1 - step
        row = lambda i: mod_ref[l, i: i + 1, :]

        @pl.when(step == 0)
        def _():
            g_ref[...] = cot_ref[...].astype(F32)

        load(feed, l).wait()
        g = g_ref[...]
        g_feed = (row(5) * g).astype(BF16)
        gf_ref[s] = g_feed
        mine, theirs = gf_ref.at[s], gf_ref.at[across]
        to_partner = rcopy(mine, mine, g_s.at[0], g_r.at[0], {"seq": partner})
        to_across = rcopy(mine, mine, g_s.at[1], g_r.at[1], {"seq": across})
        relay = rcopy(theirs, theirs, g_s.at[2], g_r.at[2], {"seq": partner})
        to_across.start()
        to_partner.start()
        dmod_ref[l, 5:6, :] = sums(g * loaded[feed][...])
        gdb_ref[l] = sums(g_feed.astype(F32))
        gub_ref[l] = jnp.zeros((1, gub_ref.shape[2]), F32)
        for i in (wd, up, wu, mlp):
            load(i, l).wait()

        def mlp_block(i, carry):
            @pl.when(i == 1)
            def _():
                ref = gf_ref.at[partner]
                rcopy(ref, ref, g_s.at[0], g_r.at[0], {"seq": partner}).wait_recv()

            @pl.when(i == 2)
            def _():
                rcopy(theirs, theirs, g_s.at[1], g_r.at[1], {"seq": across}).wait_recv()
                relay.start()

            @pl.when(i == 3)
            def _():
                ref = gf_ref.at[diagonal]
                rcopy(ref, ref, g_s.at[2], g_r.at[2], {"seq": partner}).wait_recv()

            j = (3 - i) * (1 - i // 2) + (i - 2) * (i // 2)
            t = relative(s, j)
            value, slope = gelu_parts(loaded[up][t])
            act_ref[t] = value.astype(BF16)
            g_up = (mm_nt(gf_ref[t], matrix(wd)) * slope).astype(BF16)
            gup_ref[t] = g_up
            gub_ref[l] = gub_ref[l] + sums(g_up.astype(F32))
            place(j, mm_nt(g_up, matrix(wu)))
            return carry

        lax.fori_loop(0, 4, mlp_block, 0)
        for copy in (to_partner, to_across, relay):
            copy.wait_send()
        send_across()

        @pl.when(step > 0)
        def _():
            z_start(l + 1, qkvw)
            z_finish(l + 1, outw)

        whole = lambda ref: ref[...].reshape(4 * block, ref.shape[2])
        grads[down][...] = mm_tn(whole(act_ref), whole(gf_ref)).astype(BF16).reshape(grads[down].shape)
        y_copy(l, down).start()
        grads[upw][...] = mm_tn(whole(loaded[mlp]), whole(gup_ref)).astype(BF16).reshape(grads[upw].shape)
        y_copy(l, upw).start()

        @pl.when(l > 0)
        def _():
            for i in (feed, wd, up, wu, mlp):
                load(i, l - 1).start()

        load(mid, l).wait()
        normed, inverse = normalize(loaded[mid][...])
        for i in (branch, wo, tok):
            load(i, l).wait()
        collect()
        g_min = own_part[...]
        dmod_ref[l, 4:5, :] = sums(g_min * normed)
        dmod_ref[l, 3:4, :] = sums(g_min)
        g_mid = g_ref[...] + norm_back(g_min * (1.0 + row(4)), normed, inverse)
        gmid_ref[...] = g_mid
        g_branch = (row(2) * g_mid).astype(BF16)
        dmod_ref[l, 2:3, :] = sums(g_mid * loaded[branch][...])
        gob_ref[l] = sums(g_branch.astype(F32))
        g_o = mm_nt(g_branch, matrix(wo)).astype(BF16)
        for t in range(4):
            gosend[t] = g_o[:, t * hc: (t + 1) * hc]

        def head_copy(j):
            t = relative(s, j)
            return rcopy(gosend.at[t], go_ref.at[s], t_s.at[j], t_r.at[j], {"seq": t})

        for j in range(3):
            head_copy(j).start()
        go_ref[s] = gosend[s]
        tokens_out = jnp.concatenate([loaded[tok][t] for t in range(4)], axis=1)
        grads[outw][...] = mm_tn(tokens_out, g_branch).astype(BF16).reshape(grads[outw].shape)
        y_copy(l, outw).start()

        @pl.when(l > 0)
        def _():
            for i in (mid, branch, wo, tok):
                load(i, l - 1).start()

        @pl.when(step > 0)
        def _():
            z_finish(l + 1, qkvw)

        load(qh, l).wait()
        for j in range(3):
            t = relative(s, j)
            rcopy(gosend.at[t], go_ref.at[t], t_s.at[j], t_r.at[j], {"seq": t}).wait_recv()
        for t in range(4):
            part = go_ref[t]
            for h in range(heads):
                goh_ref[h, t * block: (t + 1) * block, :] = part[:, h * HEAD_DIM: (h + 1) * HEAD_DIM]

        for h in range(heads):
            dk_acc[...] = jnp.zeros_like(dk_acc)
            dv_acc[...] = jnp.zeros_like(dv_acc)

            def tile(t, carry):
                at = pl.ds(pl.multiple_of(t * block, block), block)
                q = loaded[qh][h, at, :]
                k = loaded[qh][heads + h]
                g_out = goh_ref[h, at, :]
                e = jnp.exp(mm_nt(q, k) * SCORE_SCALE)
                prob = e * (1.0 / jnp.sum(e, axis=-1, keepdims=True))
                dv_acc[...] = dv_acc[...] + mm_tn(prob.astype(BF16), g_out)
                dp = mm_nt(g_out, loaded[qh][2 * heads + h])
                inner = jnp.sum(prob * dp, axis=-1, keepdims=True)
                ds = (prob * (dp - inner)).astype(BF16)
                gqh_ref[h, at, :] = (mm(ds, k) * SCORE_SCALE).astype(BF16)
                dk_acc[...] = dk_acc[...] + mm_tn(ds, q)
                return carry

            lax.fori_loop(0, 4, tile, 0)
            gqh_ref[heads + h] = (dk_acc[...] * SCORE_SCALE).astype(BF16)
            gqh_ref[2 * heads + h] = dv_acc[...].astype(BF16)
            if h < 2:
                z_start(l, h)

        for j in range(3):
            head_copy(j).wait_send()

        @pl.when(l > 0)
        def _():
            load(qh, l - 1).start()

        for t in range(4):
            gqkv_ref[t] = jnp.concatenate(
                [gqh_ref[i, t * block: (t + 1) * block, :] for i in range(3 * heads)], axis=1
            )
        load(wq, l).wait()

        def back_block(i, carry):
            j = (1 - i) * (1 - i // 2) + i * (i // 2)
            place(j, mm_nt(gqkv_ref[relative(s, j)], matrix(wq)))
            return carry

        lax.fori_loop(0, 4, back_block, 0)
        send_across()
        load(attn, l).wait()
        grads[qkvw][...] = mm_tn(whole(loaded[attn]), whole(gqkv_ref)).astype(BF16).reshape(grads[qkvw].shape)
        y_copy(l, qkvw).start()
        gqb_ref[l] = sums(whole(gqkv_ref).astype(F32))
        z_start(l, outw)
        z_finish(l, down)
        z_finish(l, upw)
        load(xs, l).wait()
        normed, inverse = normalize(loaded[xs][...])

        @pl.when(l > 0)
        def _():
            for i in (wq, attn, xs):
                load(i, l - 1).start()

        collect()
        g_ain = own_part[...]
        dmod_ref[l, 1:2, :] = sums(g_ain * normed)
        dmod_ref[l, 0:1, :] = sums(g_ain)
        g_ref[...] = gmid_ref[...] + norm_back(g_ain * (1.0 + row(1)), normed, inverse)
        return carry

    lax.fori_loop(0, layers, layer, 0)
    z_start(0, qkvw)
    z_finish(0, outw)
    z_finish(0, qkvw)
    for l in reversed(range(layers)):
        for p in (down, upw, outw, qkvw):
            fin_arrived(l, p, 1)
            fin_copy(l, p, 2).start()
    for l in range(layers):
        for p in range(4):
            fin_arrived(l, p, 0)
            fin_arrived(l, p, 2)
            for i in range(3):
                fin_copy(l, p, i).wait_send()


def backward(n, cot, mod, stored):
    layers = mod.shape[0]
    block, width = cot.shape
    rows = width // n
    slow = n // FAST
    qc = stored[0].shape[3]
    uc = stored[2].shape[3]
    hc = qc // 3
    nh = qc // HEAD_DIM
    sds = jax.ShapeDtypeStruct
    dma = pltpu.SemaphoreType.DMA
    columns = (width, uc, width, qc)
    outs = [
        sds((block, width), F32),
        sds((layers, 6, width), F32),
        sds((layers, 1, width), F32),
        sds((layers, 1, width), F32),
        sds((layers, 1, uc), F32),
        sds((layers, 1, qc), F32),
    ] + [sds((layers, 4, rows, c), BF16) for c in columns]
    scratch = (
        [pltpu.VMEM(x.shape[1:], x.dtype) for x in stored]
        + [pltpu.VMEM((slow, FAST, rows, c), BF16) for c in columns]
        + [pltpu.VMEM((layers, slow, rows, c), BF16) for c in columns]
        + [pltpu.VMEM((slow, rows, c), BF16) for c in columns]
        + [pltpu.VMEM((layers, slow - 1, rows, c), BF16) for c in columns]
        + [pltpu.VMEM((rows, c), F32) for c in columns]
        + [
            pltpu.VMEM((4, block, width), BF16),
            pltpu.VMEM((4, block, uc), BF16),
            pltpu.VMEM((4, block, uc), BF16),
            pltpu.VMEM((4, block, hc), BF16),
            pltpu.VMEM((4, block, hc), BF16),
            pltpu.VMEM((nh // 3, 4 * block, HEAD_DIM), BF16),
            pltpu.VMEM((nh, 4 * block, HEAD_DIM), BF16),
            pltpu.VMEM((4, block, qc), BF16),
            pltpu.VMEM((2, block, width), F32),
            pltpu.VMEM((2, block, width), F32),
            pltpu.VMEM((block, width), F32),
            pltpu.VMEM((block, width), F32),
            pltpu.VMEM((block, width), F32),
            pltpu.VMEM((block, width), F32),
            pltpu.VMEM((4 * block, HEAD_DIM), F32),
            pltpu.VMEM((4 * block, HEAD_DIM), F32),
            dma((13,)),
            dma((4,)), dma((layers, 4)),
            dma((4, slow)), dma((layers, 4, slow)),
            dma((layers, 4, 3)), dma((layers, 4, 3)),
        ]
        + [dma((3,))] * 6
    )
    return pl.pallas_call(
        functools.partial(backward_kernel, n),
        out_shape=tuple(outs),
        in_specs=vmem_specs(2) + [pl.BlockSpec(memory_space=pl.ANY)] * 13,
        out_specs=tuple(vmem_specs(len(outs))),
        scratch_shapes=scratch,
        compiler_params=pltpu.CompilerParams(
            collective_id=2, has_side_effects=True, vmem_limit_bytes=VMEM_LIMIT
        ),
    )(cot, mod, *stored)


def tail_kernel(n, sum_ref, cat_ref, sums_all, cats_all, s_in, c_all, s_tot,
                a_s, a_r, b_s, b_r, c_s, c_r, d_s, d_r):
    f = lax.axis_index("fsdp")
    s = lax.axis_index("seq")
    entry_barrier([{"seq": relative(s, j)} for j in range(3)] + [{"fsdp": (f + k) % n} for k in range(1, n)])
    sends = []
    for j in range(3):
        t = relative(s, j)
        sends.append(rcopy(sum_ref, s_in.at[s], a_s.at[j], a_r.at[j], {"seq": t}))
        sends[-1].start()
        sends.append(rcopy(cat_ref, c_all.at[s], b_s.at[j], b_r.at[j], {"seq": t}))
        sends[-1].start()
    s_in[s] = sum_ref[...]
    c_all[s] = cat_ref[...]
    for j in range(3):
        t = relative(s, j)
        rcopy(sum_ref, s_in.at[t], a_s.at[j], a_r.at[j], {"seq": t}).wait_recv()
        rcopy(cat_ref, c_all.at[t], b_s.at[j], b_r.at[j], {"seq": t}).wait_recv()
    s_tot[...] = jnp.sum(s_in[...], axis=0)
    sums_all[f] = s_tot[...]
    cats_all[f] = c_all[...]
    for k in range(1, n):
        to = {"fsdp": (f + k) % n}
        sends.append(rcopy(s_tot, sums_all.at[f], c_s.at[k], c_r.at[k], to))
        sends[-1].start()
        sends.append(rcopy(c_all, cats_all.at[f], d_s.at[k], d_r.at[k], to))
        sends[-1].start()
    for k in range(1, n):
        at = (f - k + n) % n
        rcopy(s_tot, sums_all.at[at], c_s.at[k], c_r.at[k], {"fsdp": at}).wait_recv()
        rcopy(c_all, cats_all.at[at], d_s.at[k], d_r.at[k], {"fsdp": at}).wait_recv()
    for copy in sends:
        copy.wait_send()


def tail(n, sums, cats):
    sds = jax.ShapeDtypeStruct
    dma = pltpu.SemaphoreType.DMA
    return pl.pallas_call(
        functools.partial(tail_kernel, n),
        out_shape=(sds((n,) + sums.shape, F32), sds((n, 4) + cats.shape, F32)),
        in_specs=vmem_specs(2),
        out_specs=tuple(vmem_specs(2)),
        scratch_shapes=[
            pltpu.VMEM((4,) + sums.shape, F32), pltpu.VMEM((4,) + cats.shape, F32), pltpu.VMEM(sums.shape, F32),
        ] + [dma((3,))] * 4 + [dma((n,))] * 4,
        compiler_params=pltpu.CompilerParams(collective_id=3, has_side_effects=True),
    )(sums, cats)


def fused_device(
    tokens, condition, ada_weight, ada_bias, qkv_weight, qv_bias, out_weight, out_bias,
    up_weight, up_bias, down_weight, down_bias, cotangent,
):
    n = lax.axis_size("fsdp")
    ns = lax.axis_size("seq")
    f = lax.axis_index("fsdp")
    s = lax.axis_index("seq")
    layers, rows, width6 = ada_weight.shape
    width = rows * n
    ff = up_weight.shape[2]
    hc = width // ns
    fc = ff // (ns * n)

    def take(x, axis):
        return lax.dynamic_index_in_dim(x, s, axis, keepdims=False)

    def own(x, axis, size):
        return lax.dynamic_slice_in_dim(x, f * size, size, axis)

    fw = n * fc
    s_q = take(qkv_weight.reshape(layers, rows, 3, ns, hc), 3).reshape(layers, rows, 3 * hc)
    s_u = take(up_weight.reshape(layers, rows, n, ns, fc), 3).reshape(layers, rows, fw)
    s_d = take(down_weight.reshape(layers, ns, fc, width), 1)

    cond_float = condition.astype(F32)
    cond_act = jax.nn.silu(cond_float).astype(BF16)
    cond_blocks = jnp.pad(cond_act.astype(F32).reshape(n, 1, rows), ((0, 0), (0, 7), (0, -rows % 128)))
    small = jnp.concatenate(
        [ada_bias.reshape(-1), qv_bias.reshape(-1), out_bias.reshape(-1), up_bias.reshape(-1),
         down_bias.reshape(-1)]
    ).astype(F32).reshape(8, -1)
    cond_rows, small, mod = prep(n, cond_blocks, small, ada_weight)
    cond_rows = cond_rows[:, :rows]
    small = small.reshape(n, -1)
    pos = 0

    def unpack(per_layer):
        nonlocal pos
        part = small[:, pos: pos + layers * per_layer].reshape(n, layers, per_layer)
        pos += layers * per_layer
        return part.transpose(1, 0, 2).reshape(layers, n * per_layer)

    ada_b = unpack(ada_bias.shape[1])
    qv_b = unpack(qv_bias.shape[1])
    out_b = unpack(out_bias.shape[1])
    up_b = unpack(up_bias.shape[1])
    down_b = unpack(down_bias.shape[1])
    q_b = take(qv_b[:, :width].reshape(layers, ns, hc), 1)
    v_b = take(qv_b[:, width:].reshape(layers, ns, hc), 1)
    qkv_b = jnp.concatenate([q_b, jnp.zeros_like(q_b), v_b], axis=1)
    up_bs = take(up_b.reshape(layers, n, ns, fc), 2).reshape(layers, fw)
    mod = mod + ada_b

    (block_out, w_q, w_o, w_u, w_d, xs, attn, qh, tok, branches, mids, mlp, ups, feeds) = forward(
        n, tokens[0], mod.reshape(layers, 6, width), qkv_b[:, None], out_b[:, None], up_bs[:, None],
        down_b[:, None], s_q, out_weight, s_u, s_d)
    (g, d_mod, g_ob, g_db, g_ub, g_qb, grad_down, grad_up, grad_out, grad_qkv) = backward(
        n, cotangent[0], mod.reshape(layers, 6, width),
        (w_q, w_o, w_u, w_d, xs, attn, qh, tok, branches, mids, mlp, ups, feeds))
    grad_up = grad_up.reshape(layers, ns, rows, n, fc).transpose(0, 2, 3, 1, 4).reshape(layers, rows, ff).astype(F32)
    grad_down = grad_down.reshape(layers, ns * fc, width).astype(F32)
    grad_qkv = grad_qkv.reshape(layers, ns, rows, 3, hc).transpose(0, 2, 3, 1, 4)
    grad_qkv = grad_qkv.reshape(layers, rows, 3 * width).astype(F32)
    grad_out = jnp.sum(grad_out.astype(F32), axis=1)

    sums = jnp.concatenate([d_mod.reshape(-1), g_ob.reshape(-1), g_db.reshape(-1)])
    g_qvb = jnp.concatenate([g_qb[:, 0, :hc], g_qb[:, 0, 2 * hc:]], axis=1)
    cats = jnp.concatenate([g_ub.reshape(-1), g_qvb.reshape(-1)])
    sums_all, cats_all = tail(n, sums.reshape(8, -1), cats.reshape(8, -1))
    sums_all = sums_all.reshape(n, -1)
    d_mod_all = sums_all[:, : layers * width6].reshape(n, layers, width6)
    g_bias = jnp.sum(sums_all[:, layers * width6:], axis=0).reshape(2, layers, n, rows)
    g_bias = lax.dynamic_index_in_dim(g_bias, f, 2, keepdims=False)
    cats_all = jnp.sum(cats_all.reshape(n, ns, -1), axis=0)
    g_ub = cats_all[:, : layers * fw].reshape(ns, layers, n, fc)
    g_ub = lax.dynamic_index_in_dim(g_ub, f, 2, keepdims=False).transpose(1, 0, 2).reshape(layers, ns * fc)
    g_qvb = cats_all[:, layers * fw:].reshape(ns, layers, 2, hc).transpose(1, 2, 0, 3).reshape(layers, -1)
    g_qvb = own(g_qvb, 1, qv_bias.shape[1])

    grad_ada = jnp.stack([
        lax.dot_general(cond_rows, d_mod_all[:, l], (((0,), (0,)), ((), ())), precision=HIGHEST,
                        preferred_element_type=F32) for l in range(layers)])
    grad_ada_bias = own(jnp.sum(d_mod_all, axis=0), 1, width6 // n)
    g_cond = sum(
        lax.dot_general(d_mod_all[:, l], ada_weight[l].astype(F32), (((1,), (1,)), ((), ())),
                        precision=HIGHEST, preferred_element_type=F32) for l in range(layers))
    g_cond = lax.all_to_all(g_cond, "fsdp", split_axis=0, concat_axis=1, tiled=True)
    _, silu_back = jax.vjp(jax.nn.silu, cond_float)
    grad_condition = silu_back(g_cond)[0]
    return (
        block_out[None], g[None], grad_condition, grad_ada, grad_ada_bias, grad_qkv, g_qvb,
        grad_out, g_bias[0], grad_up, g_ub, grad_down, g_bias[1],
    )


def solution(mesh):
    token = P("fsdp", "seq", None)
    matrix = P(None, "fsdp", None)
    vector = P(None, "fsdp")

    def per_device(*args):
        rows = args[2].shape[1]
        fits = rows % 32 == 0 and mesh.shape["seq"] == 4 and args[0].shape[0] == 1
        return (fused_device if fits else plain_device)(*args)

    return jax.shard_map(
        per_device,
        mesh=mesh,
        in_specs=(token, P("fsdp", None)) + (matrix, vector) * 5 + (token,),
        out_specs=(token, token, P("fsdp", None)) + (matrix, vector) * 5,
        check_vma=False,
    )
```

```python
import functools

import jax
import jax.numpy as jnp
from jax import lax
from jax.experimental import pallas as pl
from jax.experimental.pallas import tpu as pltpu
from jax.sharding import PartitionSpec as P

HEAD_DIM = 64
SCORE_SCALE = HEAD_DIM ** (-0.5)
EPSILON = 1e-06
HIGHEST = lax.Precision.HIGHEST
F32 = jnp.float32
BF16 = jnp.bfloat16


def normalize(values):
    centred = values - jnp.mean(values, axis=-1, keepdims=True)
    inverse = lax.rsqrt(jnp.mean(centred * centred, axis=-1, keepdims=True) + EPSILON)
    return centred * inverse, inverse


def norm_back(gradient, normed, inverse):
    return inverse * (
        gradient
        - jnp.mean(gradient, axis=-1, keepdims=True)
        - normed * jnp.mean(gradient * normed, axis=-1, keepdims=True)
    )


def mm(a, b):
    return lax.dot_general(a, b, (((1,), (0,)), ((), ())), preferred_element_type=F32)


def mm_nt(a, b):
    return lax.dot_general(a, b, (((1,), (1,)), ((), ())), preferred_element_type=F32)


def mm_tn(a, b):
    return lax.dot_general(a, b, (((0,), (0,)), ((), ())), preferred_element_type=F32)


def split_heads(rows):
    return rows.reshape(rows.shape[0], -1, HEAD_DIM).transpose(1, 0, 2)


def join_heads(heads):
    return heads.transpose(1, 0, 2).reshape(heads.shape[1], -1)


def attend(q, k, v):
    q, k, v = split_heads(q), split_heads(k), split_heads(v)
    scores = jnp.einsum("hqd,hkd->hqk", q, k, preferred_element_type=F32) * SCORE_SCALE
    logsum = jnp.log(jnp.sum(jnp.exp(scores), axis=-1, keepdims=True))
    prob = jnp.exp(scores - logsum).astype(BF16)
    out = jnp.einsum("hqk,hkd->hqd", prob, v, preferred_element_type=F32)
    return join_heads(out).astype(BF16), logsum


def attend_back(q, k, v, logsum, out_grad):
    q, k, v, out_grad = split_heads(q), split_heads(k), split_heads(v), split_heads(out_grad)
    scores = jnp.einsum("hqd,hkd->hqk", q, k, preferred_element_type=F32) * SCORE_SCALE
    prob = jnp.exp(scores - logsum)
    dv = jnp.einsum("hqk,hqd->hkd", prob.astype(BF16), out_grad, preferred_element_type=F32)
    dp = jnp.einsum("hqd,hkd->hqk", out_grad, v, preferred_element_type=F32)
    inner = jnp.sum(prob * dp, axis=-1, keepdims=True)
    ds = (prob * (dp - inner)).astype(BF16)
    dq = jnp.einsum("hqk,hkd->hqd", ds, k, preferred_element_type=F32) * SCORE_SCALE
    dk = jnp.einsum("hqk,hqd->hkd", ds, q, preferred_element_type=F32) * SCORE_SCALE
    return [join_heads(t).astype(BF16) for t in (dq, dk, dv)]


def gelu_parts(u):
    c = 0.7978845608028654
    inner = c * (u + 0.044715 * (u * u * u))
    t = jnp.tanh(inner)
    value = 0.5 * u * (1.0 + t)
    slope = 0.5 * (1.0 + t) + 0.5 * u * (1.0 - t * t) * (c * (1.0 + 3.0 * 0.044715 * u * u))
    return value, slope


def plain_device(
    tokens, condition, ada_weight, ada_bias, qkv_weight, qv_bias, out_weight, out_bias,
    up_weight, up_bias, down_weight, down_bias, cotangent,
):
    n = lax.axis_size("fsdp")
    ns = lax.axis_size("seq")
    f = lax.axis_index("fsdp")
    s = lax.axis_index("seq")
    layers, rows, width6 = ada_weight.shape
    width = rows * n
    ff = up_weight.shape[2]
    hc = width // ns
    fc = ff // (ns * n)

    def take(x, axis):
        return lax.dynamic_index_in_dim(x, s, axis, keepdims=False)

    def own(x, axis, size):
        return lax.dynamic_slice_in_dim(x, f * size, size, axis)

    w_qkv, w_rest = [], []
    for l in range(layers):
        q_part = take(qkv_weight[l].reshape(rows, 3, ns, hc), 2).reshape(rows, 3 * hc)
        u_part = take(up_weight[l].reshape(rows, n, ns, fc), 2).reshape(rows, n * fc)
        d_part = take(down_weight[l].reshape(ns, fc, width), 0)
        w_qkv.append(lax.all_gather(q_part, "fsdp", axis=0, tiled=True))
        rest = jnp.concatenate([u_part, d_part, out_weight[l]], axis=1)
        w_rest.append(lax.all_gather(rest, "fsdp", axis=0, tiled=True))
    fw = n * fc

    cond_float = condition.astype(F32)
    cond_act = jax.nn.silu(cond_float).astype(BF16)
    small = jnp.concatenate(
        [ada_bias.reshape(-1), qv_bias.reshape(-1), out_bias.reshape(-1), up_bias.reshape(-1),
         down_bias.reshape(-1), cond_act.reshape(-1)]
    )
    small = lax.all_gather(small, "fsdp", axis=0, tiled=False)
    pos = 0

    def unpack(per_layer):
        nonlocal pos
        part = small[:, pos: pos + layers * per_layer].reshape(n, layers, per_layer)
        pos += layers * per_layer
        return part.transpose(1, 0, 2).reshape(layers, n * per_layer)

    ada_b = unpack(ada_bias.shape[1]).astype(F32)
    qv_b = unpack(qv_bias.shape[1]).astype(F32)
    out_b = unpack(out_bias.shape[1]).astype(F32)
    up_b = unpack(up_bias.shape[1]).astype(F32)
    down_b = unpack(down_bias.shape[1]).astype(F32)
    cond_all = small[:, pos:]
    cond_rows = own(cond_all, 1, rows)
    q_b = take(qv_b[:, :width].reshape(layers, ns, hc), 1)
    v_b = take(qv_b[:, width:].reshape(layers, ns, hc), 1)
    qkv_b = jnp.concatenate([q_b, jnp.zeros_like(q_b), v_b], axis=1)
    up_bs = take(up_b.reshape(layers, n, ns, fc), 2).reshape(layers, fw)

    mod_partial = jnp.stack([mm(cond_rows, ada_weight[l]) for l in range(layers)], axis=1)
    mod = lax.psum_scatter(mod_partial, "fsdp", scatter_dimension=0, tiled=True)[0] + ada_b

    hidden = tokens[0].astype(F32)
    saved = []
    for l in range(layers):
        shift_a, scale_a, gate_a, shift_m, scale_m, gate_m = jnp.split(mod[l], 6)
        n_a, r_a = normalize(hidden)
        attn_in = (n_a * (1.0 + scale_a) + shift_a).astype(BF16)
        attn_all = lax.all_gather(attn_in, "seq", axis=0, tiled=True)
        qkv = (mm(attn_all, w_qkv[l]) + qkv_b[l]).astype(BF16)
        q, k, v = qkv[:, :hc], qkv[:, hc: 2 * hc], qkv[:, 2 * hc:]
        head_out, logsum = attend(q, k, v)
        tok_out = lax.all_to_all(head_out, "seq", split_axis=0, concat_axis=1, tiled=True)
        branch = mm(tok_out, w_rest[l][:, fw + width:]) + out_b[l]
        middle = hidden + gate_a * branch
        n_m, r_m = normalize(middle)
        mlp_in = (n_m * (1.0 + scale_m) + shift_m).astype(BF16)
        mlp_all = lax.all_gather(mlp_in, "seq", axis=0, tiled=True)
        up = mm(mlp_all, w_rest[l][:, :fw]) + up_bs[l]
        act = gelu_parts(up)[0].astype(BF16)
        feed = mm(act, w_rest[l][:, fw: fw + width])
        feed = lax.psum_scatter(feed, "seq", scatter_dimension=0, tiled=True) + down_b[l]
        saved.append((n_a, r_a, attn_all, q, k, v, logsum, tok_out, branch, n_m, r_m, mlp_all, up, act, feed))
        hidden = middle + gate_m * feed
    block_out = hidden.astype(BF16)

    g = cotangent[0].astype(F32)
    d_mods = [None] * layers
    reduced = [None] * layers
    bias_grads = [None] * layers
    for l in reversed(range(layers)):
        shift_a, scale_a, gate_a, shift_m, scale_m, gate_m = jnp.split(mod[l], 6)
        n_a, r_a, attn_all, q, k, v, logsum, tok_out, branch, n_m, r_m, mlp_all, up, act, feed = saved[l]
        g_feed = (gate_m * g).astype(BF16)
        d_gate_m = jnp.sum(g * feed, axis=0)
        g_feed_all = lax.all_gather(g_feed, "seq", axis=0, tiled=True)
        grad_down = mm_tn(act, g_feed_all)
        g_up = (mm_nt(g_feed_all, w_rest[l][:, fw: fw + width]) * gelu_parts(up)[1]).astype(BF16)
        grad_up = mm_tn(mlp_all, g_up)
        g_min = lax.psum_scatter(mm_nt(g_up, w_rest[l][:, :fw]), "seq", scatter_dimension=0, tiled=True)
        d_scale_m = jnp.sum(g_min * n_m, axis=0)
        d_shift_m = jnp.sum(g_min, axis=0)
        g_mid = g + norm_back(g_min * (1.0 + scale_m), n_m, r_m)
        g_branch = (gate_a * g_mid).astype(BF16)
        d_gate_a = jnp.sum(g_mid * branch, axis=0)
        grad_out = mm_tn(tok_out, g_branch)
        g_o = mm_nt(g_branch, w_rest[l][:, fw + width:]).astype(BF16)
        g_o_heads = lax.all_to_all(g_o, "seq", split_axis=1, concat_axis=0, tiled=True)
        dq, dk, dv = attend_back(q, k, v, logsum, g_o_heads)
        g_qkv = jnp.concatenate([dq, dk, dv], axis=1)
        grad_qkv = mm_tn(attn_all, g_qkv)
        g_ain = lax.psum_scatter(mm_nt(g_qkv, w_qkv[l]), "seq", scatter_dimension=0, tiled=True)
        d_scale_a = jnp.sum(g_ain * n_a, axis=0)
        d_shift_a = jnp.sum(g_ain, axis=0)
        g = g_mid + norm_back(g_ain * (1.0 + scale_a), n_a, r_a)
        d_mods[l] = jnp.concatenate([d_shift_a, d_scale_a, d_gate_a, d_shift_m, d_scale_m, d_gate_m])
        packed = jnp.concatenate([grad_up, grad_down, grad_out, grad_qkv], axis=1).astype(BF16)
        reduced[l] = lax.psum_scatter(packed, "fsdp", scatter_dimension=0, tiled=True)

        def place(x, axis):
            zeros = jnp.zeros(x.shape[:axis] + (ns,) + x.shape[axis + 1:], F32)
            return lax.dynamic_update_slice_in_dim(zeros, x, s, axis)

        qv_g = place(jnp.stack([jnp.sum(dq.astype(F32), axis=0), jnp.sum(dv.astype(F32), axis=0)])[:, None, :], 1)
        up_g = place(jnp.sum(g_up.astype(F32), axis=0).reshape(n, 1, fc), 1)
        bias_grads[l] = jnp.concatenate([
            qv_g.reshape(n, -1), jnp.sum(g_branch.astype(F32), axis=0).reshape(n, -1),
            up_g.reshape(n, -1), jnp.sum(g_feed.astype(F32), axis=0).reshape(n, -1)], axis=1)

    red = jnp.stack(reduced)
    shared = jnp.concatenate([red[:, :, : fw + width], red[:, :, fw + 2 * width:]], axis=2)
    shared = lax.all_gather(shared, "seq", axis=0, tiled=False).astype(F32)
    grad_up = shared[..., :fw].reshape(ns, layers, rows, n, fc).transpose(1, 2, 3, 0, 4).reshape(layers, rows, ff)
    grad_down = shared[..., fw: fw + width].transpose(1, 0, 2, 3).reshape(layers, ns * fc, width)
    grad_qkv = shared[..., fw + width:].reshape(ns, layers, rows, 3, hc).transpose(1, 2, 3, 0, 4)
    grad_qkv = grad_qkv.reshape(layers, rows, 3 * width)
    grad_out = lax.psum(red[:, :, fw + width: fw + 2 * width], "seq").astype(F32)

    bias = lax.psum(jnp.stack(bias_grads), ("fsdp", "seq"))
    bias = lax.dynamic_index_in_dim(bias, f, 1, keepdims=False)
    cuts = [qv_bias.shape[1], out_bias.shape[1], up_bias.shape[1], down_bias.shape[1]]
    grad_bias, at = [], 0
    for size in cuts:
        grad_bias.append(bias[:, at: at + size])
        at += size

    d_mod = lax.psum(jnp.stack(d_mods), "seq")
    d_mod_all = lax.all_gather(d_mod, "fsdp", axis=0, tiled=False)
    cond_rows32 = cond_rows.astype(F32)
    grad_ada = jnp.stack([
        lax.dot_general(cond_rows32, d_mod_all[:, l], (((0,), (0,)), ((), ())), precision=HIGHEST,
                        preferred_element_type=F32) for l in range(layers)])
    grad_ada_bias = own(jnp.sum(d_mod_all, axis=0), 1, width6 // n)
    g_cond = sum(
        lax.dot_general(d_mod_all[:, l], ada_weight[l].astype(F32), (((1,), (1,)), ((), ())),
                        precision=HIGHEST, preferred_element_type=F32) for l in range(layers))
    g_cond = lax.all_to_all(g_cond, "fsdp", split_axis=0, concat_axis=1, tiled=True)
    _, silu_back = jax.vjp(jax.nn.silu, cond_float)
    grad_condition = silu_back(g_cond)[0]
    return (
        block_out[None], g[None], grad_condition, grad_ada, grad_ada_bias, grad_qkv, grad_bias[0],
        grad_out, grad_bias[1], grad_up, grad_bias[2], grad_down, grad_bias[3],
    )


MESH = pl.DeviceIdType.MESH
FAST = 2
VMEM_LIMIT = 66_000_000


def rcopy(src, dst, send, recv, device):
    return pltpu.make_async_remote_copy(
        src_ref=src, dst_ref=dst, send_sem=send, recv_sem=recv, device_id=device, device_id_type=MESH
    )


def vmem_specs(count):
    return [pl.BlockSpec(memory_space=pltpu.VMEM)] * count


def entry_barrier(devices):
    barrier = pltpu.get_barrier_semaphore()
    for device in devices:
        pl.semaphore_signal(barrier, inc=1, device_id=device, device_id_type=MESH)
    pl.semaphore_wait(barrier, len(devices))


def relative(s, j):
    half = j // 2
    return ((s // 2 + 1 - half) % 2) * 2 + (s % 2 + half + j) % 2


def forward_kernel(n, *refs):
    (x_ref, cond_ref, ada_ref, adab_ref, qkvw_ref, qvb_ref, outw_ref, outb_ref, upw_ref, upb_ref,
     downw_ref, downb_ref,
     out_ref, mod_ref, rows_ref, wq_ref, wo_ref, wu_ref, wd_ref, xs_ref, attn_ref, qh_ref, tok_ref, branch_ref,
     mid_ref, mlp_ref, up_ref, feed_ref,
     osend, psend, precv, xpart, xsend, xrecv, own_feed,
     sq_ref, so_ref, su_ref, bq_ref, bo_ref, bu_ref, bd_ref, cblock, crecv, bsend, brecv, msend, mrecv,
     c_s, c_r, b_s, b_r, m_s, m_r, w_s, w_r, z_s, z_r, y_s, y_r, a_s, a_r, t_s, t_r, g_s, g_r, r_s, r_r) = refs
    f = lax.axis_index("fsdp")
    s = lax.axis_index("seq")
    slow = n // FAST
    a, b = f // FAST, f % FAST
    layers, rows = qkvw_ref.shape[0], qkvw_ref.shape[1]
    block = x_ref.shape[0]
    width = x_ref.shape[1]
    hc = sq_ref.shape[2] // 3
    heads = hc // HEAD_DIM
    fc = su_ref.shape[2] // n
    chunk = downw_ref.shape[1] // 4
    core = s % 2
    across, diagonal, partner = relative(s, 0), relative(s, 1), relative(s, 2)
    y_dev = {"fsdp": a * FAST + (1 - b)}

    def place(l, p, at):
        if p == 1:
            return wo_ref.at[l, core, at]
        return (wq_ref, None, wu_ref, wd_ref)[p].at[l, at]

    entry_barrier(
        [{"fsdp": (f + k) % n} for k in range(1, n)] + [{"seq": across}, {"seq": diagonal}, {"seq": partner}]
    )

    cond = cond_ref[...].astype(F32)
    act = cond / (1.0 + jnp.exp(-cond))
    act = act.astype(BF16).astype(F32)
    cblock[...] = jnp.zeros_like(cblock)
    for i in range(n):
        cblock[i, 0:1, :rows] = act[:, i * rows: (i + 1) * rows]
    crecv[f] = cblock[f]
    for k in range(1, n):
        to = (f + k) % n
        rcopy(cblock.at[to], crecv.at[f], c_s.at[k], c_r.at[k], {"fsdp": to}).start()
    for l in range(layers):
        bsend[l: l + 1, :] = jnp.concatenate(
            [r[l: l + 1, :].astype(F32) for r in (adab_ref, outb_ref, downb_ref)], axis=1
        )
        bsend[layers + l: layers + l + 1, : hc + 4 * fc] = jnp.concatenate(
            [r[l: l + 1, :].astype(F32) for r in (qvb_ref, upb_ref)], axis=1
        )
    brecv[f] = bsend[...]

    def shard(l, p):
        if p == 3:
            return downw_ref.at[l, pl.ds(pl.multiple_of(s * chunk, chunk), chunk)]
        return (sq_ref, so_ref, su_ref)[p].at[l]

    for i in range(4):
        @pl.when(s == i)
        def _():
            for l in range(layers):
                sq_ref[l] = jnp.concatenate(
                    [qkvw_ref[l, :, j * width + i * hc: j * width + (i + 1) * hc] for j in range(3)], axis=1
                )
                so_ref[l] = outw_ref[l, :, (i % 2) * (width // 2): (i % 2 + 1) * (width // 2)]
                su_ref[l] = jnp.concatenate(
                    [upw_ref[l, :, (4 * j + i) * fc: (4 * j + i + 1) * fc] for j in range(n)], axis=1
                )

    def z_copy(l, p, k, to):
        return rcopy(shard(l, p), place(l, p, f), z_s.at[l, p, k], z_r.at[l, p, k], {"fsdp": to})

    def y_copy(l, p, k):
        at = ((a - k + slow) % slow) * FAST + b
        src = shard(l, p) if k == 0 else place(l, p, at)
        return rcopy(src, place(l, p, at), y_s.at[l, p, k], y_r.at[l, p, k], y_dev)

    def launch(l, p):
        y_copy(l, p, 0).start()
        for k in range(1, slow):
            z_copy(l, p, k, ((a + k) % slow) * FAST + b).start()

    launch(0, 0)
    for k in range(1, n):
        to = (f + k) % n
        rcopy(bsend, brecv.at[f], b_s.at[k], b_r.at[k], {"fsdp": to}).start()

    for k in range(1, n):
        at = (f - k + n) % n
        rcopy(cblock.at[at], crecv.at[at], c_s.at[k], c_r.at[k], {"fsdp": at}).wait_recv()
    cond_rows = jnp.sum(crecv[...], axis=1)
    rows_ref[...] = cond_rows
    cond_rows = cond_rows[:, :rows].astype(BF16)
    for l in range(layers):
        part = mm(cond_rows, ada_ref[l])
        for i in range(n):
            msend[i, l: l + 1, :] = part[i: i + 1, :]
    mrecv[f] = msend[f]
    for k in range(1, n):
        to = (f + k) % n
        rcopy(msend.at[to], mrecv.at[f], m_s.at[k], m_r.at[k], {"fsdp": to}).start()
    for l in range(layers):
        for p in range(4):
            if l + p > 0:
                launch(l, p)

    def forward_weights(l, p):
        for k in range(1, slow):
            at = ((a - k + slow) % slow) * FAST + b
            rcopy(shard(l, p), place(l, p, at), z_s.at[l, p, k], z_r.at[l, p, k], {"fsdp": at}).wait_recv()
            y_copy(l, p, k).start()

    def ready(l, p):
        for k in range(slow):
            at = ((a - k + slow) % slow) * FAST + 1 - b
            rcopy(shard(l, p), place(l, p, at), y_s.at[l, p, k], y_r.at[l, p, k], y_dev).wait_recv()

    xs_ref[0] = x_ref[...].astype(F32)
    for k in range(1, n):
        at = (f - k + n) % n
        rcopy(bsend, brecv.at[at], b_s.at[k], b_r.at[k], {"fsdp": at}).wait_recv()
    ac = adab_ref.shape[1]
    for l in range(layers):
        gathered = lambda lo, size, r=l: jnp.concatenate([brecv[i, r: r + 1, lo: lo + size] for i in range(n)], axis=1)
        bo_ref[l] = gathered(ac, rows)
        bd_ref[l] = gathered(ac + rows, rows)
        q_b, v_b = brecv[s, layers + l: layers + l + 1, :hc], brecv[4 + s, layers + l: layers + l + 1, :hc]
        bq_ref[l] = jnp.concatenate([q_b, jnp.zeros_like(q_b), v_b], axis=1)
    for i in range(4):
        @pl.when(s == i)
        def _():
            for l in range(layers):
                lo = hc + i * fc
                bu_ref[l] = jnp.concatenate(
                    [brecv[j, layers + l: layers + l + 1, lo: lo + fc] for j in range(n)], axis=1
                )
    for k in range(1, n):
        at = (f - k + n) % n
        rcopy(msend.at[at], mrecv.at[at], m_s.at[k], m_r.at[k], {"fsdp": at}).wait_recv()
    mod = jnp.sum(mrecv[...], axis=0)
    for l in range(layers):
        full = mod[l: l + 1] + jnp.concatenate([brecv[i, l: l + 1, :ac] for i in range(n)], axis=1)
        for r in range(6):
            mod_ref[l, r: r + 1, :] = full[:, r * width: (r + 1) * width]
    for l in range(layers):
        for p in range(4):
            place(l, p, f)[...] = shard(l, p)[...]

    def matrix(ref, l):
        return ref[l].reshape(n * rows, ref.shape[3])

    def half_copy(l):
        ref = wo_ref.at[l, core]
        return rcopy(ref, ref, w_s.at[l], w_r.at[l], {"seq": partner})

    def half_arrived(l):
        ref = wo_ref.at[l, 1 - core]
        rcopy(ref, ref, w_s.at[l], w_r.at[l], {"seq": partner}).wait_recv()

    def gather(buf, l, send, recv, visit):
        mine = buf.at[l, s]
        to_partner = rcopy(mine, mine, send.at[0], recv.at[0], {"seq": partner})
        to_across = rcopy(mine, mine, send.at[1], recv.at[1], {"seq": across})
        to_across.start()
        to_partner.start()
        theirs = buf.at[l, across]
        relay = rcopy(theirs, theirs, send.at[2], recv.at[2], {"seq": partner})

        def step(i, carry):
            @pl.when(i == 1)
            def _():
                ref = buf.at[l, partner]
                rcopy(ref, ref, send.at[0], recv.at[0], {"seq": partner}).wait_recv()

            @pl.when(i == 2)
            def _():
                rcopy(theirs, theirs, send.at[1], recv.at[1], {"seq": across}).wait_recv()
                relay.start()

            @pl.when(i == 3)
            def _():
                ref = buf.at[l, diagonal]
                rcopy(ref, ref, send.at[2], recv.at[2], {"seq": partner}).wait_recv()

            visit(i, relative(s, pick(i)))
            return carry

        lax.fori_loop(0, 4, step, 0)
        for copy in (to_partner, to_across, relay):
            copy.wait_send()

    def pick(i):
        return (3 - i) * (1 - i // 2) + (i - 2) * (i // 2)

    def layer(l, carry):
        row = lambda i: mod_ref[l, i: i + 1, :]
        x = xs_ref[l]
        normed, _ = normalize(x)
        attn_ref[l, s] = (normed * (1.0 + row(1)) + row(0)).astype(BF16)

        @pl.when(l == 0)
        def _():
            forward_weights(0, 0)

        def qkv_block(i, t):
            @pl.when(i == 0)
            def _():
                ready(l, 0)

            val = (mm(attn_ref[l, t], matrix(wq_ref, l)) + bq_ref[l]).astype(BF16)
            for h in range(3 * heads):
                qh_ref[l, h, pl.ds(pl.multiple_of(t * block, block), block), :] = (
                    val[:, h * HEAD_DIM: (h + 1) * HEAD_DIM]
                )

        gather(attn_ref, l, a_s, a_r, qkv_block)

        @pl.when(l == 0)
        def _():
            forward_weights(0, 1)

        @pl.when(l > 0)
        def _():
            forward_weights(l, 2)

        def attend_block(j, carry):
            t = relative(s, j)
            outs = []
            for h in range(heads):
                q = qh_ref[l, h, pl.ds(pl.multiple_of(t * block, block), block), :]
                scores = mm_nt(q, qh_ref[l, heads + h]) * SCORE_SCALE
                e = jnp.exp(scores)
                inverse = 1.0 / jnp.sum(e, axis=-1, keepdims=True)
                prob = (e * inverse).astype(BF16)
                outs.append(mm(prob, qh_ref[l, 2 * heads + h]))
            osend[j] = jnp.concatenate(outs, axis=1).astype(BF16)

            @pl.when(j < 3)
            def _():
                rcopy(osend.at[j], tok_ref.at[l, s], t_s.at[j], t_r.at[j], {"seq": t}).start()

            @pl.when((j == 1) & (l == 0))
            def _():
                forward_weights(0, 2)

            @pl.when((j == 1) & (l > 0))
            def _():
                forward_weights(l, 3)

            @pl.when(j == 2)
            def _():
                ready(l, 1)
                half_copy(l).start()

            return carry

        lax.fori_loop(0, 4, attend_block, 0)
        tok_ref[l, s] = osend[3]
        for j in range(3):
            t = relative(s, j)
            rcopy(osend.at[j], tok_ref.at[l, t], t_s.at[j], t_r.at[j], {"seq": t}).wait_recv()
        tokens_out = jnp.concatenate([tok_ref[l, t] for t in range(4)], axis=1)
        half_arrived(l)
        branch = jnp.concatenate(
            [mm(tokens_out, wo_ref[l, c].reshape(n * rows, width // 2)) for c in range(2)], axis=1
        ) + bo_ref[l]
        branch_ref[l] = branch
        middle = xs_ref[l] + row(2) * branch
        mid_ref[l] = middle
        normed, _ = normalize(middle)
        mlp_ref[l, s] = (normed * (1.0 + row(4)) + row(3)).astype(BF16)

        def mlp_block(i, t):
            @pl.when((i == 0) & (l == 0))
            def _():
                forward_weights(0, 3)

            @pl.when(i == 0)
            def _():
                ready(l, 2)
                ready(l, 3)

            up = mm(mlp_ref[l, t], matrix(wu_ref, l)) + bu_ref[l]
            up_ref[l, t] = up
            act = gelu_parts(up)[0].astype(BF16)
            part = mm(act, matrix(wd_ref, l))

            @pl.when(i == 0)
            def _():
                own_feed[...] = part

            @pl.when(i == 1)
            def _():
                psend[0] = part
                rcopy(psend.at[0], precv.at[0], r_s.at[0], r_r.at[0], {"seq": partner}).start()

            @pl.when(i == 2)
            def _():
                xpart[...] = part

            @pl.when(i == 3)
            def _():
                psend[1] = part
                rcopy(psend.at[1], precv.at[1], r_s.at[1], r_r.at[1], {"seq": partner}).start()

            @pl.when((i == 2) & (l + 1 < layers))
            def _():
                forward_weights(1, 0)

        gather(mlp_ref, l, g_s, g_r, mlp_block)
        rcopy(psend.at[1], precv.at[1], r_s.at[1], r_r.at[1], {"seq": partner}).wait_recv()
        xsend[...] = (xpart[...] + precv[1]).astype(BF16)
        over = rcopy(xsend, xrecv, r_s.at[2], r_r.at[2], {"seq": across})
        over.start()

        @pl.when(l + 1 < layers)
        def _():
            forward_weights(1, 1)

        rcopy(psend.at[0], precv.at[0], r_s.at[0], r_r.at[0], {"seq": partner}).wait_recv()
        own_feed[...] = own_feed[...] + precv[0] + bd_ref[l]
        over.wait_recv()
        feed = own_feed[...] + xrecv[...].astype(F32)
        feed_ref[l] = feed
        nxt = mid_ref[l] + row(5) * feed

        @pl.when(l + 1 < layers)
        def _():
            xs_ref[1] = nxt

        @pl.when(l + 1 == layers)
        def _():
            out_ref[...] = nxt.astype(BF16)

        over.wait_send()
        half_copy(l).wait_send()
        for i in range(2):
            rcopy(psend.at[i], precv.at[i], r_s.at[i], r_r.at[i], {"seq": partner}).wait_send()
        for j in range(3):
            rcopy(osend.at[j], tok_ref.at[l, s], t_s.at[j], t_r.at[j], {"seq": relative(s, j)}).wait_send()
        return carry

    lax.fori_loop(0, layers, layer, 0)
    for l in range(layers):
        for p in range(4):
            y_copy(l, p, 0).wait_send()
            for k in range(1, slow):
                z_copy(l, p, k, ((a + k) % slow) * FAST + b).wait_send()
                y_copy(l, p, k).wait_send()
    for k in range(1, n):
        to = (f + k) % n
        rcopy(cblock.at[to], crecv.at[f], c_s.at[k], c_r.at[k], {"fsdp": to}).wait_send()
        rcopy(bsend, brecv.at[f], b_s.at[k], b_r.at[k], {"fsdp": to}).wait_send()
        rcopy(msend.at[to], mrecv.at[f], m_s.at[k], m_r.at[k], {"fsdp": to}).wait_send()


def forward(n, x, cond, weights):
    layers, rows, width6 = weights[0].shape
    block, width = x.shape
    qc = weights[2].shape[2] // 4
    hc = qc // 3
    nh = qc // HEAD_DIM
    uc = weights[6].shape[2] // 4
    total = 4 * block
    lanes = rows + -rows % 128
    sds = jax.ShapeDtypeStruct
    outs = (
        sds((block, width), BF16),
        sds((layers, 6, width), F32),
        sds((n, lanes), F32),
        sds((layers, n, rows, qc), BF16),
        sds((layers, 2, n, rows, width // 2), BF16),
        sds((layers, n, rows, uc), BF16),
        sds((layers, n, rows, width), BF16),
        sds((layers, block, width), F32),
        sds((layers, 4, block, width), BF16),
        sds((layers, nh, total, HEAD_DIM), BF16),
        sds((layers, 4, block, hc), BF16),
        sds((layers, block, width), F32),
        sds((layers, block, width), F32),
        sds((layers, 4, block, width), BF16),
        sds((layers, 4, block, uc), F32),
        sds((layers, block, width), F32),
    )
    slow = n // FAST
    dma = pltpu.SemaphoreType.DMA
    scratch = [
        pltpu.VMEM((4, block, hc), BF16),
        pltpu.VMEM((2, block, width), F32),
        pltpu.VMEM((2, block, width), F32),
        pltpu.VMEM((block, width), F32),
        pltpu.VMEM((block, width), BF16),
        pltpu.VMEM((block, width), BF16),
        pltpu.VMEM((block, width), F32),
        pltpu.VMEM((layers, rows, qc), BF16),
        pltpu.VMEM((layers, rows, width // 2), BF16),
        pltpu.VMEM((layers, rows, uc), BF16),
        pltpu.VMEM((layers, 1, qc), F32),
        pltpu.VMEM((layers, 1, width), F32),
        pltpu.VMEM((layers, 1, uc), F32),
        pltpu.VMEM((layers, 1, width), F32),
        pltpu.VMEM((n, 8, lanes), F32),
        pltpu.VMEM((n, 8, lanes), F32),
        pltpu.VMEM((2 * layers, width), F32),
        pltpu.VMEM((n, 2 * layers, width), F32),
        pltpu.VMEM((n, layers, width6), F32),
        pltpu.VMEM((n, layers, width6), F32),
    ] + [dma((n,))] * 6 + [dma((layers,))] * 2 + [dma((layers, 4, slow))] * 4 + [dma((3,))] * 8
    return pl.pallas_call(
        functools.partial(forward_kernel, n),
        out_shape=outs,
        in_specs=vmem_specs(12),
        out_specs=tuple(vmem_specs(len(outs))),
        scratch_shapes=scratch,
        compiler_params=pltpu.CompilerParams(
            collective_id=1, has_side_effects=True, vmem_limit_bytes=VMEM_LIMIT
        ),
    )(x, cond, *weights)


def backward_kernel(n, *refs):
    (cot_ref, mod_ref, ada_ref), rest = refs[:3], refs[3:]
    stored, rest = rest[:13], rest[13:]
    (g_ref, vec_all, cat_all, gcond_ref), rest = rest[:4], rest[4:]
    fin, rest = rest[:4], rest[4:]
    loaded, rest = rest[:13], rest[13:]
    grads, rest = rest[:4], rest[4:]
    y_in, rest = rest[:4], rest[4:]
    z_out, rest = rest[:4], rest[4:]
    z_in, rest = rest[:4], rest[4:]
    kept, rest = rest[:4], rest[4:]
    (gf_ref, act_ref, gup_ref, gosend, go_ref, goh_ref, gqh_ref, gqkv_ref, psend, precv, xpart, xsend, xrecv,
     own_part, gmid_ref, osend, orecv,
     vec_ref, cat_ref, vec_in, vec_sum, cat_in, gc_send, gc_recv, v_s, v_r, u_s, u_r, k_s, k_r, h_s, h_r, i_s, i_r, dk_acc, dv_acc,
     l_s, o_s, o_r, y_s, y_r, z_s, z_r, f_s, f_r, g_s, g_r, t_s, t_r, r_s, r_r) = rest
    wq, wo, wu, wd, xs, attn, qh, tok, branch, mid, mlp, up, feed = range(13)
    down, upw, outw, qkvw = range(4)
    f = lax.axis_index("fsdp")
    s = lax.axis_index("seq")
    slow = n // FAST
    a, b = f // FAST, f % FAST
    layers = mod_ref.shape[0]
    block, width = cot_ref.shape
    rows = width // n
    hc = gosend.shape[2]
    heads = hc // HEAD_DIM
    across, diagonal, partner = relative(s, 0), relative(s, 1), relative(s, 2)
    y_dev = {"fsdp": a * FAST + (1 - b)}

    def load(i, l):
        return pltpu.make_async_copy(stored[i].at[l], loaded[i], l_s.at[i])

    for i in (feed, wd, up, wu, mlp, mid, branch, wo, tok, qh, wq, attn, xs):
        load(i, layers - 1).start()

    entry_barrier(
        [{"fsdp": (f + k) % n} for k in range(1, n)]
        + [{"seq": across}, {"seq": diagonal}, {"seq": partner}]
    )

    def y_copy(l, p):
        return rcopy(grads[p].at[:, 1 - b], y_in[p].at[l], y_s.at[p], y_r.at[l, p], y_dev)

    def z_copy(l, p, k):
        to = (a + k) % slow
        return rcopy(z_out[p].at[to], z_in[p].at[l, k - 1], z_s.at[p, k], z_r.at[l, p, k], {"fsdp": to * FAST + b})

    def z_start(l, p):
        y_copy(l, p).wait_recv()
        for i in range(slow):
            z_out[p][i] = (grads[p][i, b].astype(F32) + y_in[p][l, i].astype(F32)).astype(BF16)
        kept[p][...] = grads[p][a, b].astype(F32) + y_in[p][l, a].astype(F32)
        for k in range(1, slow):
            z_copy(l, p, k).start()
        y_copy(l, p).wait_send()

    def fin_copy(l, p, i):
        mine, theirs = fin[p].at[l, s], fin[p].at[l, across]
        ref = theirs if i == 2 else mine
        return rcopy(ref, ref, f_s.at[l, p, i], f_r.at[l, p, i], {"seq": across if i == 1 else partner})

    def z_finish(l, p):
        total = kept[p][...]
        for k in range(1, slow):
            z_copy(l, p, k).wait_recv()
            total = total + z_in[p][l, k - 1].astype(F32)
        fin[p][l, s] = total.astype(BF16)
        fin_copy(l, p, 1).start()
        fin_copy(l, p, 0).start()
        for k in range(1, slow):
            z_copy(l, p, k).wait_send()

    def fin_arrived(l, p, i):
        ref = fin[p].at[l, (partner, across, diagonal)[i]]
        rcopy(ref, ref, f_s.at[l, p, i], f_r.at[l, p, i], {"seq": partner}).wait_recv()

    def matrix(i):
        return loaded[i][...].reshape(width, loaded[i].shape[2])

    def part_copy(i):
        return rcopy(psend.at[i], precv.at[i], r_s.at[i], r_r.at[i], {"seq": partner})

    over = rcopy(xsend, xrecv, r_s.at[2], r_r.at[2], {"seq": across})

    def place(j, part):
        @pl.when(j == 3)
        def _():
            own_part[...] = part

        @pl.when(j == 2)
        def _():
            psend[0] = part
            part_copy(0).start()

        @pl.when(j == 0)
        def _():
            xpart[...] = part

        @pl.when(j == 1)
        def _():
            psend[1] = part
            part_copy(1).start()

    def send_across():
        part_copy(1).wait_recv()
        xsend[...] = (xpart[...] + precv[1]).astype(BF16)
        over.start()

    def collect():
        part_copy(0).wait_recv()
        own_part[...] = own_part[...] + precv[0]
        over.wait_recv()
        own_part[...] = own_part[...] + xrecv[...].astype(F32)
        over.wait_send()
        part_copy(0).wait_send()
        part_copy(1).wait_send()

    def vec_copy(l, j):
        return rcopy(vec_ref.at[l], vec_in.at[l, s], v_s.at[l, j], v_r.at[l, j], {"seq": relative(s, j)})

    def vec_start(l):
        vec_in[l, s] = vec_ref[l]
        for j in range(3):
            vec_copy(l, j).start()

    def vec_spread(l):
        for j in range(3):
            ref = vec_in.at[l, relative(s, j)]
            rcopy(ref, ref, v_s.at[l, j], v_r.at[l, j], {"seq": relative(s, j)}).wait_recv()
        vec_sum[l] = jnp.sum(vec_in[l], axis=0)
        vec_all[l, f] = vec_sum[l]
        cat_in[l, f] = cat_ref[l]
        for k in range(1, n):
            to = {"fsdp": (f + k) % n}
            rcopy(vec_sum.at[l], vec_all.at[l, f], u_s.at[l, k], u_r.at[l, k], to).start()
            rcopy(cat_ref.at[l], cat_in.at[l, f], k_s.at[l, k], k_r.at[l, k], to).start()

    def vec_arrived(l):
        for k in range(1, n):
            at = (f - k + n) % n
            rcopy(vec_sum.at[l], vec_all.at[l, at], u_s.at[l, k], u_r.at[l, k], {"fsdp": at}).wait_recv()
            rcopy(cat_ref.at[l], cat_in.at[l, at], k_s.at[l, k], k_r.at[l, k], {"fsdp": at}).wait_recv()

    def sums(value):
        return jnp.sum(value, axis=0, keepdims=True)

    def layer(step, carry):
        l = layers - 1 - step
        row = lambda i: mod_ref[l, i: i + 1, :]

        @pl.when(step == 0)
        def _():
            g_ref[...] = cot_ref[...].astype(F32)

        load(feed, l).wait()
        g = g_ref[...]
        g_feed = (row(5) * g).astype(BF16)
        gf_ref[s] = g_feed
        mine, theirs = gf_ref.at[s], gf_ref.at[across]
        to_partner = rcopy(mine, mine, g_s.at[0], g_r.at[0], {"seq": partner})
        to_across = rcopy(mine, mine, g_s.at[1], g_r.at[1], {"seq": across})
        relay = rcopy(theirs, theirs, g_s.at[2], g_r.at[2], {"seq": partner})
        to_across.start()
        to_partner.start()
        vec_ref[l, 5:6, :] = sums(g * loaded[feed][...])
        vec_ref[l, 7:8, :] = sums(g_feed.astype(F32))
        cat_ref[l] = jnp.zeros_like(cat_ref[l])
        for i in (wd, up, wu, mlp):
            load(i, l).wait()

        def mlp_block(i, carry):
            @pl.when(i == 1)
            def _():
                ref = gf_ref.at[partner]
                rcopy(ref, ref, g_s.at[0], g_r.at[0], {"seq": partner}).wait_recv()

            @pl.when(i == 2)
            def _():
                rcopy(theirs, theirs, g_s.at[1], g_r.at[1], {"seq": across}).wait_recv()
                relay.start()

            @pl.when(i == 3)
            def _():
                ref = gf_ref.at[diagonal]
                rcopy(ref, ref, g_s.at[2], g_r.at[2], {"seq": partner}).wait_recv()

            j = (3 - i) * (1 - i // 2) + (i - 2) * (i // 2)
            t = relative(s, j)
            value, slope = gelu_parts(loaded[up][t])
            act_ref[t] = value.astype(BF16)
            g_up = (mm_nt(gf_ref[t], matrix(wd)) * slope).astype(BF16)
            gup_ref[t] = g_up
            cat_ref[l, 0:1, :] = cat_ref[l, 0:1, :] + sums(g_up.astype(F32))
            place(j, mm_nt(g_up, matrix(wu)))
            return carry

        lax.fori_loop(0, 4, mlp_block, 0)
        for copy in (to_partner, to_across, relay):
            copy.wait_send()
        send_across()

        @pl.when(step > 0)
        def _():
            z_start(l + 1, qkvw)
            z_finish(l + 1, outw)

        whole = lambda ref: ref[...].reshape(4 * block, ref.shape[2])
        grads[down][...] = mm_tn(whole(act_ref), whole(gf_ref)).astype(BF16).reshape(grads[down].shape)
        y_copy(l, down).start()
        grads[upw][...] = mm_tn(whole(loaded[mlp]), whole(gup_ref)).astype(BF16).reshape(grads[upw].shape)
        y_copy(l, upw).start()

        @pl.when(l > 0)
        def _():
            for i in (feed, wd, up, wu, mlp):
                load(i, l - 1).start()

        load(mid, l).wait()
        normed, inverse = normalize(loaded[mid][...])
        for i in (branch, wo, tok):
            load(i, l).wait()
        collect()
        g_min = own_part[...]
        vec_ref[l, 4:5, :] = sums(g_min * normed)
        vec_ref[l, 3:4, :] = sums(g_min)
        g_mid = g_ref[...] + norm_back(g_min * (1.0 + row(4)), normed, inverse)
        gmid_ref[...] = g_mid
        g_branch = (row(2) * g_mid).astype(BF16)
        vec_ref[l, 2:3, :] = sums(g_mid * loaded[branch][...])
        vec_ref[l, 6:7, :] = sums(g_branch.astype(F32))
        half = width // 2
        g_o = sum(
            mm_nt(g_branch[:, c * half: (c + 1) * half], loaded[wo][c].reshape(width, half)) for c in range(2)
        ).astype(BF16)
        for t in range(4):
            gosend[t] = g_o[:, t * hc: (t + 1) * hc]

        def head_copy(j):
            t = relative(s, j)
            return rcopy(gosend.at[t], go_ref.at[s], t_s.at[j], t_r.at[j], {"seq": t})

        for j in range(3):
            head_copy(j).start()
        go_ref[s] = gosend[s]
        tokens_out = jnp.concatenate([loaded[tok][t] for t in range(4)], axis=1)
        for c in range(2):
            osend[c] = mm_tn(tokens_out, g_branch[:, c * half: (c + 1) * half]).astype(BF16)
        pair = rcopy(osend.at[1 - s % 2], orecv.at[l], o_s.at[0], o_r.at[l], {"seq": partner})
        pair.start()

        @pl.when(l > 0)
        def _():
            for i in (mid, branch, wo, tok):
                load(i, l - 1).start()

        @pl.when(step > 0)
        def _():
            z_finish(l + 1, qkvw)
            vec_spread(l + 1)

        pair.wait_recv()
        out_sum = osend[s % 2].astype(F32) + orecv[l].astype(F32)
        grads[outw][...] = out_sum.astype(BF16).reshape(grads[outw].shape)
        y_copy(l, outw).start()
        pair.wait_send()
        load(qh, l).wait()
        for j in range(3):
            t = relative(s, j)
            rcopy(gosend.at[t], go_ref.at[t], t_s.at[j], t_r.at[j], {"seq": t}).wait_recv()
        for t in range(4):
            part = go_ref[t]
            for h in range(heads):
                goh_ref[h, t * block: (t + 1) * block, :] = part[:, h * HEAD_DIM: (h + 1) * HEAD_DIM]

        for h in range(heads):
            dk_acc[...] = jnp.zeros_like(dk_acc)
            dv_acc[...] = jnp.zeros_like(dv_acc)

            def tile(t, carry):
                at = pl.ds(pl.multiple_of(t * block, block), block)
                q = loaded[qh][h, at, :]
                k = loaded[qh][heads + h]
                g_out = goh_ref[h, at, :]
                e = jnp.exp(mm_nt(q, k) * SCORE_SCALE)
                prob = e * (1.0 / jnp.sum(e, axis=-1, keepdims=True))
                dv_acc[...] = dv_acc[...] + mm_tn(prob.astype(BF16), g_out)
                dp = mm_nt(g_out, loaded[qh][2 * heads + h])
                inner = jnp.sum(prob * dp, axis=-1, keepdims=True)
                ds = (prob * (dp - inner)).astype(BF16)
                gqh_ref[h, at, :] = (mm(ds, k) * SCORE_SCALE).astype(BF16)
                dk_acc[...] = dk_acc[...] + mm_tn(ds, q)
                return carry

            lax.fori_loop(0, 4, tile, 0)
            gqh_ref[heads + h] = (dk_acc[...] * SCORE_SCALE).astype(BF16)
            gqh_ref[2 * heads + h] = dv_acc[...].astype(BF16)
            if h < 2:
                z_start(l, h)

        for j in range(3):
            head_copy(j).wait_send()

        @pl.when(l > 0)
        def _():
            load(qh, l - 1).start()

        for t in range(4):
            gqkv_ref[t] = jnp.concatenate(
                [gqh_ref[i, t * block: (t + 1) * block, :] for i in range(3 * heads)], axis=1
            )
        load(wq, l).wait()

        def back_block(i, carry):
            j = (1 - i) * (1 - i // 2) + i * (i // 2)
            place(j, mm_nt(gqkv_ref[relative(s, j)], matrix(wq)))
            return carry

        lax.fori_loop(0, 4, back_block, 0)
        send_across()
        load(attn, l).wait()
        grads[qkvw][...] = mm_tn(whole(loaded[attn]), whole(gqkv_ref)).astype(BF16).reshape(grads[qkvw].shape)
        y_copy(l, qkvw).start()
        cat_ref[l, 1:2, : 3 * hc] = sums(whole(gqkv_ref).astype(F32))
        z_start(l, outw)
        z_finish(l, down)
        z_finish(l, upw)
        load(xs, l).wait()
        normed, inverse = normalize(loaded[xs][...])

        @pl.when(l > 0)
        def _():
            for i in (wq, attn, xs):
                load(i, l - 1).start()

        collect()
        g_ain = own_part[...]
        vec_ref[l, 1:2, :] = sums(g_ain * normed)
        vec_ref[l, 0:1, :] = sums(g_ain)
        g_ref[...] = gmid_ref[...] + norm_back(g_ain * (1.0 + row(1)), normed, inverse)

        @pl.when(l > 0)
        def _():
            vec_start(l)

        return carry

    lax.fori_loop(0, layers, layer, 0)
    vec_start(0)
    z_start(0, qkvw)
    z_finish(0, outw)
    vec_spread(0)
    for l in range(1, layers):
        for p in (down, upw, outw, qkvw):
            fin_arrived(l, p, 1)
            fin_copy(l, p, 2).start()
    z_finish(0, qkvw)
    for l in range(layers):
        vec_arrived(l)
        cat_all[l, s] = jnp.sum(cat_in[l], axis=0)
    for j in range(3):
        ref = cat_all.at[:, s]
        rcopy(ref, ref, h_s.at[j], h_r.at[j], {"seq": relative(s, j)}).start()
    g_cond = jnp.zeros((n, rows), F32)
    for l in range(layers):
        for r in range(6):
            d = vec_all[l, :, r, :]
            high = d.astype(BF16)
            low = (d - high.astype(F32)).astype(BF16)
            w = ada_ref[l, :, r * width: (r + 1) * width]
            g_cond = g_cond + mm_nt(high, w) + mm_nt(low, w)
    for i in range(n):
        gc_send[i, 0:1, :rows] = g_cond[i: i + 1, :]

    def cond_copy(k):
        to = (f + k) % n
        return rcopy(gc_send.at[to], gc_recv.at[f], i_s.at[k], i_r.at[k], {"fsdp": to})

    gc_recv[f] = gc_send[f]
    for k in range(1, n):
        cond_copy(k).start()
    for p in (down, upw, outw, qkvw):
        fin_arrived(0, p, 1)
        fin_copy(0, p, 2).start()
    for k in range(1, n):
        at = (f - k + n) % n
        rcopy(gc_send.at[at], gc_recv.at[at], i_s.at[k], i_r.at[k], {"fsdp": at}).wait_recv()
    gcond_ref[...] = jnp.concatenate([gc_recv[i, 0:1, :rows] for i in range(n)], axis=1)
    for j in range(3):
        ref = cat_all.at[:, relative(s, j)]
        rcopy(ref, ref, h_s.at[j], h_r.at[j], {"seq": relative(s, j)}).wait_recv()
    for l in range(layers):
        for p in range(4):
            fin_arrived(l, p, 0)
            fin_arrived(l, p, 2)
            for i in range(3):
                fin_copy(l, p, i).wait_send()
    for k in range(1, n):
        cond_copy(k).wait_send()
        to = {"fsdp": (f + k) % n}
        for l in range(layers):
            rcopy(vec_sum.at[l], vec_all.at[l, f], u_s.at[l, k], u_r.at[l, k], to).wait_send()
            rcopy(cat_ref.at[l], cat_in.at[l, f], k_s.at[l, k], k_r.at[l, k], to).wait_send()
    for j in range(3):
        ref = cat_all.at[:, s]
        rcopy(ref, ref, h_s.at[j], h_r.at[j], {"seq": relative(s, j)}).wait_send()
        for l in range(layers):
            vec_copy(l, j).wait_send()


def backward(n, cot, mod, ada, stored):
    layers = mod.shape[0]
    block, width = cot.shape
    rows = width // n
    slow = n // FAST
    qc = stored[0].shape[3]
    uc = stored[2].shape[3]
    hc = qc // 3
    nh = qc // HEAD_DIM
    sds = jax.ShapeDtypeStruct
    dma = pltpu.SemaphoreType.DMA
    columns = (width, uc, width // 2, qc)
    outs = [
        sds((block, width), F32),
        sds((layers, n, 8, width), F32),
        sds((layers, 4, 2, uc), F32),
        sds((1, width), F32),
    ] + [sds((layers, 4, rows, c), BF16) for c in columns]
    scratch = (
        [pltpu.VMEM(x.shape[1:], x.dtype) for x in stored]
        + [pltpu.VMEM((slow, FAST, rows, c), BF16) for c in columns]
        + [pltpu.VMEM((layers, slow, rows, c), BF16) for c in columns]
        + [pltpu.VMEM((slow, rows, c), BF16) for c in columns]
        + [pltpu.VMEM((layers, slow - 1, rows, c), BF16) for c in columns]
        + [pltpu.VMEM((rows, c), F32) for c in columns]
        + [
            pltpu.VMEM((4, block, width), BF16),
            pltpu.VMEM((4, block, uc), BF16),
            pltpu.VMEM((4, block, uc), BF16),
            pltpu.VMEM((4, block, hc), BF16),
            pltpu.VMEM((4, block, hc), BF16),
            pltpu.VMEM((nh // 3, 4 * block, HEAD_DIM), BF16),
            pltpu.VMEM((nh, 4 * block, HEAD_DIM), BF16),
            pltpu.VMEM((4, block, qc), BF16),
            pltpu.VMEM((2, block, width), F32),
            pltpu.VMEM((2, block, width), F32),
            pltpu.VMEM((block, width), F32),
            pltpu.VMEM((block, width), BF16),
            pltpu.VMEM((block, width), BF16),
            pltpu.VMEM((block, width), F32),
            pltpu.VMEM((block, width), F32),
            pltpu.VMEM((2, width, width // 2), BF16),
            pltpu.VMEM((layers, width, width // 2), BF16),
            pltpu.VMEM((layers, 8, width), F32),
            pltpu.VMEM((layers, 2, uc), F32),
            pltpu.VMEM((layers, 4, 8, width), F32),
            pltpu.VMEM((layers, 8, width), F32),
            pltpu.VMEM((layers, n, 2, uc), F32),
            pltpu.VMEM((n, 8, rows + -rows % 128), F32),
            pltpu.VMEM((n, 8, rows + -rows % 128), F32),
            dma((layers, 3)), dma((layers, 3)),
            dma((layers, n)), dma((layers, n)), dma((layers, n)), dma((layers, n)),
            dma((3,)), dma((3,)), dma((n,)), dma((n,)),
            pltpu.VMEM((4 * block, HEAD_DIM), F32),
            pltpu.VMEM((4 * block, HEAD_DIM), F32),
            dma((13,)), dma((1,)), dma((layers,)),
            dma((4,)), dma((layers, 4)),
            dma((4, slow)), dma((layers, 4, slow)),
            dma((layers, 4, 3)), dma((layers, 4, 3)),
        ]
        + [dma((3,))] * 6
    )
    return pl.pallas_call(
        functools.partial(backward_kernel, n),
        out_shape=tuple(outs),
        in_specs=vmem_specs(3) + [pl.BlockSpec(memory_space=pl.ANY)] * 13,
        out_specs=tuple(vmem_specs(len(outs))),
        scratch_shapes=scratch,
        compiler_params=pltpu.CompilerParams(
            collective_id=2, has_side_effects=True, vmem_limit_bytes=VMEM_LIMIT
        ),
    )(cot, mod, ada, *stored)


def assemble_kernel(n, vec_ref, cat_ref, rows_ref, gcond_ref, cond_ref, fd_ref, fu_ref, fo_ref, fq_ref,
                    gcondition, g_adab, g_qvb, g_ob, g_ub, g_db, g_ada, g_qkv, g_out, g_up, g_down,
                    ada_buf, qkv_buf, out_buf, up_buf, down_buf, sem):
    f = lax.axis_index("fsdp")
    layers, rows = fd_ref.shape[0], fd_ref.shape[2]
    width = rows * n
    hc = fq_ref.shape[3] // 3
    fc = fu_ref.shape[3] // n
    ac = g_adab.shape[1]
    copies = []

    def write(i, l, buf, out):
        copies.append(pltpu.make_async_copy(buf.at[l], out.at[l], sem.at[i, l]))
        copies[-1].start()

    for l in range(layers):
        for t in range(4):
            down_buf[l, t * rows: (t + 1) * rows, :] = fd_ref[l, t].astype(F32)
        write(0, l, down_buf, g_down)
    for l in range(layers):
        for j in range(n):
            up_buf[l, :, 4 * j * fc: 4 * (j + 1) * fc] = jnp.concatenate(
                [fu_ref[l, t, :, j * fc: (j + 1) * fc].astype(F32) for t in range(4)], axis=1
            )
        write(1, l, up_buf, g_up)
    cond_rows = rows_ref[:, :rows].astype(BF16)
    for l in range(layers):
        for r in range(6):
            d = vec_ref[l, :, r, :]
            high = d.astype(BF16)
            low = d - high.astype(F32)
            mid = low.astype(BF16)
            low = (low - mid.astype(F32)).astype(BF16)
            ada_buf[l, :, r * width: (r + 1) * width] = (
                mm_tn(cond_rows, high) + mm_tn(cond_rows, mid) + mm_tn(cond_rows, low)
            )
        write(2, l, ada_buf, g_ada)
    for l in range(layers):
        for j in range(3):
            qkv_buf[l, :, j * width: (j + 1) * width] = jnp.concatenate(
                [fq_ref[l, t, :, j * hc: (j + 1) * hc].astype(F32) for t in range(4)], axis=1
            )
        write(3, l, qkv_buf, g_qkv)
    for l in range(layers):
        for c in range(2):
            out_buf[l, :, c * (width // 2): (c + 1) * (width // 2)] = (
                fo_ref[l, c].astype(F32) + fo_ref[l, 2 + c].astype(F32)
            )
        write(4, l, out_buf, g_out)
    cond = cond_ref[...].astype(F32)
    gate = 1.0 / (1.0 + jnp.exp(-cond))
    gcondition[...] = gcond_ref[...] * (gate * (1.0 + cond * (1.0 - gate)))
    total = [jnp.sum(vec_ref[l], axis=0) for l in range(layers)]
    for i in range(n):
        @pl.when(f == i)
        def _():
            for l in range(layers):
                at = slice(l, l + 1)
                flat = jnp.concatenate([total[l][r: r + 1, :] for r in range(6)], axis=1)
                g_adab[at, :] = flat[:, i * ac: (i + 1) * ac]
                g_ob[at, :] = total[l][6:7, i * rows: (i + 1) * rows]
                g_db[at, :] = total[l][7:8, i * rows: (i + 1) * rows]
                g_ub[at, :] = jnp.concatenate(
                    [cat_ref[l, t, 0:1, i * fc: (i + 1) * fc] for t in range(4)], axis=1
                )
                lo = (i // 4) * 2 * hc
                g_qvb[at, :] = cat_ref[l, i % 4, 1:2, lo: lo + hc]
    for copy in copies:
        copy.wait()


def assemble(n, vec_all, cat_all, cond_rows, g_cond, cond, fins):
    layers, _, rows, width = fins[0].shape
    uc, qc = fins[1].shape[3], fins[3].shape[3]
    sds = jax.ShapeDtypeStruct
    big = [(layers, rows, 6 * width), (layers, rows, 4 * qc), (layers, rows, width),
           (layers, rows, 4 * uc), (layers, 4 * rows, width)]
    small = [(1, width), (layers, 6 * width // n), (layers, 2 * width // n), (layers, rows),
             (layers, 4 * uc // n), (layers, rows)]
    return pl.pallas_call(
        functools.partial(assemble_kernel, n),
        out_shape=tuple(sds(x, F32) for x in small + big),
        in_specs=vmem_specs(9),
        out_specs=tuple(vmem_specs(6) + [pl.BlockSpec(memory_space=pl.ANY)] * 5),
        scratch_shapes=[pltpu.VMEM(x, F32) for x in big] + [pltpu.SemaphoreType.DMA((5, layers))],
        compiler_params=pltpu.CompilerParams(vmem_limit_bytes=VMEM_LIMIT),
    )(vec_all, cat_all, cond_rows, g_cond, cond, *fins)


def fused_device(
    tokens, condition, ada_weight, ada_bias, qkv_weight, qv_bias, out_weight, out_bias,
    up_weight, up_bias, down_weight, down_bias, cotangent,
):
    n = lax.axis_size("fsdp")
    block_out, mod, cond_rows, *stored = forward(
        n, tokens[0], condition,
        (ada_weight, ada_bias, qkv_weight, qv_bias, out_weight, out_bias, up_weight, up_bias, down_weight, down_bias))
    g, vec_all, cat_all, g_cond, *fins = backward(n, cotangent[0], mod, ada_weight, stored)
    (g_condition, g_adab, g_qvb, g_ob, g_ub, g_db, g_ada, g_qkv, g_out, g_up, g_down) = assemble(
        n, vec_all, cat_all, cond_rows, g_cond, condition, fins)
    return (
        block_out[None], g[None], g_condition, g_ada, g_adab, g_qkv, g_qvb, g_out, g_ob, g_up, g_ub, g_down, g_db,
    )


def solution(mesh):
    token = P("fsdp", "seq", None)
    matrix = P(None, "fsdp", None)
    vector = P(None, "fsdp")

    def per_device(*args):
        rows = args[2].shape[1]
        fits = rows % 32 == 0 and mesh.shape["seq"] == 4 and mesh.shape["fsdp"] == 8 and args[0].shape[0] == 1
        return (fused_device if fits else plain_device)(*args)

    return jax.shard_map(
        per_device,
        mesh=mesh,
        in_specs=(token, P("fsdp", None)) + (matrix, vector) * 5 + (token,),
        out_specs=(token, token, P("fsdp", None)) + (matrix, vector) * 5,
        check_vma=False,
    )
```

```python
import functools

import jax
import jax.numpy as jnp
from jax import lax
from jax.experimental import pallas as pl
from jax.experimental.pallas import tpu as pltpu
from jax.sharding import PartitionSpec as P

HEAD_DIM = 64
SCORE_SCALE = HEAD_DIM ** (-0.5)
EPSILON = 1e-06
HIGHEST = lax.Precision.HIGHEST
F32 = jnp.float32
BF16 = jnp.bfloat16


def normalize(values):
    centred = values - jnp.mean(values, axis=-1, keepdims=True)
    inverse = lax.rsqrt(jnp.mean(centred * centred, axis=-1, keepdims=True) + EPSILON)
    return centred * inverse, inverse


def norm_back(gradient, normed, inverse):
    return inverse * (
        gradient
        - jnp.mean(gradient, axis=-1, keepdims=True)
        - normed * jnp.mean(gradient * normed, axis=-1, keepdims=True)
    )


def mm(a, b):
    return lax.dot_general(a, b, (((1,), (0,)), ((), ())), preferred_element_type=F32)


def mm_nt(a, b):
    return lax.dot_general(a, b, (((1,), (1,)), ((), ())), preferred_element_type=F32)


def mm_tn(a, b):
    return lax.dot_general(a, b, (((0,), (0,)), ((), ())), preferred_element_type=F32)


def split_heads(rows):
    return rows.reshape(rows.shape[0], -1, HEAD_DIM).transpose(1, 0, 2)


def join_heads(heads):
    return heads.transpose(1, 0, 2).reshape(heads.shape[1], -1)


def attend(q, k, v):
    q, k, v = split_heads(q), split_heads(k), split_heads(v)
    scores = jnp.einsum("hqd,hkd->hqk", q, k, preferred_element_type=F32) * SCORE_SCALE
    logsum = jnp.log(jnp.sum(jnp.exp(scores), axis=-1, keepdims=True))
    prob = jnp.exp(scores - logsum).astype(BF16)
    out = jnp.einsum("hqk,hkd->hqd", prob, v, preferred_element_type=F32)
    return join_heads(out).astype(BF16), logsum


def attend_back(q, k, v, logsum, out_grad):
    q, k, v, out_grad = split_heads(q), split_heads(k), split_heads(v), split_heads(out_grad)
    scores = jnp.einsum("hqd,hkd->hqk", q, k, preferred_element_type=F32) * SCORE_SCALE
    prob = jnp.exp(scores - logsum)
    dv = jnp.einsum("hqk,hqd->hkd", prob.astype(BF16), out_grad, preferred_element_type=F32)
    dp = jnp.einsum("hqd,hkd->hqk", out_grad, v, preferred_element_type=F32)
    inner = jnp.sum(prob * dp, axis=-1, keepdims=True)
    ds = (prob * (dp - inner)).astype(BF16)
    dq = jnp.einsum("hqk,hkd->hqd", ds, k, preferred_element_type=F32) * SCORE_SCALE
    dk = jnp.einsum("hqk,hqd->hkd", ds, q, preferred_element_type=F32) * SCORE_SCALE
    return [join_heads(t).astype(BF16) for t in (dq, dk, dv)]


def gelu_parts(u):
    c = 0.7978845608028654
    inner = c * (u + 0.044715 * (u * u * u))
    t = jnp.tanh(inner)
    value = 0.5 * u * (1.0 + t)
    slope = 0.5 * (1.0 + t) + 0.5 * u * (1.0 - t * t) * (c * (1.0 + 3.0 * 0.044715 * u * u))
    return value, slope


def plain_device(
    tokens, condition, ada_weight, ada_bias, qkv_weight, qv_bias, out_weight, out_bias,
    up_weight, up_bias, down_weight, down_bias, cotangent,
):
    n = lax.axis_size("fsdp")
    ns = lax.axis_size("seq")
    f = lax.axis_index("fsdp")
    s = lax.axis_index("seq")
    layers, rows, width6 = ada_weight.shape
    width = rows * n
    ff = up_weight.shape[2]
    hc = width // ns
    fc = ff // (ns * n)

    def take(x, axis):
        return lax.dynamic_index_in_dim(x, s, axis, keepdims=False)

    def own(x, axis, size):
        return lax.dynamic_slice_in_dim(x, f * size, size, axis)

    w_qkv, w_rest = [], []
    for l in range(layers):
        q_part = take(qkv_weight[l].reshape(rows, 3, ns, hc), 2).reshape(rows, 3 * hc)
        u_part = take(up_weight[l].reshape(rows, n, ns, fc), 2).reshape(rows, n * fc)
        d_part = take(down_weight[l].reshape(ns, fc, width), 0)
        w_qkv.append(lax.all_gather(q_part, "fsdp", axis=0, tiled=True))
        rest = jnp.concatenate([u_part, d_part, out_weight[l]], axis=1)
        w_rest.append(lax.all_gather(rest, "fsdp", axis=0, tiled=True))
    fw = n * fc

    cond_float = condition.astype(F32)
    cond_act = jax.nn.silu(cond_float).astype(BF16)
    small = jnp.concatenate(
        [ada_bias.reshape(-1), qv_bias.reshape(-1), out_bias.reshape(-1), up_bias.reshape(-1),
         down_bias.reshape(-1), cond_act.reshape(-1)]
    )
    small = lax.all_gather(small, "fsdp", axis=0, tiled=False)
    pos = 0

    def unpack(per_layer):
        nonlocal pos
        part = small[:, pos: pos + layers * per_layer].reshape(n, layers, per_layer)
        pos += layers * per_layer
        return part.transpose(1, 0, 2).reshape(layers, n * per_layer)

    ada_b = unpack(ada_bias.shape[1]).astype(F32)
    qv_b = unpack(qv_bias.shape[1]).astype(F32)
    out_b = unpack(out_bias.shape[1]).astype(F32)
    up_b = unpack(up_bias.shape[1]).astype(F32)
    down_b = unpack(down_bias.shape[1]).astype(F32)
    cond_all = small[:, pos:]
    cond_rows = own(cond_all, 1, rows)
    q_b = take(qv_b[:, :width].reshape(layers, ns, hc), 1)
    v_b = take(qv_b[:, width:].reshape(layers, ns, hc), 1)
    qkv_b = jnp.concatenate([q_b, jnp.zeros_like(q_b), v_b], axis=1)
    up_bs = take(up_b.reshape(layers, n, ns, fc), 2).reshape(layers, fw)

    mod_partial = jnp.stack([mm(cond_rows, ada_weight[l]) for l in range(layers)], axis=1)
    mod = lax.psum_scatter(mod_partial, "fsdp", scatter_dimension=0, tiled=True)[0] + ada_b

    hidden = tokens[0].astype(F32)
    saved = []
    for l in range(layers):
        shift_a, scale_a, gate_a, shift_m, scale_m, gate_m = jnp.split(mod[l], 6)
        n_a, r_a = normalize(hidden)
        attn_in = (n_a * (1.0 + scale_a) + shift_a).astype(BF16)
        attn_all = lax.all_gather(attn_in, "seq", axis=0, tiled=True)
        qkv = (mm(attn_all, w_qkv[l]) + qkv_b[l]).astype(BF16)
        q, k, v = qkv[:, :hc], qkv[:, hc: 2 * hc], qkv[:, 2 * hc:]
        head_out, logsum = attend(q, k, v)
        tok_out = lax.all_to_all(head_out, "seq", split_axis=0, concat_axis=1, tiled=True)
        branch = mm(tok_out, w_rest[l][:, fw + width:]) + out_b[l]
        middle = hidden + gate_a * branch
        n_m, r_m = normalize(middle)
        mlp_in = (n_m * (1.0 + scale_m) + shift_m).astype(BF16)
        mlp_all = lax.all_gather(mlp_in, "seq", axis=0, tiled=True)
        up = mm(mlp_all, w_rest[l][:, :fw]) + up_bs[l]
        act = gelu_parts(up)[0].astype(BF16)
        feed = mm(act, w_rest[l][:, fw: fw + width])
        feed = lax.psum_scatter(feed, "seq", scatter_dimension=0, tiled=True) + down_b[l]
        saved.append((n_a, r_a, attn_all, q, k, v, logsum, tok_out, branch, n_m, r_m, mlp_all, up, act, feed))
        hidden = middle + gate_m * feed
    block_out = hidden.astype(BF16)

    g = cotangent[0].astype(F32)
    d_mods = [None] * layers
    reduced = [None] * layers
    bias_grads = [None] * layers
    for l in reversed(range(layers)):
        shift_a, scale_a, gate_a, shift_m, scale_m, gate_m = jnp.split(mod[l], 6)
        n_a, r_a, attn_all, q, k, v, logsum, tok_out, branch, n_m, r_m, mlp_all, up, act, feed = saved[l]
        g_feed = (gate_m * g).astype(BF16)
        d_gate_m = jnp.sum(g * feed, axis=0)
        g_feed_all = lax.all_gather(g_feed, "seq", axis=0, tiled=True)
        grad_down = mm_tn(act, g_feed_all)
        g_up = (mm_nt(g_feed_all, w_rest[l][:, fw: fw + width]) * gelu_parts(up)[1]).astype(BF16)
        grad_up = mm_tn(mlp_all, g_up)
        g_min = lax.psum_scatter(mm_nt(g_up, w_rest[l][:, :fw]), "seq", scatter_dimension=0, tiled=True)
        d_scale_m = jnp.sum(g_min * n_m, axis=0)
        d_shift_m = jnp.sum(g_min, axis=0)
        g_mid = g + norm_back(g_min * (1.0 + scale_m), n_m, r_m)
        g_branch = (gate_a * g_mid).astype(BF16)
        d_gate_a = jnp.sum(g_mid * branch, axis=0)
        grad_out = mm_tn(tok_out, g_branch)
        g_o = mm_nt(g_branch, w_rest[l][:, fw + width:]).astype(BF16)
        g_o_heads = lax.all_to_all(g_o, "seq", split_axis=1, concat_axis=0, tiled=True)
        dq, dk, dv = attend_back(q, k, v, logsum, g_o_heads)
        g_qkv = jnp.concatenate([dq, dk, dv], axis=1)
        grad_qkv = mm_tn(attn_all, g_qkv)
        g_ain = lax.psum_scatter(mm_nt(g_qkv, w_qkv[l]), "seq", scatter_dimension=0, tiled=True)
        d_scale_a = jnp.sum(g_ain * n_a, axis=0)
        d_shift_a = jnp.sum(g_ain, axis=0)
        g = g_mid + norm_back(g_ain * (1.0 + scale_a), n_a, r_a)
        d_mods[l] = jnp.concatenate([d_shift_a, d_scale_a, d_gate_a, d_shift_m, d_scale_m, d_gate_m])
        packed = jnp.concatenate([grad_up, grad_down, grad_out, grad_qkv], axis=1).astype(BF16)
        reduced[l] = lax.psum_scatter(packed, "fsdp", scatter_dimension=0, tiled=True)

        def place(x, axis):
            zeros = jnp.zeros(x.shape[:axis] + (ns,) + x.shape[axis + 1:], F32)
            return lax.dynamic_update_slice_in_dim(zeros, x, s, axis)

        qv_g = place(jnp.stack([jnp.sum(dq.astype(F32), axis=0), jnp.sum(dv.astype(F32), axis=0)])[:, None, :], 1)
        up_g = place(jnp.sum(g_up.astype(F32), axis=0).reshape(n, 1, fc), 1)
        bias_grads[l] = jnp.concatenate([
            qv_g.reshape(n, -1), jnp.sum(g_branch.astype(F32), axis=0).reshape(n, -1),
            up_g.reshape(n, -1), jnp.sum(g_feed.astype(F32), axis=0).reshape(n, -1)], axis=1)

    red = jnp.stack(reduced)
    shared = jnp.concatenate([red[:, :, : fw + width], red[:, :, fw + 2 * width:]], axis=2)
    shared = lax.all_gather(shared, "seq", axis=0, tiled=False).astype(F32)
    grad_up = shared[..., :fw].reshape(ns, layers, rows, n, fc).transpose(1, 2, 3, 0, 4).reshape(layers, rows, ff)
    grad_down = shared[..., fw: fw + width].transpose(1, 0, 2, 3).reshape(layers, ns * fc, width)
    grad_qkv = shared[..., fw + width:].reshape(ns, layers, rows, 3, hc).transpose(1, 2, 3, 0, 4)
    grad_qkv = grad_qkv.reshape(layers, rows, 3 * width)
    grad_out = lax.psum(red[:, :, fw + width: fw + 2 * width], "seq").astype(F32)

    bias = lax.psum(jnp.stack(bias_grads), ("fsdp", "seq"))
    bias = lax.dynamic_index_in_dim(bias, f, 1, keepdims=False)
    cuts = [qv_bias.shape[1], out_bias.shape[1], up_bias.shape[1], down_bias.shape[1]]
    grad_bias, at = [], 0
    for size in cuts:
        grad_bias.append(bias[:, at: at + size])
        at += size

    d_mod = lax.psum(jnp.stack(d_mods), "seq")
    d_mod_all = lax.all_gather(d_mod, "fsdp", axis=0, tiled=False)
    cond_rows32 = cond_rows.astype(F32)
    grad_ada = jnp.stack([
        lax.dot_general(cond_rows32, d_mod_all[:, l], (((0,), (0,)), ((), ())), precision=HIGHEST,
                        preferred_element_type=F32) for l in range(layers)])
    grad_ada_bias = own(jnp.sum(d_mod_all, axis=0), 1, width6 // n)
    g_cond = sum(
        lax.dot_general(d_mod_all[:, l], ada_weight[l].astype(F32), (((1,), (1,)), ((), ())),
                        precision=HIGHEST, preferred_element_type=F32) for l in range(layers))
    g_cond = lax.all_to_all(g_cond, "fsdp", split_axis=0, concat_axis=1, tiled=True)
    _, silu_back = jax.vjp(jax.nn.silu, cond_float)
    grad_condition = silu_back(g_cond)[0]
    return (
        block_out[None], g[None], grad_condition, grad_ada, grad_ada_bias, grad_qkv, grad_bias[0],
        grad_out, grad_bias[1], grad_up, grad_bias[2], grad_down, grad_bias[3],
    )


MESH = pl.DeviceIdType.MESH
FAST = 2
VMEM_LIMIT = 67_043_328
EXP2_SCALE = SCORE_SCALE * 1.4426950408889634


def rcopy(src, dst, send, recv, device):
    return pltpu.make_async_remote_copy(
        src_ref=src, dst_ref=dst, send_sem=send, recv_sem=recv, device_id=device, device_id_type=MESH
    )


def vmem_specs(count):
    return [pl.BlockSpec(memory_space=pltpu.VMEM)] * count


def entry_barrier(devices):
    barrier = pltpu.get_barrier_semaphore()
    for device in devices:
        pl.semaphore_signal(barrier, inc=1, device_id=device, device_id_type=MESH)
    pl.semaphore_wait(barrier, len(devices))


def relative(s, j):
    half = j // 2
    return ((s // 2 + 1 - half) % 2) * 2 + (s % 2 + half + j) % 2


def forward_kernel(n, *refs):
    (x_ref, cond_ref, ada_ref, adab_ref, qkvw_ref, qvb_ref, outw_ref, outb_ref, upw_ref, upb_ref,
     downw_ref, downb_ref,
     out_ref, mod_ref, rows_ref), refs = refs[:15], refs[15:]
    stored, held, refs = refs[:13], refs[13:26], refs[26:]
    wq_ref, wo_ref, wu_ref, wd_ref, xs_ref, attn_ref, qh_ref, tok_ref, branch_ref, mid_ref, mlp_ref, up_ref, feed_ref = held
    (osend, psend, precv, chip_sum, xsend, xrecv, xin,
     sq_ref, so_ref, su_ref, bq_ref, bo_ref, bu_ref, bd_ref, cblock, crecv, bsend, brecv, msend, mrecv, mgath,
     c_s, c_r, b_s, b_r, m_s, m_r, w_s, w_r, z_s, z_r, y_s, y_r, a_s, a_r, t_s, t_r, g_s, g_r, r_s, r_r, e_s, e_r, n_s, n_r, q_s, q_r, o_s) = refs
    f = lax.axis_index("fsdp")
    s = lax.axis_index("seq")
    slow = n // FAST
    a, b = f // FAST, f % FAST
    layers, rows = qkvw_ref.shape[0], qkvw_ref.shape[1]
    block = x_ref.shape[0]
    width = x_ref.shape[1]
    hc = sq_ref.shape[2] // 3
    heads = hc // HEAD_DIM
    fc = su_ref.shape[2] // n
    chunk = downw_ref.shape[1] // 4
    core = s % 2
    across, diagonal, partner = relative(s, 0), relative(s, 1), relative(s, 2)
    y_dev = {"fsdp": a * FAST + (1 - b)}

    def place(l, p, at):
        if p == 1:
            return wo_ref.at[l, core, at]
        return (wq_ref, None, wu_ref, wd_ref)[p].at[l, at]

    peers = [{"fsdp": (f + k) % n} for k in range(1, n)] + [{"seq": across}, {"seq": diagonal}, {"seq": partner}]
    barrier = pltpu.get_barrier_semaphore()
    for device in peers:
        pl.semaphore_signal(barrier, inc=1, device_id=device, device_id_type=MESH)

    def cut_qkv(l, i):
        sq_ref[l] = jnp.concatenate(
            [qkvw_ref[l, :, j * width + i * hc: j * width + (i + 1) * hc] for j in range(3)], axis=1
        )

    def cut_rest(l, i):
        so_ref[l] = outw_ref[l, :, (i % 2) * (width // 2): (i % 2 + 1) * (width // 2)]
        su_ref[l] = jnp.concatenate(
            [upw_ref[l, :, (4 * j + i) * fc: (4 * j + i + 1) * fc] for j in range(n)], axis=1
        )

    def by_member(work):
        for i in range(4):
            @pl.when(s == i)
            def _():
                work(i)

    by_member(lambda i: cut_qkv(0, i))
    cond = cond_ref[...].astype(F32)
    act = cond / (1.0 + jnp.exp(-cond))
    act = act.astype(BF16).astype(F32)
    cblock[...] = jnp.zeros_like(cblock)
    for i in range(n):
        cblock[i, 0:1, :rows] = act[:, i * rows: (i + 1) * rows]
    crecv[f] = cblock[f]
    for l in range(layers):
        bsend[l: l + 1, :] = jnp.concatenate(
            [r[l: l + 1, :].astype(F32) for r in (adab_ref, outb_ref, downb_ref)], axis=1
        )
        bsend[layers + l: layers + l + 1, : hc + 4 * fc] = jnp.concatenate(
            [r[l: l + 1, :].astype(F32) for r in (qvb_ref, upb_ref)], axis=1
        )
    brecv[f] = bsend[...]
    tokens_over = rcopy(x_ref, xin, n_s.at[0], n_r.at[0], {"seq": across})

    def shard(l, p):
        if p == 3:
            return downw_ref.at[l, pl.ds(pl.multiple_of(s * chunk, chunk), chunk)]
        return (sq_ref, so_ref, su_ref)[p].at[l]

    pl.semaphore_wait(barrier, len(peers))
    for k in range(1, n):
        to = (f + k) % n
        rcopy(cblock.at[to], crecv.at[f], c_s.at[k], c_r.at[k], {"fsdp": to}).start()

    def z_copy(l, p, k, to):
        return rcopy(shard(l, p), place(l, p, f), z_s.at[l, p, k], z_r.at[l, p, k], {"fsdp": to})

    def y_copy(l, p, k):
        at = ((a - k + slow) % slow) * FAST + b
        src = shard(l, p) if k == 0 else place(l, p, at)
        return rcopy(src, place(l, p, at), y_s.at[l, p, k], y_r.at[l, p, k], y_dev)

    def launch(l, p):
        y_copy(l, p, 0).start()
        for k in range(1, slow):
            z_copy(l, p, k, ((a + k) % slow) * FAST + b).start()

    launch(0, 0)
    tokens_over.start()
    for k in range(1, n):
        to = (f + k) % n
        rcopy(bsend, brecv.at[f], b_s.at[k], b_r.at[k], {"fsdp": to}).start()

    by_member(lambda i: cut_rest(0, i))
    for k in range(1, n):
        at = (f - k + n) % n
        rcopy(cblock.at[at], crecv.at[at], c_s.at[k], c_r.at[k], {"fsdp": at}).wait_recv()
    cond_rows = jnp.sum(crecv[...], axis=1)
    rows_ref[...] = cond_rows
    cond_rows = cond_rows[:, :rows].astype(BF16)
    for l in range(layers):
        quarter = msend.shape[2]
        part = mm(cond_rows, ada_ref[l, :, pl.ds(pl.multiple_of(s * quarter, quarter), quarter)])
        for i in range(n):
            msend[i, l: l + 1, :] = part[i: i + 1, :]
    mrecv[f] = msend[f]
    for k in range(1, n):
        to = (f + k) % n
        rcopy(msend.at[to], mrecv.at[f], m_s.at[k], m_r.at[k], {"fsdp": to}).start()
    for p in range(1, 4):
        launch(0, p)
    for l in range(1, layers):
        by_member(lambda i: cut_qkv(l, i))
        by_member(lambda i: cut_rest(l, i))
        for p in range(4):
            launch(l, p)

    def forward_weights(l, p):
        for k in range(1, slow):
            at = ((a - k + slow) % slow) * FAST + b
            rcopy(shard(l, p), place(l, p, at), z_s.at[l, p, k], z_r.at[l, p, k], {"fsdp": at}).wait_recv()
            y_copy(l, p, k).start()

    def ready(l, p):
        for k in range(slow):
            at = ((a - k + slow) % slow) * FAST + 1 - b
            rcopy(shard(l, p), place(l, p, at), y_s.at[l, p, k], y_r.at[l, p, k], y_dev).wait_recv()

    for k in range(1, n):
        at = (f - k + n) % n
        rcopy(bsend, brecv.at[at], b_s.at[k], b_r.at[k], {"fsdp": at}).wait_recv()
    ac = adab_ref.shape[1]
    for l in range(layers):
        gathered = lambda lo, size, r=l: jnp.concatenate([brecv[i, r: r + 1, lo: lo + size] for i in range(n)], axis=1)
        bo_ref[l] = gathered(ac, rows)
        bd_ref[l] = gathered(ac + rows, rows)
        q_b, v_b = brecv[s, layers + l: layers + l + 1, :hc], brecv[4 + s, layers + l: layers + l + 1, :hc]
        bq_ref[l] = jnp.concatenate([q_b, jnp.zeros_like(q_b), v_b], axis=1)
    for i in range(4):
        @pl.when(s == i)
        def _():
            for l in range(layers):
                lo = hc + i * fc
                bu_ref[l] = jnp.concatenate(
                    [brecv[j, layers + l: layers + l + 1, lo: lo + fc] for j in range(n)], axis=1
                )
    for k in range(1, n):
        at = (f - k + n) % n
        rcopy(msend.at[at], mrecv.at[at], m_s.at[k], m_r.at[k], {"fsdp": at}).wait_recv()
    mgath[s] = jnp.sum(mrecv[...], axis=0)
    for j in range(3):
        rcopy(mgath.at[s], mgath.at[s], q_s.at[j], q_r.at[j], {"seq": relative(s, j)}).start()
    for j in range(3):
        ref = mgath.at[relative(s, j)]
        rcopy(ref, ref, q_s.at[j], q_r.at[j], {"seq": relative(s, j)}).wait_recv()
    for l in range(layers):
        full = jnp.concatenate([mgath[i, l: l + 1, :] for i in range(4)], axis=1) + jnp.concatenate([brecv[i, l: l + 1, :ac] for i in range(n)], axis=1)
        for r in range(6):
            mod_ref[l, r: r + 1, :] = full[:, r * width: (r + 1) * width]
    for l in range(layers):
        for p in range(4):
            place(l, p, f)[...] = shard(l, p)[...]

    core, side = s % 2, s // 2
    xs_ref[0, side] = x_ref[...].astype(F32)
    tokens_over.wait_recv()
    xs_ref[0, 1 - side] = xin[...].astype(F32)

    def save(l, *members):
        for i in members:
            save_copy(l, i).start()

    def save_copy(l, i):
        src = held[i].at[l, side] if i in (7, 8) else held[i].at[l]
        return pltpu.make_async_copy(src, stored[i].at[l], o_s.at[l, i])

    def matrix(ref, l):
        return ref[l].reshape(n * rows, ref.shape[3])

    def half_copy(l):
        ref = wo_ref.at[l, core]
        return rcopy(ref, ref, w_s.at[l], w_r.at[l], {"seq": partner})

    def half_arrived(l):
        ref = wo_ref.at[l, 1 - core]
        rcopy(ref, ref, w_s.at[l], w_r.at[l], {"seq": partner}).wait_recv()

    def share(buf, l, i, send, recv):
        ref = buf.at[l, 2 * i + core]
        return rcopy(ref, ref, send.at[i], recv.at[i], {"seq": partner})

    def shared(buf, l, i, send, recv):
        ref = buf.at[l, 2 * i + 1 - core]
        rcopy(ref, ref, send.at[i], recv.at[i], {"seq": partner}).wait_recv()

    def part_copy(i):
        return rcopy(psend.at[i], precv.at[i], r_s.at[i], r_r.at[i], {"seq": partner})

    def over(i):
        return rcopy(xsend.at[i], xrecv.at[i], e_s.at[i], e_r.at[i], {"seq": across})

    def out_copy(l, j, i, t):
        return rcopy(osend.at[t], tok_ref.at[l, i, s], t_s.at[j, i], t_r.at[j, i], {"seq": relative(s, j)})

    def layer(l, carry):
        row = lambda i: mod_ref[l, i: i + 1, :]

        def qkv_block(t):
            val = (mm(attn_ref[l, t], matrix(wq_ref, l)) + bq_ref[l]).astype(BF16)
            for h in range(3 * heads):
                qh_ref[l, h, pl.ds(pl.multiple_of(t * block, block), block), :] = (
                    val[:, h * HEAD_DIM: (h + 1) * HEAD_DIM]
                )

        def enter(i, carry):
            @pl.when(l > 0)
            def _():
                over(i).wait_recv()
                feed = chip_sum[i] + xrecv[i].astype(F32) + bd_ref[l - 1]
                xs_ref[l, i] = mid_ref[l - 1, i] + mod_ref[l - 1, 5:6, :] * feed

                @pl.when(i == side)
                def _():
                    feed_ref[l - 1] = feed

                over(i).wait_send()

            normed, _ = normalize(xs_ref[l, i])
            attn_ref[l, 2 * i + core] = (normed * (1.0 + row(1)) + row(0)).astype(BF16)
            share(attn_ref, l, i, a_s, a_r).start()

            @pl.when((l == 0) & (i == 0))
            def _():
                forward_weights(0, 0)

            @pl.when(i == 0)
            def _():
                ready(l, 0)

            def both(w, carry):
                @pl.when(w == 1)
                def _():
                    shared(attn_ref, l, i, a_s, a_r)

                qkv_block(2 * i + (core + w) % 2)
                return carry

            lax.fori_loop(0, 2, both, 0)
            return carry

        lax.fori_loop(0, 2, enter, 0)

        @pl.when(l > 0)
        def _():
            save(l - 1, 12)
            forward_weights(l, 2)

        def attend_block(t, carry):
            outs = []
            for h in range(heads):
                q = qh_ref[l, h, pl.ds(pl.multiple_of(t * block, block), block), :]
                e = jnp.exp2(mm_nt(q, qh_ref[l, heads + h]) * EXP2_SCALE)
                inverse = 1.0 / jnp.sum(e, axis=-1, keepdims=True)
                prob = (e * inverse).astype(BF16)
                outs.append(mm(prob, qh_ref[l, 2 * heads + h]))
            val = jnp.concatenate(outs, axis=1).astype(BF16)
            osend[t] = val
            i = t // 2

            @pl.when(t % 2 == core)
            def _():
                tok_ref[l, i, s] = val
                out_copy(l, 0, i, t).start()

            @pl.when(t % 2 != core)
            def _():
                out_copy(l, 1, i, t).start()
                out_copy(l, 2, i, t).start()

            @pl.when((t == 2) & (l == 0))
            def _():
                forward_weights(0, 1)

            return carry

        lax.fori_loop(0, 4, attend_block, 0)
        save(l, 0, 4, 5, 6)
        ready(l, 1)
        half_copy(l).start()

        @pl.when(l > 0)
        def _():
            forward_weights(l, 3)

        half_arrived(l)

        def exchange(i):
            part_copy(i).wait_recv()
            chip_sum[i] = chip_sum[i] + precv[i]

            @pl.when((l + 1 < layers) | (i != side))
            def _():
                xsend[i] = chip_sum[i].astype(BF16)
                over(i).start()

        def mlp(i, carry):
            for j in range(3):
                ref = tok_ref.at[l, i, relative(s, j)]
                rcopy(ref, ref, t_s.at[j, i], t_r.at[j, i], {"seq": relative(s, j)}).wait_recv()
            tokens_out = jnp.concatenate([tok_ref[l, i, t] for t in range(4)], axis=1)
            branch = jnp.concatenate(
                [mm(tokens_out, wo_ref[l, c].reshape(n * rows, width // 2)) for c in range(2)], axis=1
            ) + bo_ref[l]
            branch_ref[l, i] = branch
            middle = xs_ref[l, i] + row(2) * branch
            mid_ref[l, i] = middle
            normed, _ = normalize(middle)
            mlp_ref[l, 2 * i + core] = (normed * (1.0 + row(4)) + row(3)).astype(BF16)
            share(mlp_ref, l, i, g_s, g_r).start()

            @pl.when((i == 0) & (l == 0))
            def _():
                forward_weights(0, 2)
                forward_weights(0, 3)

            @pl.when(i == 0)
            def _():
                ready(l, 2)
                ready(l, 3)

            def both(w, carry):
                @pl.when(w == 1)
                def _():
                    shared(mlp_ref, l, i, g_s, g_r)

                t = 2 * i + (core + w) % 2
                up = mm(mlp_ref[l, t], matrix(wu_ref, l)) + bu_ref[l]
                up_ref[l, t] = up
                act = gelu_parts(up)[0].astype(BF16)
                part = mm(act, matrix(wd_ref, l))

                @pl.when(w == 0)
                def _():
                    chip_sum[i] = part

                @pl.when(w == 1)
                def _():
                    psend[i] = part
                    part_copy(i).start()

                @pl.when((w == 0) & (i == 1))
                def _():
                    exchange(0)

                return carry

            lax.fori_loop(0, 2, both, 0)
            return carry

        lax.fori_loop(0, 2, mlp, 0)
        exchange(1)
        save(l, 1, 2, 3, 7, 8, 9, 10, 11)

        @pl.when(l + 1 < layers)
        def _():
            forward_weights(1, 0)
            forward_weights(1, 1)

        half_copy(l).wait_send()
        for i in range(2):
            share(attn_ref, l, i, a_s, a_r).wait_send()
            share(mlp_ref, l, i, g_s, g_r).wait_send()
            part_copy(i).wait_send()
            for j in range(3):
                out_copy(l, j, i, 2 * i).wait_send()
        return carry

    lax.fori_loop(0, layers, layer, 0)
    last = layers - 1
    over(side).wait_recv()
    feed = chip_sum[side] + xrecv[side].astype(F32) + bd_ref[last]
    feed_ref[last] = feed
    save(last, 12)
    out_ref[...] = (mid_ref[last, side] + mod_ref[last, 5:6, :] * feed).astype(BF16)
    over(1 - side).wait_send()
    tokens_over.wait_send()
    for j in range(3):
        rcopy(mgath.at[s], mgath.at[s], q_s.at[j], q_r.at[j], {"seq": relative(s, j)}).wait_send()
    for l in range(layers):
        for i in range(13):
            save_copy(l, i).wait()
    for l in range(layers):
        for p in range(4):
            y_copy(l, p, 0).wait_send()
            for k in range(1, slow):
                z_copy(l, p, k, ((a + k) % slow) * FAST + b).wait_send()
                y_copy(l, p, k).wait_send()
    for k in range(1, n):
        to = (f + k) % n
        rcopy(cblock.at[to], crecv.at[f], c_s.at[k], c_r.at[k], {"fsdp": to}).wait_send()
        rcopy(bsend, brecv.at[f], b_s.at[k], b_r.at[k], {"fsdp": to}).wait_send()
        rcopy(msend.at[to], mrecv.at[f], m_s.at[k], m_r.at[k], {"fsdp": to}).wait_send()


def forward(n, x, cond, weights):
    layers, rows, width6 = weights[0].shape
    block, width = x.shape
    qc = weights[2].shape[2] // 4
    hc = qc // 3
    nh = qc // HEAD_DIM
    uc = weights[6].shape[2] // 4
    total = 4 * block
    lanes = rows + -rows % 128
    sds = jax.ShapeDtypeStruct
    outs = (
        sds((block, width), BF16),
        sds((layers, 6, width), F32),
        sds((n, lanes), F32),
        sds((layers, n, rows, qc), BF16),
        sds((layers, 2, n, rows, width // 2), BF16),
        sds((layers, n, rows, uc), BF16),
        sds((layers, n, rows, width), BF16),
        sds((layers, 2, block, width), F32),
        sds((layers, 4, block, width), BF16),
        sds((layers, nh, total, HEAD_DIM), BF16),
        sds((layers, 4, block, hc), BF16),
        sds((layers, block, width), F32),
        sds((layers, 2, block, width), F32),
        sds((layers, 4, block, width), BF16),
        sds((layers, 4, block, uc), F32),
        sds((layers, block, width), F32),
    )
    slow = n // FAST
    dma = pltpu.SemaphoreType.DMA
    kept = [list(x.shape) for x in outs[3:]]
    for i in (7, 8):
        kept[i].insert(1, 2)
    scratch = [pltpu.VMEM(tuple(shape), x.dtype) for shape, x in zip(kept, outs[3:])] + [
        pltpu.VMEM((4, block, hc), BF16),
        pltpu.VMEM((2, block, width), F32),
        pltpu.VMEM((2, block, width), F32),
        pltpu.VMEM((2, block, width), F32),
        pltpu.VMEM((2, block, width), BF16),
        pltpu.VMEM((2, block, width), BF16),
        pltpu.VMEM((block, width), BF16),
        pltpu.VMEM((layers, rows, qc), BF16),
        pltpu.VMEM((layers, rows, width // 2), BF16),
        pltpu.VMEM((layers, rows, uc), BF16),
        pltpu.VMEM((layers, 1, qc), F32),
        pltpu.VMEM((layers, 1, width), F32),
        pltpu.VMEM((layers, 1, uc), F32),
        pltpu.VMEM((layers, 1, width), F32),
        pltpu.VMEM((n, 8, lanes), F32),
        pltpu.VMEM((n, 8, lanes), F32),
        pltpu.VMEM((2 * layers, width), F32),
        pltpu.VMEM((n, 2 * layers, width), F32),
        pltpu.VMEM((n, layers, width6 // 4), F32),
        pltpu.VMEM((n, layers, width6 // 4), F32),
        pltpu.VMEM((4, layers, width6 // 4), F32),
    ] + [dma((n,))] * 6 + [dma((layers,))] * 2 + [dma((layers, 4, slow))] * 4 + [dma((2,))] * 2 + [dma((3, 2))] * 2 + [dma((2,))] * 6 + [dma((1,))] * 2 + [dma((3,))] * 2 + [dma((layers, 13))]
    return pl.pallas_call(
        functools.partial(forward_kernel, n),
        out_shape=outs,
        in_specs=vmem_specs(12),
        out_specs=tuple(vmem_specs(3) + [pl.BlockSpec(memory_space=pl.ANY)] * 13),
        scratch_shapes=scratch,
        compiler_params=pltpu.CompilerParams(
            collective_id=1, has_side_effects=True, vmem_limit_bytes=VMEM_LIMIT
        ),
    )(x, cond, *weights)


def backward_kernel(n, *refs):
    (cot_ref, mod_ref, ada_ref), rest = refs[:3], refs[3:]
    stored, rest = rest[:13], rest[13:]
    (g_ref, vec_all, cat_all, gcond_ref), rest = rest[:4], rest[4:]
    fin, rest = rest[:4], rest[4:]
    loaded, rest = list(rest[:11]), rest[11:]
    loaded.insert(5, loaded[8])
    loaded.insert(8, loaded[11])
    grads, rest = rest[:4], rest[4:]
    y_in, rest = rest[:4], rest[4:]
    z_out, rest = rest[:4], rest[4:]
    z_in, rest = rest[:4], rest[4:]
    kept, rest = rest[:4], rest[4:]
    (gf_ref, gb_ref, act_ref, gup_ref, gqkv_ref, psend, precv, chip_sum, xsend, xrecv,
     gx_ref, gmid_ref, dk_acc, dv_acc, orecv,
     vec_ref, cat_ref, vec_in, vec_sum, cat_in, gc_send, gc_recv, v_s, v_r, u_s, u_r, k_s, k_r, h_s, h_r, i_s, i_r,
     l_s, o_s, o_r, y_s, y_r, z_s, z_r, f_s, f_r, g_s, g_r, t_s, t_r, r_s, r_r, e_s, e_r, n_s, n_r, ada_s) = rest
    wq, wo, wu, wd, xs, attn, qh, tok, branch, mid, mlp, up, feed = range(13)
    down, upw, outw, qkvw = range(4)
    f = lax.axis_index("fsdp")
    s = lax.axis_index("seq")
    slow = n // FAST
    a, b = f // FAST, f % FAST
    layers = mod_ref.shape[0]
    block, width = cot_ref.shape
    rows = width // n
    hc = gqkv_ref.shape[2] // 3
    half = width // 2
    core, side = s % 2, s // 2
    heads = hc // HEAD_DIM
    across, diagonal, partner = relative(s, 0), relative(s, 1), relative(s, 2)
    y_dev = {"fsdp": a * FAST + (1 - b)}

    def load(i, l):
        return pltpu.make_async_copy(stored[i].at[l], loaded[i], l_s.at[i])

    for i in (feed, wd, up, wu, mlp, mid, wo, tok, qh, wq, xs):
        load(i, layers - 1).start()

    entry_barrier(
        [{"fsdp": (f + k) % n} for k in range(1, n)]
        + [{"seq": across}, {"seq": diagonal}, {"seq": partner}]
    )

    def y_copy(l, p):
        return rcopy(grads[p].at[:, 1 - b], y_in[p].at[l], y_s.at[p], y_r.at[l, p], y_dev)

    def z_copy(l, p, k):
        to = (a + k) % slow
        return rcopy(z_out[p].at[to], z_in[p].at[l, k - 1], z_s.at[p, k], z_r.at[l, p, k], {"fsdp": to * FAST + b})

    def z_start(l, p):
        y_copy(l, p).wait_recv()
        for i in range(slow):
            z_out[p][i] = (grads[p][i, b].astype(F32) + y_in[p][l, i].astype(F32)).astype(BF16)
        kept[p][...] = grads[p][a, b].astype(F32) + y_in[p][l, a].astype(F32)
        for k in range(1, slow):
            z_copy(l, p, k).start()
        y_copy(l, p).wait_send()

    def fin_copy(l, p, i):
        mine, theirs = fin[p].at[l, s], fin[p].at[l, across]
        ref = theirs if i == 2 else mine
        return rcopy(ref, ref, f_s.at[l, p, i], f_r.at[l, p, i], {"seq": across if i == 1 else partner})

    def z_finish(l, p):
        total = kept[p][...]
        for k in range(1, slow):
            z_copy(l, p, k).wait_recv()
            total = total + z_in[p][l, k - 1].astype(F32)
        fin[p][l, s] = total.astype(BF16)
        fin_copy(l, p, 1).start()
        fin_copy(l, p, 0).start()
        for k in range(1, slow):
            z_copy(l, p, k).wait_send()

    def fin_arrived(l, p, i):
        ref = fin[p].at[l, (partner, across, diagonal)[i]]
        rcopy(ref, ref, f_s.at[l, p, i], f_r.at[l, p, i], {"seq": partner}).wait_recv()

    def ada_load(q):
        l, r = q // 6, q % 6
        dst = loaded[(wd, wu)[q // n]].at[q % n]
        return pltpu.make_async_copy(ada_ref.at[l, :, pl.ds(r * width, width)], dst, ada_s.at[q])

    def matrix(i):
        return loaded[i][...].reshape(width, loaded[i].shape[2])

    def part_copy(i):
        return rcopy(psend.at[0], precv.at[i], r_s.at[i], r_r.at[i], {"seq": partner})

    def over(kind, i):
        at = 2 * kind + i
        return rcopy(xsend.at[i], xrecv.at[at], e_s.at[at], e_r.at[at], {"seq": across})

    def share(buf, i, send, recv):
        ref = buf.at[2 * i + core]
        return rcopy(ref, ref, send.at[i], recv.at[i], {"seq": partner})

    def shared(buf, i, send, recv):
        ref = buf.at[2 * i + 1 - core]
        rcopy(ref, ref, send.at[i], recv.at[i], {"seq": partner}).wait_recv()

    def place(w, i, part):
        @pl.when(w == 0)
        def _():
            chip_sum[i] = part

        @pl.when(w == 1)
        def _():
            psend[0] = part
            part_copy(i).start()

    def exchange(kind, i, wanted):
        part_copy(i).wait_recv()
        chip_sum[i] = chip_sum[i] + precv[i]

        @pl.when(wanted)
        def _():
            xsend[i] = chip_sum[i].astype(BF16)
            over(kind, i).start()

        part_copy(i).wait_send()

    def vec_copy(l, j):
        return rcopy(vec_ref.at[l], vec_in.at[l, s], v_s.at[l, j], v_r.at[l, j], {"seq": relative(s, j)})

    def vec_start(l):
        vec_in[l, s] = vec_ref[l]
        for j in range(3):
            vec_copy(l, j).start()

    def vec_spread(l):
        for j in range(3):
            ref = vec_in.at[l, relative(s, j)]
            rcopy(ref, ref, v_s.at[l, j], v_r.at[l, j], {"seq": relative(s, j)}).wait_recv()
        vec_sum[l] = jnp.sum(vec_in[l], axis=0)
        vec_all[l, f] = vec_sum[l]
        cat_in[l, f] = cat_ref[l]
        for k in range(1, n):
            to = {"fsdp": (f + k) % n}
            rcopy(vec_sum.at[l], vec_all.at[l, f], u_s.at[l, k], u_r.at[l, k], to).start()
            rcopy(cat_ref.at[l], cat_in.at[l, f], k_s.at[l, k], k_r.at[l, k], to).start()

    def vec_arrived(l):
        for k in range(1, n):
            at = (f - k + n) % n
            rcopy(vec_sum.at[l], vec_all.at[l, at], u_s.at[l, k], u_r.at[l, k], {"fsdp": at}).wait_recv()
            rcopy(cat_ref.at[l], cat_in.at[l, at], k_s.at[l, k], k_r.at[l, k], {"fsdp": at}).wait_recv()

    def sums(value):
        return jnp.sum(value, axis=0, keepdims=True)

    def leave(l, i):
        g_ain = chip_sum[i] + xrecv[2 + i].astype(F32)
        normed, inverse = normalize(loaded[xs][i])

        @pl.when(i == side)
        def _():
            vec_ref[l, 1:2, :] = sums(g_ain * normed)
            vec_ref[l, 0:1, :] = sums(g_ain)

        return gmid_ref[i] + norm_back(g_ain * (1.0 + mod_ref[l, 1:2, :]), normed, inverse)

    cot_over = rcopy(cot_ref, xrecv.at[2 + side], n_s.at[0], n_r.at[0], {"seq": across})
    cot_over.start()
    gx_ref[side] = cot_ref[...].astype(F32)

    def layer(step, carry):
        l = layers - 1 - step
        row = lambda i: mod_ref[l, i: i + 1, :]
        cat_ref[l] = jnp.zeros_like(cat_ref[l])
        for i in (feed, wd, up, wu, mlp):
            load(i, l).wait()

        @pl.when(step > 0)
        def _():
            load(xs, l + 1).wait()

        def enter(turn, carry):
            i = (turn + side * (1 - (step + layers - 1) // layers)) % 2

            @pl.when((step == 0) & (turn == 1))
            def _():
                theirs = xrecv.at[3 - side]
                rcopy(cot_ref, theirs, n_s.at[0], n_r.at[0], {"seq": across}).wait_recv()
                gx_ref[1 - side] = theirs[...].astype(F32)

            @pl.when(step > 0)
            def _():
                over(1, i).wait_recv()
                over(1, i).wait_send()
                gx_ref[i] = leave(l + 1, i)

            g = gx_ref[i]
            g_feed = (row(5) * g).astype(BF16)
            gf_ref[2 * i + core] = g_feed
            share(gf_ref, i, g_s, g_r).start()

            @pl.when(i == side)
            def _():
                vec_ref[l, 5:6, :] = sums(g * loaded[feed][...])
                vec_ref[l, 7:8, :] = sums(g_feed.astype(F32))

            def both(w, carry):
                @pl.when(w == 1)
                def _():
                    shared(gf_ref, i, g_s, g_r)

                t = 2 * i + (core + w) % 2
                value, slope = gelu_parts(loaded[up][t])
                act_ref[pl.ds(pl.multiple_of(t * block, block), block), :] = value.astype(BF16)
                g_up = (mm_nt(gf_ref[t], matrix(wd)) * slope).astype(BF16)
                gup_ref[t] = g_up
                cat_ref[l, 0:1, :] = cat_ref[l, 0:1, :] + sums(g_up.astype(F32))
                place(w, i, mm_nt(g_up, matrix(wu)))
                return carry

            lax.fori_loop(0, 2, both, 0)
            exchange(0, i, l >= 0)
            return carry

        lax.fori_loop(0, 2, enter, 0)

        load(branch, l).start()

        @pl.when(step > 0)
        def _():
            load(xs, l).start()
            vec_start(l + 1)

        whole = lambda ref: ref[...].reshape(4 * block, ref.shape[2])
        grads[down][...] = mm_tn(act_ref[...], whole(gf_ref)).astype(BF16).reshape(grads[down].shape)
        y_copy(l, down).start()
        grads[upw][...] = mm_tn(whole(loaded[mlp]), whole(gup_ref)).astype(BF16).reshape(grads[upw].shape)
        y_copy(l, upw).start()

        load(attn, l).start()

        @pl.when(step > 0)
        def _():
            z_start(l + 1, outw)
            z_start(l + 1, qkvw)

        @pl.when(l > 0)
        def _():
            for i in (wd, up, wu):
                load(i, l - 1).start()

        @pl.when(l == 0)
        def _():
            for q in range(6 * layers):
                ada_load(q).start()

        for i in (mid, branch, wo, tok, qh):
            load(i, l).wait()
        dk_acc[...] = jnp.zeros_like(dk_acc)
        dv_acc[...] = jnp.zeros_like(dv_acc)

        def pair(c):
            src = act_ref.at[pl.ds(0, width), pl.ds(c * half, half)]
            return rcopy(src, orecv.at[l], o_s.at[0], o_r.at[l], {"seq": partner})

        def inner(i, carry):
            over(0, i).wait_recv()
            over(0, i).wait_send()
            g_min = chip_sum[i] + xrecv[i].astype(F32)
            normed, inverse = normalize(loaded[mid][i])
            g_mid = gx_ref[i] + norm_back(g_min * (1.0 + row(4)), normed, inverse)
            gmid_ref[i] = g_mid
            g_branch = (row(2) * g_mid).astype(BF16)
            gb_ref[2 * i + core] = g_branch
            share(gb_ref, i, t_s, t_r).start()

            @pl.when(i == side)
            def _():
                vec_ref[l, 4:5, :] = sums(g_min * normed)
                vec_ref[l, 3:4, :] = sums(g_min)
                vec_ref[l, 2:3, :] = sums(g_mid * loaded[branch][...])
                vec_ref[l, 6:7, :] = sums(g_branch.astype(F32))

            @pl.when(i == 1)
            def _():
                tokens_out = jnp.concatenate([loaded[tok][t] for t in range(4)], axis=1)
                for c in range(2):
                    act_ref[:width, c * half: (c + 1) * half] = mm_tn(
                        tokens_out, gb_ref[s, :, c * half: (c + 1) * half]
                    ).astype(BF16)
                for c in range(2):
                    @pl.when(core != c)
                    def _():
                        pair(c).start()

            def tile(w, carry):
                @pl.when(w == 1)
                def _():
                    shared(gb_ref, i, t_s, t_r)

                t = 2 * i + (core + w) % 2
                at = pl.ds(pl.multiple_of(t * block, block), block)
                lines = hc // rows
                g_o = sum(
                    mm_nt(
                        gb_ref[t, :, c * half: (c + 1) * half],
                        loaded[wo][c, pl.ds(s * lines, lines)].reshape(hc, half),
                    )
                    for c in range(2)
                ).astype(BF16)
                for h in range(heads):
                    q = loaded[qh][h, at, :]
                    k = loaded[qh][heads + h]
                    g_out = g_o[:, h * HEAD_DIM: (h + 1) * HEAD_DIM]
                    e = jnp.exp2(mm_nt(k, q) * EXP2_SCALE)
                    prob = e * (1.0 / jnp.sum(e, axis=0, keepdims=True))
                    dv_acc[h] = dv_acc[h] + mm(prob.astype(BF16), g_out)
                    dp = mm_nt(loaded[qh][2 * heads + h], g_out)
                    inner_sum = jnp.sum(prob * dp, axis=0, keepdims=True)
                    ds = (prob * (dp - inner_sum)).astype(BF16)
                    gqkv_ref[t, :, h * HEAD_DIM: (h + 1) * HEAD_DIM] = (mm_tn(ds, k) * SCORE_SCALE).astype(BF16)
                    dk_acc[h] = dk_acc[h] + mm(ds, q)
                return carry

            lax.fori_loop(0, 2, tile, 0)

            return carry

        lax.fori_loop(0, 2, inner, 0)
        pair(0).wait_recv()
        for c in range(2):
            @pl.when(core == c)
            def _():
                out_sum = act_ref[:width, c * half: (c + 1) * half].astype(F32) + orecv[l].astype(F32)
                grads[outw][...] = out_sum.astype(BF16).reshape(grads[outw].shape)
        y_copy(l, outw).start()
        pair(0).wait_send()

        @pl.when(step > 0)
        def _():
            z_finish(l + 1, down)
            z_finish(l + 1, upw)
            z_finish(l + 1, outw)

        z_start(l, down)
        for h in range(heads):
            for j, acc, scale in ((1, dk_acc, SCORE_SCALE), (2, dv_acc, 1.0)):
                lo = (j * heads + h) * HEAD_DIM
                value = (acc[h] * scale).astype(BF16)
                for t in range(4):
                    gqkv_ref[t, :, lo: lo + HEAD_DIM] = value[t * block: (t + 1) * block]

        @pl.when(l > 0)
        def _():
            for i in (feed, mid, wo, tok, qh):
                load(i, l - 1).start()

        load(wq, l).wait()

        def back(i, carry):
            def both(w, carry):
                place(1 - w, i, mm_nt(gqkv_ref[2 * i + (core + 1 - w) % 2], matrix(wq)))
                return carry

            lax.fori_loop(0, 2, both, 0)
            exchange(1, i, (l > 0) | (i != side))
            return carry

        lax.fori_loop(0, 2, back, 0)
        load(attn, l).wait()
        grads[qkvw][...] = mm_tn(whole(loaded[attn]), whole(gqkv_ref)).astype(BF16).reshape(grads[qkvw].shape)
        y_copy(l, qkvw).start()
        cat_ref[l, 1:2, : 3 * hc] = sums(whole(gqkv_ref).astype(F32))

        @pl.when(l > 0)
        def _():
            for i in (wq, mlp):
                load(i, l - 1).start()

        for i in range(2):
            share(gf_ref, i, g_s, g_r).wait_send()
            share(gb_ref, i, t_s, t_r).wait_send()
        z_start(l, upw)

        @pl.when(step > 0)
        def _():
            z_finish(l + 1, qkvw)
            vec_spread(l + 1)

        return carry

    lax.fori_loop(0, layers, layer, 0)
    load(xs, 0).wait()
    z_start(0, outw)
    over(1, side).wait_recv()
    g_ref[...] = leave(0, side)
    vec_start(0)
    z_start(0, qkvw)
    vec_spread(0)
    over(1, 1 - side).wait_send()
    cot_over.wait_send()
    z_finish(0, down)
    z_finish(0, upw)
    z_finish(0, outw)
    for l in range(1, layers):
        for p in (down, upw, outw, qkvw):
            fin_arrived(l, p, 1)
            fin_copy(l, p, 2).start()
    for l in range(layers):
        vec_arrived(l)
        cat_all[l, s] = jnp.sum(cat_in[l], axis=0)
    for j in range(3):
        ref = cat_all.at[:, s]
        rcopy(ref, ref, h_s.at[j], h_r.at[j], {"seq": relative(s, j)}).start()
    for q in range(6 * layers):
        ada_load(q).wait()
    g_cond = jnp.zeros((n, rows), F32)
    for l in range(layers):
        for r in range(6):
            d = vec_all[l, :, r, :]
            high = d.astype(BF16)
            low = (d - high.astype(F32)).astype(BF16)
            q = 6 * l + r
            w = loaded[(wd, wu)[q // n]][q % n]
            g_cond = g_cond + mm_nt(high, w) + mm_nt(low, w)
    for i in range(n):
        gc_send[i, 0:1, :rows] = g_cond[i: i + 1, :]

    def cond_copy(k):
        to = (f + k) % n
        return rcopy(gc_send.at[to], gc_recv.at[f], i_s.at[k], i_r.at[k], {"fsdp": to})

    gc_recv[f] = gc_send[f]
    for k in range(1, n):
        cond_copy(k).start()
    z_finish(0, qkvw)
    for p in (down, upw, outw, qkvw):
        fin_arrived(0, p, 1)
        fin_copy(0, p, 2).start()
    for k in range(1, n):
        at = (f - k + n) % n
        rcopy(gc_send.at[at], gc_recv.at[at], i_s.at[k], i_r.at[k], {"fsdp": at}).wait_recv()
    gcond_ref[...] = jnp.concatenate([gc_recv[i, 0:1, :rows] for i in range(n)], axis=1)
    for j in range(3):
        ref = cat_all.at[:, relative(s, j)]
        rcopy(ref, ref, h_s.at[j], h_r.at[j], {"seq": relative(s, j)}).wait_recv()
    for l in range(layers):
        for p in range(4):
            fin_arrived(l, p, 0)
            fin_arrived(l, p, 2)
            for i in range(3):
                fin_copy(l, p, i).wait_send()
    for k in range(1, n):
        cond_copy(k).wait_send()
        to = {"fsdp": (f + k) % n}
        for l in range(layers):
            rcopy(vec_sum.at[l], vec_all.at[l, f], u_s.at[l, k], u_r.at[l, k], to).wait_send()
            rcopy(cat_ref.at[l], cat_in.at[l, f], k_s.at[l, k], k_r.at[l, k], to).wait_send()
    for j in range(3):
        ref = cat_all.at[:, s]
        rcopy(ref, ref, h_s.at[j], h_r.at[j], {"seq": relative(s, j)}).wait_send()
        for l in range(layers):
            vec_copy(l, j).wait_send()


def backward(n, cot, mod, ada, stored):
    layers = mod.shape[0]
    block, width = cot.shape
    rows = width // n
    slow = n // FAST
    qc = stored[0].shape[3]
    uc = stored[2].shape[3]
    hc = qc // 3
    nh = qc // HEAD_DIM
    sds = jax.ShapeDtypeStruct
    dma = pltpu.SemaphoreType.DMA
    columns = (width, uc, width // 2, qc)
    outs = [
        sds((block, width), F32),
        sds((layers, n, 8, width), F32),
        sds((layers, 4, 2, uc), F32),
        sds((1, width), F32),
    ] + [sds((layers, 4, rows, c), BF16) for c in columns]
    scratch = (
        [pltpu.VMEM(x.shape[1:], x.dtype) for i, x in enumerate(stored) if i not in (5, 8)]
        + [pltpu.VMEM((slow, FAST, rows, c), BF16) for c in columns]
        + [pltpu.VMEM((layers, slow, rows, c), BF16) for c in columns]
        + [pltpu.VMEM((slow, rows, c), BF16) for c in columns]
        + [pltpu.VMEM((layers, slow - 1, rows, c), BF16) for c in columns]
        + [pltpu.VMEM((rows, c), F32) for c in columns]
        + [
            pltpu.VMEM((4, block, width), BF16),
            pltpu.VMEM((4, block, width), BF16),
            pltpu.VMEM((4 * block, uc), BF16),
            pltpu.VMEM((4, block, uc), BF16),
            pltpu.VMEM((4, block, qc), BF16),
            pltpu.VMEM((1, block, width), F32),
            pltpu.VMEM((2, block, width), F32),
            pltpu.VMEM((2, block, width), F32),
            pltpu.VMEM((2, block, width), BF16),
            pltpu.VMEM((4, block, width), BF16),
            pltpu.VMEM((2, block, width), F32),
            pltpu.VMEM((2, block, width), F32),
            pltpu.VMEM((nh // 3, 4 * block, HEAD_DIM), F32),
            pltpu.VMEM((nh // 3, 4 * block, HEAD_DIM), F32),
            pltpu.VMEM((layers, width, width // 2), BF16),
            pltpu.VMEM((layers, 8, width), F32),
            pltpu.VMEM((layers, 2, uc), F32),
            pltpu.VMEM((layers, 4, 8, width), F32),
            pltpu.VMEM((layers, 8, width), F32),
            pltpu.VMEM((layers, n, 2, uc), F32),
            pltpu.VMEM((n, 8, rows + -rows % 128), F32),
            pltpu.VMEM((n, 8, rows + -rows % 128), F32),
            dma((layers, 3)), dma((layers, 3)),
            dma((layers, n)), dma((layers, n)), dma((layers, n)), dma((layers, n)),
            dma((3,)), dma((3,)), dma((n,)), dma((n,)),
            dma((13,)), dma((1,)), dma((layers,)),
            dma((4,)), dma((layers, 4)),
            dma((4, slow)), dma((layers, 4, slow)),
            dma((layers, 4, 3)), dma((layers, 4, 3)),
        ]
        + [dma((2,))] * 6 + [dma((4,))] * 2 + [dma((1,))] * 2 + [dma((6 * layers,))]
    )
    return pl.pallas_call(
        functools.partial(backward_kernel, n),
        out_shape=tuple(outs),
        in_specs=vmem_specs(2) + [pl.BlockSpec(memory_space=pl.ANY)] * 14,
        out_specs=tuple(vmem_specs(len(outs))),
        scratch_shapes=scratch,
        compiler_params=pltpu.CompilerParams(
            collective_id=2, has_side_effects=True, vmem_limit_bytes=VMEM_LIMIT
        ),
    )(cot, mod, ada, *stored)


def assemble_kernel(n, vec_ref, cat_ref, rows_ref, gcond_ref, cond_ref, fd_ref, fu_ref, fo_ref, fq_ref,
                    gcondition, g_adab, g_qvb, g_ob, g_ub, g_db, g_ada, g_qkv, g_out, g_up, g_down,
                    ada_buf, qkv_buf, out_buf, up_buf, down_buf, sem):
    f = lax.axis_index("fsdp")
    layers, rows = fd_ref.shape[0], fd_ref.shape[2]
    width = rows * n
    hc = fq_ref.shape[3] // 3
    fc = fu_ref.shape[3] // n
    ac = g_adab.shape[1]
    copies = []

    def write(i, l, buf, out):
        copies.append(pltpu.make_async_copy(buf.at[l], out.at[l], sem.at[i, l]))
        copies[-1].start()

    for l in range(layers):
        for t in range(4):
            down_buf[l, t * rows: (t + 1) * rows, :] = fd_ref[l, t].astype(F32)
        write(0, l, down_buf, g_down)
    for l in range(layers):
        for j in range(n):
            up_buf[l, :, 4 * j * fc: 4 * (j + 1) * fc] = jnp.concatenate(
                [fu_ref[l, t, :, j * fc: (j + 1) * fc].astype(F32) for t in range(4)], axis=1
            )
        write(1, l, up_buf, g_up)
    cond_rows = rows_ref[:, :rows].astype(BF16)
    for l in range(layers):
        for r in range(6):
            d = vec_ref[l, :, r, :]
            high = d.astype(BF16)
            low = d - high.astype(F32)
            mid = low.astype(BF16)
            low = (low - mid.astype(F32)).astype(BF16)
            ada_buf[l, :, r * width: (r + 1) * width] = (
                mm_tn(cond_rows, high) + mm_tn(cond_rows, mid) + mm_tn(cond_rows, low)
            )
        write(2, l, ada_buf, g_ada)
    for l in range(layers):
        for j in range(3):
            qkv_buf[l, :, j * width: (j + 1) * width] = jnp.concatenate(
                [fq_ref[l, t, :, j * hc: (j + 1) * hc].astype(F32) for t in range(4)], axis=1
            )
        write(3, l, qkv_buf, g_qkv)
    for l in range(layers):
        for c in range(2):
            out_buf[l, :, c * (width // 2): (c + 1) * (width // 2)] = (
                fo_ref[l, c].astype(F32) + fo_ref[l, 2 + c].astype(F32)
            )
        write(4, l, out_buf, g_out)
    cond = cond_ref[...].astype(F32)
    gate = 1.0 / (1.0 + jnp.exp(-cond))
    gcondition[...] = gcond_ref[...] * (gate * (1.0 + cond * (1.0 - gate)))
    total = [jnp.sum(vec_ref[l], axis=0) for l in range(layers)]
    for i in range(n):
        @pl.when(f == i)
        def _():
            for l in range(layers):
                at = slice(l, l + 1)
                flat = jnp.concatenate([total[l][r: r + 1, :] for r in range(6)], axis=1)
                g_adab[at, :] = flat[:, i * ac: (i + 1) * ac]
                g_ob[at, :] = total[l][6:7, i * rows: (i + 1) * rows]
                g_db[at, :] = total[l][7:8, i * rows: (i + 1) * rows]
                g_ub[at, :] = jnp.concatenate(
                    [cat_ref[l, t, 0:1, i * fc: (i + 1) * fc] for t in range(4)], axis=1
                )
                lo = (i // 4) * 2 * hc
                g_qvb[at, :] = cat_ref[l, i % 4, 1:2, lo: lo + hc]
    for copy in copies:
        copy.wait()


def assemble(n, vec_all, cat_all, cond_rows, g_cond, cond, fins):
    layers, _, rows, width = fins[0].shape
    uc, qc = fins[1].shape[3], fins[3].shape[3]
    sds = jax.ShapeDtypeStruct
    big = [(layers, rows, 6 * width), (layers, rows, 4 * qc), (layers, rows, width),
           (layers, rows, 4 * uc), (layers, 4 * rows, width)]
    small = [(1, width), (layers, 6 * width // n), (layers, 2 * width // n), (layers, rows),
             (layers, 4 * uc // n), (layers, rows)]
    return pl.pallas_call(
        functools.partial(assemble_kernel, n),
        out_shape=tuple(sds(x, F32) for x in small + big),
        in_specs=vmem_specs(9),
        out_specs=tuple(vmem_specs(6) + [pl.BlockSpec(memory_space=pl.ANY)] * 5),
        scratch_shapes=[pltpu.VMEM(x, F32) for x in big] + [pltpu.SemaphoreType.DMA((5, layers))],
        compiler_params=pltpu.CompilerParams(vmem_limit_bytes=VMEM_LIMIT),
    )(vec_all, cat_all, cond_rows, g_cond, cond, *fins)


def fused_device(
    tokens, condition, ada_weight, ada_bias, qkv_weight, qv_bias, out_weight, out_bias,
    up_weight, up_bias, down_weight, down_bias, cotangent,
):
    n = lax.axis_size("fsdp")
    block_out, mod, cond_rows, *stored = forward(
        n, tokens[0], condition,
        (ada_weight, ada_bias, qkv_weight, qv_bias, out_weight, out_bias, up_weight, up_bias, down_weight, down_bias))
    g, vec_all, cat_all, g_cond, *fins = backward(n, cotangent[0], mod, ada_weight, stored)
    (g_condition, g_adab, g_qvb, g_ob, g_ub, g_db, g_ada, g_qkv, g_out, g_up, g_down) = assemble(
        n, vec_all, cat_all, cond_rows, g_cond, condition, fins)
    return (
        block_out[None], g[None], g_condition, g_ada, g_adab, g_qkv, g_qvb, g_out, g_ob, g_up, g_ub, g_down, g_db,
    )


def solution(mesh):
    token = P("fsdp", "seq", None)
    matrix = P(None, "fsdp", None)
    vector = P(None, "fsdp")

    def per_device(*args):
        rows = args[2].shape[1]
        fits = rows % 32 == 0 and mesh.shape["seq"] == 4 and mesh.shape["fsdp"] == 8 and args[0].shape[0] == 1
        return (fused_device if fits else plain_device)(*args)

    return jax.shard_map(
        per_device,
        mesh=mesh,
        in_specs=(token, P("fsdp", None)) + (matrix, vector) * 5 + (token,),
        out_specs=(token, token, P("fsdp", None)) + (matrix, vector) * 5,
        check_vma=False,
    )
```

```python
import functools

import jax
import jax.numpy as jnp
from jax import lax
from jax.experimental import pallas as pl
from jax.experimental.pallas import tpu as pltpu
from jax.sharding import PartitionSpec as P

HEAD_DIM = 64
SCORE_SCALE = HEAD_DIM ** (-0.5)
EPSILON = 1e-06
HIGHEST = lax.Precision.HIGHEST
F32 = jnp.float32
BF16 = jnp.bfloat16


def normalize(values):
    centred = values - jnp.mean(values, axis=-1, keepdims=True)
    inverse = lax.rsqrt(jnp.mean(centred * centred, axis=-1, keepdims=True) + EPSILON)
    return centred * inverse, inverse


def norm_back(gradient, normed, inverse):
    return inverse * (
        gradient
        - jnp.mean(gradient, axis=-1, keepdims=True)
        - normed * jnp.mean(gradient * normed, axis=-1, keepdims=True)
    )


def mm(a, b):
    return lax.dot_general(a, b, (((1,), (0,)), ((), ())), preferred_element_type=F32)


def mm_nt(a, b):
    return lax.dot_general(a, b, (((1,), (1,)), ((), ())), preferred_element_type=F32)


def mm_tn(a, b):
    return lax.dot_general(a, b, (((0,), (0,)), ((), ())), preferred_element_type=F32)


def split_heads(rows):
    return rows.reshape(rows.shape[0], -1, HEAD_DIM).transpose(1, 0, 2)


def join_heads(heads):
    return heads.transpose(1, 0, 2).reshape(heads.shape[1], -1)


def attend(q, k, v):
    q, k, v = split_heads(q), split_heads(k), split_heads(v)
    scores = jnp.einsum("hqd,hkd->hqk", q, k, preferred_element_type=F32) * SCORE_SCALE
    logsum = jnp.log(jnp.sum(jnp.exp(scores), axis=-1, keepdims=True))
    prob = jnp.exp(scores - logsum).astype(BF16)
    out = jnp.einsum("hqk,hkd->hqd", prob, v, preferred_element_type=F32)
    return join_heads(out).astype(BF16), logsum


def attend_back(q, k, v, logsum, out_grad):
    q, k, v, out_grad = split_heads(q), split_heads(k), split_heads(v), split_heads(out_grad)
    scores = jnp.einsum("hqd,hkd->hqk", q, k, preferred_element_type=F32) * SCORE_SCALE
    prob = jnp.exp(scores - logsum)
    dv = jnp.einsum("hqk,hqd->hkd", prob.astype(BF16), out_grad, preferred_element_type=F32)
    dp = jnp.einsum("hqd,hkd->hqk", out_grad, v, preferred_element_type=F32)
    inner = jnp.sum(prob * dp, axis=-1, keepdims=True)
    ds = (prob * (dp - inner)).astype(BF16)
    dq = jnp.einsum("hqk,hkd->hqd", ds, k, preferred_element_type=F32) * SCORE_SCALE
    dk = jnp.einsum("hqk,hqd->hkd", ds, q, preferred_element_type=F32) * SCORE_SCALE
    return [join_heads(t).astype(BF16) for t in (dq, dk, dv)]


def gelu_parts(u):
    c = 0.7978845608028654
    inner = c * (u + 0.044715 * (u * u * u))
    t = jnp.tanh(inner)
    value = 0.5 * u * (1.0 + t)
    slope = 0.5 * (1.0 + t) + 0.5 * u * (1.0 - t * t) * (c * (1.0 + 3.0 * 0.044715 * u * u))
    return value, slope


def plain_device(
    tokens, condition, ada_weight, ada_bias, qkv_weight, qv_bias, out_weight, out_bias,
    up_weight, up_bias, down_weight, down_bias, cotangent,
):
    n = lax.axis_size("fsdp")
    ns = lax.axis_size("seq")
    f = lax.axis_index("fsdp")
    s = lax.axis_index("seq")
    layers, rows, width6 = ada_weight.shape
    width = rows * n
    ff = up_weight.shape[2]
    hc = width // ns
    fc = ff // (ns * n)

    def take(x, axis):
        return lax.dynamic_index_in_dim(x, s, axis, keepdims=False)

    def own(x, axis, size):
        return lax.dynamic_slice_in_dim(x, f * size, size, axis)

    w_qkv, w_rest = [], []
    for l in range(layers):
        q_part = take(qkv_weight[l].reshape(rows, 3, ns, hc), 2).reshape(rows, 3 * hc)
        u_part = take(up_weight[l].reshape(rows, n, ns, fc), 2).reshape(rows, n * fc)
        d_part = take(down_weight[l].reshape(ns, fc, width), 0)
        w_qkv.append(lax.all_gather(q_part, "fsdp", axis=0, tiled=True))
        rest = jnp.concatenate([u_part, d_part, out_weight[l]], axis=1)
        w_rest.append(lax.all_gather(rest, "fsdp", axis=0, tiled=True))
    fw = n * fc

    cond_float = condition.astype(F32)
    cond_act = jax.nn.silu(cond_float).astype(BF16)
    small = jnp.concatenate(
        [ada_bias.reshape(-1), qv_bias.reshape(-1), out_bias.reshape(-1), up_bias.reshape(-1),
         down_bias.reshape(-1), cond_act.reshape(-1)]
    )
    small = lax.all_gather(small, "fsdp", axis=0, tiled=False)
    pos = 0

    def unpack(per_layer):
        nonlocal pos
        part = small[:, pos: pos + layers * per_layer].reshape(n, layers, per_layer)
        pos += layers * per_layer
        return part.transpose(1, 0, 2).reshape(layers, n * per_layer)

    ada_b = unpack(ada_bias.shape[1]).astype(F32)
    qv_b = unpack(qv_bias.shape[1]).astype(F32)
    out_b = unpack(out_bias.shape[1]).astype(F32)
    up_b = unpack(up_bias.shape[1]).astype(F32)
    down_b = unpack(down_bias.shape[1]).astype(F32)
    cond_all = small[:, pos:]
    cond_rows = own(cond_all, 1, rows)
    q_b = take(qv_b[:, :width].reshape(layers, ns, hc), 1)
    v_b = take(qv_b[:, width:].reshape(layers, ns, hc), 1)
    qkv_b = jnp.concatenate([q_b, jnp.zeros_like(q_b), v_b], axis=1)
    up_bs = take(up_b.reshape(layers, n, ns, fc), 2).reshape(layers, fw)

    mod_partial = jnp.stack([mm(cond_rows, ada_weight[l]) for l in range(layers)], axis=1)
    mod = lax.psum_scatter(mod_partial, "fsdp", scatter_dimension=0, tiled=True)[0] + ada_b

    hidden = tokens[0].astype(F32)
    saved = []
    for l in range(layers):
        shift_a, scale_a, gate_a, shift_m, scale_m, gate_m = jnp.split(mod[l], 6)
        n_a, r_a = normalize(hidden)
        attn_in = (n_a * (1.0 + scale_a) + shift_a).astype(BF16)
        attn_all = lax.all_gather(attn_in, "seq", axis=0, tiled=True)
        qkv = (mm(attn_all, w_qkv[l]) + qkv_b[l]).astype(BF16)
        q, k, v = qkv[:, :hc], qkv[:, hc: 2 * hc], qkv[:, 2 * hc:]
        head_out, logsum = attend(q, k, v)
        tok_out = lax.all_to_all(head_out, "seq", split_axis=0, concat_axis=1, tiled=True)
        branch = mm(tok_out, w_rest[l][:, fw + width:]) + out_b[l]
        middle = hidden + gate_a * branch
        n_m, r_m = normalize(middle)
        mlp_in = (n_m * (1.0 + scale_m) + shift_m).astype(BF16)
        mlp_all = lax.all_gather(mlp_in, "seq", axis=0, tiled=True)
        up = mm(mlp_all, w_rest[l][:, :fw]) + up_bs[l]
        act = gelu_parts(up)[0].astype(BF16)
        feed = mm(act, w_rest[l][:, fw: fw + width])
        feed = lax.psum_scatter(feed, "seq", scatter_dimension=0, tiled=True) + down_b[l]
        saved.append((n_a, r_a, attn_all, q, k, v, logsum, tok_out, branch, n_m, r_m, mlp_all, up, act, feed))
        hidden = middle + gate_m * feed
    block_out = hidden.astype(BF16)

    g = cotangent[0].astype(F32)
    d_mods = [None] * layers
    reduced = [None] * layers
    bias_grads = [None] * layers
    for l in reversed(range(layers)):
        shift_a, scale_a, gate_a, shift_m, scale_m, gate_m = jnp.split(mod[l], 6)
        n_a, r_a, attn_all, q, k, v, logsum, tok_out, branch, n_m, r_m, mlp_all, up, act, feed = saved[l]
        g_feed = (gate_m * g).astype(BF16)
        d_gate_m = jnp.sum(g * feed, axis=0)
        g_feed_all = lax.all_gather(g_feed, "seq", axis=0, tiled=True)
        grad_down = mm_tn(act, g_feed_all)
        g_up = (mm_nt(g_feed_all, w_rest[l][:, fw: fw + width]) * gelu_parts(up)[1]).astype(BF16)
        grad_up = mm_tn(mlp_all, g_up)
        g_min = lax.psum_scatter(mm_nt(g_up, w_rest[l][:, :fw]), "seq", scatter_dimension=0, tiled=True)
        d_scale_m = jnp.sum(g_min * n_m, axis=0)
        d_shift_m = jnp.sum(g_min, axis=0)
        g_mid = g + norm_back(g_min * (1.0 + scale_m), n_m, r_m)
        g_branch = (gate_a * g_mid).astype(BF16)
        d_gate_a = jnp.sum(g_mid * branch, axis=0)
        grad_out = mm_tn(tok_out, g_branch)
        g_o = mm_nt(g_branch, w_rest[l][:, fw + width:]).astype(BF16)
        g_o_heads = lax.all_to_all(g_o, "seq", split_axis=1, concat_axis=0, tiled=True)
        dq, dk, dv = attend_back(q, k, v, logsum, g_o_heads)
        g_qkv = jnp.concatenate([dq, dk, dv], axis=1)
        grad_qkv = mm_tn(attn_all, g_qkv)
        g_ain = lax.psum_scatter(mm_nt(g_qkv, w_qkv[l]), "seq", scatter_dimension=0, tiled=True)
        d_scale_a = jnp.sum(g_ain * n_a, axis=0)
        d_shift_a = jnp.sum(g_ain, axis=0)
        g = g_mid + norm_back(g_ain * (1.0 + scale_a), n_a, r_a)
        d_mods[l] = jnp.concatenate([d_shift_a, d_scale_a, d_gate_a, d_shift_m, d_scale_m, d_gate_m])
        packed = jnp.concatenate([grad_up, grad_down, grad_out, grad_qkv], axis=1).astype(BF16)
        reduced[l] = lax.psum_scatter(packed, "fsdp", scatter_dimension=0, tiled=True)

        def place(x, axis):
            zeros = jnp.zeros(x.shape[:axis] + (ns,) + x.shape[axis + 1:], F32)
            return lax.dynamic_update_slice_in_dim(zeros, x, s, axis)

        qv_g = place(jnp.stack([jnp.sum(dq.astype(F32), axis=0), jnp.sum(dv.astype(F32), axis=0)])[:, None, :], 1)
        up_g = place(jnp.sum(g_up.astype(F32), axis=0).reshape(n, 1, fc), 1)
        bias_grads[l] = jnp.concatenate([
            qv_g.reshape(n, -1), jnp.sum(g_branch.astype(F32), axis=0).reshape(n, -1),
            up_g.reshape(n, -1), jnp.sum(g_feed.astype(F32), axis=0).reshape(n, -1)], axis=1)

    red = jnp.stack(reduced)
    shared = jnp.concatenate([red[:, :, : fw + width], red[:, :, fw + 2 * width:]], axis=2)
    shared = lax.all_gather(shared, "seq", axis=0, tiled=False).astype(F32)
    grad_up = shared[..., :fw].reshape(ns, layers, rows, n, fc).transpose(1, 2, 3, 0, 4).reshape(layers, rows, ff)
    grad_down = shared[..., fw: fw + width].transpose(1, 0, 2, 3).reshape(layers, ns * fc, width)
    grad_qkv = shared[..., fw + width:].reshape(ns, layers, rows, 3, hc).transpose(1, 2, 3, 0, 4)
    grad_qkv = grad_qkv.reshape(layers, rows, 3 * width)
    grad_out = lax.psum(red[:, :, fw + width: fw + 2 * width], "seq").astype(F32)

    bias = lax.psum(jnp.stack(bias_grads), ("fsdp", "seq"))
    bias = lax.dynamic_index_in_dim(bias, f, 1, keepdims=False)
    cuts = [qv_bias.shape[1], out_bias.shape[1], up_bias.shape[1], down_bias.shape[1]]
    grad_bias, at = [], 0
    for size in cuts:
        grad_bias.append(bias[:, at: at + size])
        at += size

    d_mod = lax.psum(jnp.stack(d_mods), "seq")
    d_mod_all = lax.all_gather(d_mod, "fsdp", axis=0, tiled=False)
    cond_rows32 = cond_rows.astype(F32)
    grad_ada = jnp.stack([
        lax.dot_general(cond_rows32, d_mod_all[:, l], (((0,), (0,)), ((), ())), precision=HIGHEST,
                        preferred_element_type=F32) for l in range(layers)])
    grad_ada_bias = own(jnp.sum(d_mod_all, axis=0), 1, width6 // n)
    g_cond = sum(
        lax.dot_general(d_mod_all[:, l], ada_weight[l].astype(F32), (((1,), (1,)), ((), ())),
                        precision=HIGHEST, preferred_element_type=F32) for l in range(layers))
    g_cond = lax.all_to_all(g_cond, "fsdp", split_axis=0, concat_axis=1, tiled=True)
    _, silu_back = jax.vjp(jax.nn.silu, cond_float)
    grad_condition = silu_back(g_cond)[0]
    return (
        block_out[None], g[None], grad_condition, grad_ada, grad_ada_bias, grad_qkv, grad_bias[0],
        grad_out, grad_bias[1], grad_up, grad_bias[2], grad_down, grad_bias[3],
    )


MESH = pl.DeviceIdType.MESH
FAST = 2
VMEM_LIMIT = 67_043_328
EXP2_SCALE = SCORE_SCALE * 1.4426950408889634


def rcopy(src, dst, send, recv, device):
    return pltpu.make_async_remote_copy(
        src_ref=src, dst_ref=dst, send_sem=send, recv_sem=recv, device_id=device, device_id_type=MESH
    )


def vmem_specs(count):
    return [pl.BlockSpec(memory_space=pltpu.VMEM)] * count


def entry_barrier(devices):
    barrier = pltpu.get_barrier_semaphore()
    for device in devices:
        pl.semaphore_signal(barrier, inc=1, device_id=device, device_id_type=MESH)
    pl.semaphore_wait(barrier, len(devices))


def relative(s, j):
    half = j // 2
    return ((s // 2 + 1 - half) % 2) * 2 + (s % 2 + half + j) % 2


def forward_kernel(n, *refs):
    (x_ref, cond_ref, ada_in, adab_ref, qkvw_ref, qvb_ref, outw_in, outb_ref, upw_in, upb_ref,
     downw_in, downb_ref,
     out_ref, mod_ref, rows_ref), refs = refs[:15], refs[15:]
    stored, held, refs = refs[:13], refs[13:26], refs[26:]
    wq_ref, wo_ref, wu_ref, wd_ref, xs_ref, attn_ref, qh_ref, tok_ref, branch_ref, mid_ref, mlp_ref, up_ref, feed_ref = held
    (osend, psend, precv, chip_sum, xsend, xrecv, xin,
     sq_ref, so_ref, su_ref, bq_ref, bo_ref, bu_ref, bd_ref, cblock, crecv, bsend, brecv, msend, mrecv, mgath,
     c_s, c_r, b_s, b_r, m_s, m_r, w_s, w_r, z_s, z_r, y_s, y_r, a_s, a_r, t_s, t_r, g_s, g_r, r_s, r_r, e_s, e_r, n_s, n_r, q_s, q_r, o_s,
     upw_ref, outw_ref, ada_ref, downw_ref, i_s) = refs
    loads = [
        pltpu.make_async_copy(src, dst, i_s.at[i])
        for i, (src, dst) in enumerate(
            ((upw_in, upw_ref), (outw_in, outw_ref), (ada_in, ada_ref), (downw_in, downw_ref))
        )
    ]
    for load in loads:
        load.start()
    f = lax.axis_index("fsdp")
    s = lax.axis_index("seq")
    slow = n // FAST
    a, b = f // FAST, f % FAST
    layers, rows = qkvw_ref.shape[0], qkvw_ref.shape[1]
    block = x_ref.shape[0]
    width = x_ref.shape[1]
    hc = sq_ref.shape[2] // 3
    heads = hc // HEAD_DIM
    fc = su_ref.shape[2] // n
    chunk = downw_ref.shape[1] // 4
    core = s % 2
    across, diagonal, partner = relative(s, 0), relative(s, 1), relative(s, 2)
    y_dev = {"fsdp": a * FAST + (1 - b)}

    def place(l, p, at):
        if p == 1:
            return wo_ref.at[l, core, at]
        return (wq_ref, None, wu_ref, wd_ref)[p].at[l, at]

    peers = [{"fsdp": (f + k) % n} for k in range(1, n)] + [{"seq": across}, {"seq": diagonal}, {"seq": partner}]
    barrier = pltpu.get_barrier_semaphore()
    for device in peers:
        pl.semaphore_signal(barrier, inc=1, device_id=device, device_id_type=MESH)

    def cut_qkv(l, i):
        sq_ref[l] = jnp.concatenate(
            [qkvw_ref[l, :, j * width + i * hc: j * width + (i + 1) * hc] for j in range(3)], axis=1
        )

    def cut_rest(l, i):
        so_ref[l] = outw_ref[l, :, (i % 2) * (width // 2): (i % 2 + 1) * (width // 2)]
        su_ref[l] = jnp.concatenate(
            [upw_ref[l, :, (4 * j + i) * fc: (4 * j + i + 1) * fc] for j in range(n)], axis=1
        )

    def by_member(work):
        for i in range(4):
            @pl.when(s == i)
            def _():
                work(i)

    by_member(lambda i: cut_qkv(0, i))
    cond = cond_ref[...].astype(F32)
    act = cond / (1.0 + jnp.exp(-cond))
    act = act.astype(BF16).astype(F32)
    cblock[...] = jnp.zeros_like(cblock)
    for i in range(n):
        cblock[i, 0:1, :rows] = act[:, i * rows: (i + 1) * rows]
    crecv[f] = cblock[f]
    for l in range(layers):
        bsend[l: l + 1, :] = jnp.concatenate(
            [r[l: l + 1, :].astype(F32) for r in (adab_ref, outb_ref, downb_ref)], axis=1
        )
        bsend[layers + l: layers + l + 1, : hc + 4 * fc] = jnp.concatenate(
            [r[l: l + 1, :].astype(F32) for r in (qvb_ref, upb_ref)], axis=1
        )
    brecv[f] = bsend[...]
    tokens_over = rcopy(x_ref, xin, n_s.at[0], n_r.at[0], {"seq": across})

    def shard(l, p):
        if p == 3:
            return downw_ref.at[l, pl.ds(pl.multiple_of(s * chunk, chunk), chunk)]
        return (sq_ref, so_ref, su_ref)[p].at[l]

    pl.semaphore_wait(barrier, len(peers))
    for k in range(1, n):
        to = (f + k) % n
        rcopy(cblock.at[to], crecv.at[f], c_s.at[k], c_r.at[k], {"fsdp": to}).start()

    def z_copy(l, p, k, to):
        return rcopy(shard(l, p), place(l, p, f), z_s.at[l, p, k], z_r.at[l, p, k], {"fsdp": to})

    def y_copy(l, p, k):
        at = ((a - k + slow) % slow) * FAST + b
        src = shard(l, p) if k == 0 else place(l, p, at)
        return rcopy(src, place(l, p, at), y_s.at[l, p, k], y_r.at[l, p, k], y_dev)

    def launch(l, p):
        y_copy(l, p, 0).start()
        for k in range(1, slow):
            z_copy(l, p, k, ((a + k) % slow) * FAST + b).start()

    launch(0, 0)
    tokens_over.start()
    for k in range(1, n):
        to = (f + k) % n
        rcopy(bsend, brecv.at[f], b_s.at[k], b_r.at[k], {"fsdp": to}).start()

    loads[0].wait()
    loads[1].wait()
    by_member(lambda i: cut_rest(0, i))
    loads[2].wait()
    loads[3].wait()
    for k in range(1, n):
        at = (f - k + n) % n
        rcopy(cblock.at[at], crecv.at[at], c_s.at[k], c_r.at[k], {"fsdp": at}).wait_recv()
    cond_rows = jnp.sum(crecv[...], axis=1)
    rows_ref[...] = cond_rows
    cond_rows = cond_rows[:, :rows].astype(BF16)
    for l in range(layers):
        quarter = msend.shape[2]
        part = mm(cond_rows, ada_ref[l, :, pl.ds(pl.multiple_of(s * quarter, quarter), quarter)])
        for i in range(n):
            msend[i, l: l + 1, :] = part[i: i + 1, :]
    mrecv[f] = msend[f]
    for k in range(1, n):
        to = (f + k) % n
        rcopy(msend.at[to], mrecv.at[f], m_s.at[k], m_r.at[k], {"fsdp": to}).start()
    for p in range(1, 4):
        launch(0, p)
    for l in range(1, layers):
        by_member(lambda i: cut_qkv(l, i))
        by_member(lambda i: cut_rest(l, i))
        for p in range(4):
            launch(l, p)

    def forward_weights(l, p):
        for k in range(1, slow):
            at = ((a - k + slow) % slow) * FAST + b
            rcopy(shard(l, p), place(l, p, at), z_s.at[l, p, k], z_r.at[l, p, k], {"fsdp": at}).wait_recv()
            y_copy(l, p, k).start()

    def ready(l, p):
        for k in range(slow):
            at = ((a - k + slow) % slow) * FAST + 1 - b
            rcopy(shard(l, p), place(l, p, at), y_s.at[l, p, k], y_r.at[l, p, k], y_dev).wait_recv()

    for k in range(1, n):
        at = (f - k + n) % n
        rcopy(bsend, brecv.at[at], b_s.at[k], b_r.at[k], {"fsdp": at}).wait_recv()
    ac = adab_ref.shape[1]
    for l in range(layers):
        gathered = lambda lo, size, r=l: jnp.concatenate([brecv[i, r: r + 1, lo: lo + size] for i in range(n)], axis=1)
        bo_ref[l] = gathered(ac, rows)
        bd_ref[l] = gathered(ac + rows, rows)
        q_b, v_b = brecv[s, layers + l: layers + l + 1, :hc], brecv[4 + s, layers + l: layers + l + 1, :hc]
        bq_ref[l] = jnp.concatenate([q_b, jnp.zeros_like(q_b), v_b], axis=1)
    for i in range(4):
        @pl.when(s == i)
        def _():
            for l in range(layers):
                lo = hc + i * fc
                bu_ref[l] = jnp.concatenate(
                    [brecv[j, layers + l: layers + l + 1, lo: lo + fc] for j in range(n)], axis=1
                )
    for k in range(1, n):
        at = (f - k + n) % n
        rcopy(msend.at[at], mrecv.at[at], m_s.at[k], m_r.at[k], {"fsdp": at}).wait_recv()
    mgath[s] = jnp.sum(mrecv[...], axis=0)
    for j in range(3):
        rcopy(mgath.at[s], mgath.at[s], q_s.at[j], q_r.at[j], {"seq": relative(s, j)}).start()
    for j in range(3):
        ref = mgath.at[relative(s, j)]
        rcopy(ref, ref, q_s.at[j], q_r.at[j], {"seq": relative(s, j)}).wait_recv()
    for l in range(layers):
        full = jnp.concatenate([mgath[i, l: l + 1, :] for i in range(4)], axis=1) + jnp.concatenate([brecv[i, l: l + 1, :ac] for i in range(n)], axis=1)
        for r in range(6):
            mod_ref[l, r: r + 1, :] = full[:, r * width: (r + 1) * width]
    for l in range(layers):
        for p in range(4):
            place(l, p, f)[...] = shard(l, p)[...]

    core, side = s % 2, s // 2
    xs_ref[0, side] = x_ref[...].astype(F32)
    tokens_over.wait_recv()
    xs_ref[0, 1 - side] = xin[...].astype(F32)

    def save(l, *members):
        for i in members:
            save_copy(l, i).start()

    def save_copy(l, i):
        src = held[i].at[l, side] if i in (7, 8) else held[i].at[l]
        return pltpu.make_async_copy(src, stored[i].at[l], o_s.at[l, i])

    def matrix(ref, l):
        return ref[l].reshape(n * rows, ref.shape[3])

    def half_copy(l):
        ref = wo_ref.at[l, core]
        return rcopy(ref, ref, w_s.at[l], w_r.at[l], {"seq": partner})

    def half_arrived(l):
        ref = wo_ref.at[l, 1 - core]
        rcopy(ref, ref, w_s.at[l], w_r.at[l], {"seq": partner}).wait_recv()

    def share(buf, l, i, send, recv):
        ref = buf.at[l, 2 * i + core]
        return rcopy(ref, ref, send.at[i], recv.at[i], {"seq": partner})

    def shared(buf, l, i, send, recv):
        ref = buf.at[l, 2 * i + 1 - core]
        rcopy(ref, ref, send.at[i], recv.at[i], {"seq": partner}).wait_recv()

    def part_copy(i):
        return rcopy(psend.at[i], precv.at[i], r_s.at[i], r_r.at[i], {"seq": partner})

    def over(i):
        return rcopy(xsend.at[i], xrecv.at[i], e_s.at[i], e_r.at[i], {"seq": across})

    def out_copy(l, j, i, t):
        return rcopy(osend.at[t], tok_ref.at[l, i, s], t_s.at[j, i], t_r.at[j, i], {"seq": relative(s, j)})

    def layer(l, carry):
        row = lambda i: mod_ref[l, i: i + 1, :]

        def qkv_block(t):
            val = (mm(attn_ref[l, t], matrix(wq_ref, l)) + bq_ref[l]).astype(BF16)
            for h in range(3 * heads):
                qh_ref[l, h, pl.ds(pl.multiple_of(t * block, block), block), :] = (
                    val[:, h * HEAD_DIM: (h + 1) * HEAD_DIM]
                )

        def enter(i, carry):
            @pl.when(l > 0)
            def _():
                over(i).wait_recv()
                feed = chip_sum[i] + xrecv[i].astype(F32) + bd_ref[l - 1]
                xs_ref[l, i] = mid_ref[l - 1, i] + mod_ref[l - 1, 5:6, :] * feed

                @pl.when(i == side)
                def _():
                    feed_ref[l - 1] = feed

                over(i).wait_send()

            normed, _ = normalize(xs_ref[l, i])
            attn_ref[l, 2 * i + core] = (normed * (1.0 + row(1)) + row(0)).astype(BF16)
            share(attn_ref, l, i, a_s, a_r).start()

            @pl.when((l == 0) & (i == 0))
            def _():
                forward_weights(0, 0)

            @pl.when(i == 0)
            def _():
                ready(l, 0)

            def both(w, carry):
                @pl.when(w == 1)
                def _():
                    shared(attn_ref, l, i, a_s, a_r)

                qkv_block(2 * i + (core + w) % 2)
                return carry

            lax.fori_loop(0, 2, both, 0)
            return carry

        lax.fori_loop(0, 2, enter, 0)

        @pl.when(l > 0)
        def _():
            save(l - 1, 12)
            forward_weights(l, 2)

        def attend_block(t, carry):
            outs = []
            for h in range(heads):
                q = qh_ref[l, h, pl.ds(pl.multiple_of(t * block, block), block), :]
                e = jnp.exp2(mm_nt(q, qh_ref[l, heads + h]) * EXP2_SCALE)
                inverse = 1.0 / jnp.sum(e, axis=-1, keepdims=True)
                prob = (e * inverse).astype(BF16)
                outs.append(mm(prob, qh_ref[l, 2 * heads + h]))
            val = jnp.concatenate(outs, axis=1).astype(BF16)
            osend[t] = val
            i = t // 2

            @pl.when(t % 2 == core)
            def _():
                tok_ref[l, i, s] = val
                out_copy(l, 0, i, t).start()

            @pl.when(t % 2 != core)
            def _():
                out_copy(l, 1, i, t).start()
                out_copy(l, 2, i, t).start()

            @pl.when((t == 2) & (l == 0))
            def _():
                forward_weights(0, 1)

            return carry

        lax.fori_loop(0, 4, attend_block, 0)
        save(l, 0, 4, 5, 6)
        ready(l, 1)
        half_copy(l).start()

        @pl.when(l > 0)
        def _():
            forward_weights(l, 3)

        half_arrived(l)

        def exchange(i):
            part_copy(i).wait_recv()
            chip_sum[i] = chip_sum[i] + precv[i]

            @pl.when((l + 1 < layers) | (i != side))
            def _():
                xsend[i] = chip_sum[i].astype(BF16)
                over(i).start()

        flip = (1 - side) * ((l + 1) // layers)

        def mlp(turn, carry):
            i = (turn + flip) % 2
            for j in range(3):
                ref = tok_ref.at[l, i, relative(s, j)]
                rcopy(ref, ref, t_s.at[j, i], t_r.at[j, i], {"seq": relative(s, j)}).wait_recv()
            tokens_out = jnp.concatenate([tok_ref[l, i, t] for t in range(4)], axis=1)
            branch = jnp.concatenate(
                [mm(tokens_out, wo_ref[l, c].reshape(n * rows, width // 2)) for c in range(2)], axis=1
            ) + bo_ref[l]
            branch_ref[l, i] = branch
            middle = xs_ref[l, i] + row(2) * branch
            mid_ref[l, i] = middle
            normed, _ = normalize(middle)
            mlp_ref[l, 2 * i + core] = (normed * (1.0 + row(4)) + row(3)).astype(BF16)
            share(mlp_ref, l, i, g_s, g_r).start()

            @pl.when((turn == 0) & (l == 0))
            def _():
                forward_weights(0, 2)

            @pl.when(turn == 0)
            def _():
                ready(l, 2)

            def both(w, carry):
                @pl.when(w == 1)
                def _():
                    shared(mlp_ref, l, i, g_s, g_r)

                t = 2 * i + (core + w) % 2
                up = mm(mlp_ref[l, t], matrix(wu_ref, l)) + bu_ref[l]
                up_ref[l, t] = up
                act = gelu_parts(up)[0].astype(BF16)

                @pl.when((turn == 0) & (w == 0) & (l == 0))
                def _():
                    forward_weights(0, 3)

                @pl.when((turn == 0) & (w == 0))
                def _():
                    ready(l, 3)

                part = mm(act, matrix(wd_ref, l))

                @pl.when(w == 0)
                def _():
                    chip_sum[i] = part

                @pl.when(w == 1)
                def _():
                    psend[i] = part
                    part_copy(i).start()

                @pl.when((w == 0) & (turn == 1))
                def _():
                    exchange(1 - i)

                return carry

            lax.fori_loop(0, 2, both, 0)
            return carry

        lax.fori_loop(0, 2, mlp, 0)
        exchange((1 + flip) % 2)
        save(l, 1, 2, 3, 7, 8, 9, 10, 11)

        @pl.when(l + 1 < layers)
        def _():
            forward_weights(1, 0)
            forward_weights(1, 1)

        half_copy(l).wait_send()
        for i in range(2):
            share(attn_ref, l, i, a_s, a_r).wait_send()
            share(mlp_ref, l, i, g_s, g_r).wait_send()
            part_copy(i).wait_send()
            for j in range(3):
                out_copy(l, j, i, 2 * i).wait_send()
        return carry

    lax.fori_loop(0, layers, layer, 0)
    last = layers - 1
    over(side).wait_recv()
    feed = chip_sum[side] + xrecv[side].astype(F32) + bd_ref[last]
    feed_ref[last] = feed
    save(last, 12)
    out_ref[...] = (mid_ref[last, side] + mod_ref[last, 5:6, :] * feed).astype(BF16)
    over(1 - side).wait_send()
    tokens_over.wait_send()
    for j in range(3):
        rcopy(mgath.at[s], mgath.at[s], q_s.at[j], q_r.at[j], {"seq": relative(s, j)}).wait_send()
    for l in range(layers):
        for i in range(13):
            save_copy(l, i).wait()
    for l in range(layers):
        for p in range(4):
            y_copy(l, p, 0).wait_send()
            for k in range(1, slow):
                z_copy(l, p, k, ((a + k) % slow) * FAST + b).wait_send()
                y_copy(l, p, k).wait_send()
    for k in range(1, n):
        to = (f + k) % n
        rcopy(cblock.at[to], crecv.at[f], c_s.at[k], c_r.at[k], {"fsdp": to}).wait_send()
        rcopy(bsend, brecv.at[f], b_s.at[k], b_r.at[k], {"fsdp": to}).wait_send()
        rcopy(msend.at[to], mrecv.at[f], m_s.at[k], m_r.at[k], {"fsdp": to}).wait_send()


def forward(n, x, cond, weights):
    layers, rows, width6 = weights[0].shape
    block, width = x.shape
    qc = weights[2].shape[2] // 4
    hc = qc // 3
    nh = qc // HEAD_DIM
    uc = weights[6].shape[2] // 4
    total = 4 * block
    lanes = rows + -rows % 128
    sds = jax.ShapeDtypeStruct
    outs = (
        sds((block, width), BF16),
        sds((layers, 6, width), F32),
        sds((n, lanes), F32),
        sds((layers, n, rows, qc), BF16),
        sds((layers, 2, n, rows, width // 2), BF16),
        sds((layers, n, rows, uc), BF16),
        sds((layers, n, rows, width), BF16),
        sds((layers, 2, block, width), F32),
        sds((layers, 4, block, width), BF16),
        sds((layers, nh, total, HEAD_DIM), BF16),
        sds((layers, 4, block, hc), BF16),
        sds((layers, block, width), F32),
        sds((layers, 2, block, width), F32),
        sds((layers, 4, block, width), BF16),
        sds((layers, 4, block, uc), F32),
        sds((layers, block, width), F32),
    )
    slow = n // FAST
    dma = pltpu.SemaphoreType.DMA
    kept = [list(x.shape) for x in outs[3:]]
    for i in (7, 8):
        kept[i].insert(1, 2)
    scratch = [pltpu.VMEM(tuple(shape), x.dtype) for shape, x in zip(kept, outs[3:])] + [
        pltpu.VMEM((4, block, hc), BF16),
        pltpu.VMEM((2, block, width), F32),
        pltpu.VMEM((2, block, width), F32),
        pltpu.VMEM((2, block, width), F32),
        pltpu.VMEM((2, block, width), BF16),
        pltpu.VMEM((2, block, width), BF16),
        pltpu.VMEM((block, width), BF16),
        pltpu.VMEM((layers, rows, qc), BF16),
        pltpu.VMEM((layers, rows, width // 2), BF16),
        pltpu.VMEM((layers, rows, uc), BF16),
        pltpu.VMEM((layers, 1, qc), F32),
        pltpu.VMEM((layers, 1, width), F32),
        pltpu.VMEM((layers, 1, uc), F32),
        pltpu.VMEM((layers, 1, width), F32),
        pltpu.VMEM((n, 8, lanes), F32),
        pltpu.VMEM((n, 8, lanes), F32),
        pltpu.VMEM((2 * layers, width), F32),
        pltpu.VMEM((n, 2 * layers, width), F32),
        pltpu.VMEM((n, layers, width6 // 4), F32),
        pltpu.VMEM((n, layers, width6 // 4), F32),
        pltpu.VMEM((4, layers, width6 // 4), F32),
    ] + [dma((n,))] * 6 + [dma((layers,))] * 2 + [dma((layers, 4, slow))] * 4 + [dma((2,))] * 2 + [dma((3, 2))] * 2 + [dma((2,))] * 6 + [dma((1,))] * 2 + [dma((3,))] * 2 + [dma((layers, 13))] + [
        pltpu.VMEM(weights[i].shape, BF16) for i in (6, 4, 0, 8)
    ] + [dma((4,))]
    return pl.pallas_call(
        functools.partial(forward_kernel, n),
        out_shape=outs,
        in_specs=[
            pl.BlockSpec(memory_space=pl.ANY if i in (2, 6, 8, 10) else pltpu.VMEM) for i in range(12)
        ],
        out_specs=tuple(vmem_specs(3) + [pl.BlockSpec(memory_space=pl.ANY)] * 13),
        scratch_shapes=scratch,
        compiler_params=pltpu.CompilerParams(
            collective_id=1, has_side_effects=True, vmem_limit_bytes=VMEM_LIMIT
        ),
    )(x, cond, *weights)


def backward_kernel(n, *refs):
    (cot_ref, mod_ref, ada_ref), rest = refs[:3], refs[3:]
    stored, rest = rest[:13], rest[13:]
    (g_ref, vec_all, cat_all, gcond_ref), rest = rest[:4], rest[4:]
    fin, rest = rest[:4], rest[4:]
    loaded, rest = list(rest[:11]), rest[11:]
    loaded.insert(5, loaded[8])
    loaded.insert(8, loaded[11])
    grads, rest = rest[:4], rest[4:]
    y_in, rest = rest[:4], rest[4:]
    z_out, rest = rest[:4], rest[4:]
    z_in, rest = rest[:4], rest[4:]
    kept, rest = rest[:4], rest[4:]
    (gf_ref, gb_ref, act_ref, gup_ref, gqkv_ref, psend, precv, chip_sum, xsend, xrecv,
     gx_ref, gmid_ref, dk_acc, dv_acc, orecv,
     vec_ref, cat_ref, vec_in, vec_sum, cat_in, gc_send, gc_recv, v_s, v_r, u_s, u_r, k_s, k_r, h_s, h_r, i_s, i_r,
     l_s, o_s, o_r, y_s, y_r, z_s, z_r, f_s, f_r, g_s, g_r, t_s, t_r, r_s, r_r, e_s, e_r, n_s, n_r, ada_s) = rest
    wq, wo, wu, wd, xs, attn, qh, tok, branch, mid, mlp, up, feed = range(13)
    down, upw, outw, qkvw = range(4)
    f = lax.axis_index("fsdp")
    s = lax.axis_index("seq")
    slow = n // FAST
    a, b = f // FAST, f % FAST
    layers = mod_ref.shape[0]
    block, width = cot_ref.shape
    rows = width // n
    hc = gqkv_ref.shape[2] // 3
    half = width // 2
    core, side = s % 2, s // 2
    heads = hc // HEAD_DIM
    across, diagonal, partner = relative(s, 0), relative(s, 1), relative(s, 2)
    y_dev = {"fsdp": a * FAST + (1 - b)}

    def load(i, l):
        return pltpu.make_async_copy(stored[i].at[l], loaded[i], l_s.at[i])

    for i in (feed, wd, up, wu, mlp, mid, wo, tok, qh, wq, xs):
        load(i, layers - 1).start()

    entry_barrier(
        [{"fsdp": (f + k) % n} for k in range(1, n)]
        + [{"seq": across}, {"seq": diagonal}, {"seq": partner}]
    )

    def y_copy(l, p):
        return rcopy(grads[p].at[:, 1 - b], y_in[p].at[l], y_s.at[p], y_r.at[l, p], y_dev)

    def z_copy(l, p, k):
        to = (a + k) % slow
        return rcopy(z_out[p].at[to], z_in[p].at[l, k - 1], z_s.at[p, k], z_r.at[l, p, k], {"fsdp": to * FAST + b})

    def z_start(l, p):
        y_copy(l, p).wait_recv()
        for i in range(slow):
            z_out[p][i] = (grads[p][i, b].astype(F32) + y_in[p][l, i].astype(F32)).astype(BF16)
        kept[p][...] = grads[p][a, b].astype(F32) + y_in[p][l, a].astype(F32)
        for k in range(1, slow):
            z_copy(l, p, k).start()
        y_copy(l, p).wait_send()

    def fin_copy(l, p, i):
        mine, theirs = fin[p].at[l, s], fin[p].at[l, across]
        ref = theirs if i == 2 else mine
        return rcopy(ref, ref, f_s.at[l, p, i], f_r.at[l, p, i], {"seq": across if i == 1 else partner})

    def z_finish(l, p):
        total = kept[p][...]
        for k in range(1, slow):
            z_copy(l, p, k).wait_recv()
            total = total + z_in[p][l, k - 1].astype(F32)
        fin[p][l, s] = total.astype(BF16)
        fin_copy(l, p, 1).start()
        fin_copy(l, p, 0).start()
        for k in range(1, slow):
            z_copy(l, p, k).wait_send()

    def fin_arrived(l, p, i):
        ref = fin[p].at[l, (partner, across, diagonal)[i]]
        rcopy(ref, ref, f_s.at[l, p, i], f_r.at[l, p, i], {"seq": partner}).wait_recv()

    def ada_load(q):
        l, r = q // 6, q % 6
        dst = loaded[(wd, wu)[q // n]].at[q % n]
        return pltpu.make_async_copy(ada_ref.at[l, :, pl.ds(r * width, width)], dst, ada_s.at[q])

    def matrix(i):
        return loaded[i][...].reshape(width, loaded[i].shape[2])

    def part_copy(i):
        return rcopy(psend.at[0], precv.at[i], r_s.at[i], r_r.at[i], {"seq": partner})

    def over(kind, i):
        at = 2 * kind + i
        return rcopy(xsend.at[i], xrecv.at[at], e_s.at[at], e_r.at[at], {"seq": across})

    def share(buf, i, send, recv):
        ref = buf.at[2 * i + core]
        return rcopy(ref, ref, send.at[i], recv.at[i], {"seq": partner})

    def shared(buf, i, send, recv):
        ref = buf.at[2 * i + 1 - core]
        rcopy(ref, ref, send.at[i], recv.at[i], {"seq": partner}).wait_recv()

    def place(w, i, part):
        @pl.when(w == 0)
        def _():
            chip_sum[i] = part

        @pl.when(w == 1)
        def _():
            psend[0] = part
            part_copy(i).start()

    def exchange(kind, i, wanted):
        part_copy(i).wait_recv()
        chip_sum[i] = chip_sum[i] + precv[i]

        @pl.when(wanted)
        def _():
            xsend[i] = chip_sum[i].astype(BF16)
            over(kind, i).start()

        part_copy(i).wait_send()

    def vec_copy(l, j):
        return rcopy(vec_ref.at[l], vec_in.at[l, s], v_s.at[l, j], v_r.at[l, j], {"seq": relative(s, j)})

    def vec_start(l):
        vec_in[l, s] = vec_ref[l]
        for j in range(3):
            vec_copy(l, j).start()

    def vec_spread(l):
        for j in range(3):
            ref = vec_in.at[l, relative(s, j)]
            rcopy(ref, ref, v_s.at[l, j], v_r.at[l, j], {"seq": relative(s, j)}).wait_recv()
        vec_sum[l] = jnp.sum(vec_in[l], axis=0)
        vec_all[l, f] = vec_sum[l]
        cat_in[l, f] = cat_ref[l]
        for k in range(1, n):
            to = {"fsdp": (f + k) % n}
            rcopy(vec_sum.at[l], vec_all.at[l, f], u_s.at[l, k], u_r.at[l, k], to).start()
            rcopy(cat_ref.at[l], cat_in.at[l, f], k_s.at[l, k], k_r.at[l, k], to).start()

    def vec_arrived(l):
        for k in range(1, n):
            at = (f - k + n) % n
            rcopy(vec_sum.at[l], vec_all.at[l, at], u_s.at[l, k], u_r.at[l, k], {"fsdp": at}).wait_recv()
            rcopy(cat_ref.at[l], cat_in.at[l, at], k_s.at[l, k], k_r.at[l, k], {"fsdp": at}).wait_recv()

    def sums(value):
        return jnp.sum(value, axis=0, keepdims=True)

    def leave(l, i):
        g_ain = chip_sum[i] + xrecv[2 + i].astype(F32)
        normed, inverse = normalize(loaded[xs][i])

        @pl.when(i == side)
        def _():
            vec_ref[l, 1:2, :] = sums(g_ain * normed)
            vec_ref[l, 0:1, :] = sums(g_ain)

        return gmid_ref[i] + norm_back(g_ain * (1.0 + mod_ref[l, 1:2, :]), normed, inverse)

    cot_over = rcopy(cot_ref, xrecv.at[2 + side], n_s.at[0], n_r.at[0], {"seq": across})
    cot_over.start()
    gx_ref[side] = cot_ref[...].astype(F32)

    def layer(step, carry):
        l = layers - 1 - step
        row = lambda i: mod_ref[l, i: i + 1, :]
        cat_ref[l] = jnp.zeros_like(cat_ref[l])
        for i in (feed, wd, up, wu, mlp):
            load(i, l).wait()

        @pl.when(step > 0)
        def _():
            load(xs, l + 1).wait()

        def enter(turn, carry):
            i = (turn + side * (1 - (step + layers - 1) // layers)) % 2

            @pl.when((step == 0) & (turn == 1))
            def _():
                theirs = xrecv.at[3 - side]
                rcopy(cot_ref, theirs, n_s.at[0], n_r.at[0], {"seq": across}).wait_recv()
                gx_ref[1 - side] = theirs[...].astype(F32)

            @pl.when(step > 0)
            def _():
                over(1, i).wait_recv()
                over(1, i).wait_send()
                gx_ref[i] = leave(l + 1, i)

            g = gx_ref[i]
            g_feed = (row(5) * g).astype(BF16)
            gf_ref[2 * i + core] = g_feed
            share(gf_ref, i, g_s, g_r).start()

            @pl.when(i == side)
            def _():
                vec_ref[l, 5:6, :] = sums(g * loaded[feed][...])
                vec_ref[l, 7:8, :] = sums(g_feed.astype(F32))

            def both(w, carry):
                @pl.when(w == 1)
                def _():
                    shared(gf_ref, i, g_s, g_r)

                t = 2 * i + (core + w) % 2
                value, slope = gelu_parts(loaded[up][t])
                act_ref[pl.ds(pl.multiple_of(t * block, block), block), :] = value.astype(BF16)
                g_up = (mm_nt(gf_ref[t], matrix(wd)) * slope).astype(BF16)
                gup_ref[t] = g_up
                cat_ref[l, 0:1, :] = cat_ref[l, 0:1, :] + sums(g_up.astype(F32))
                place(w, i, mm_nt(g_up, matrix(wu)))
                return carry

            lax.fori_loop(0, 2, both, 0)
            exchange(0, i, l >= 0)
            return carry

        lax.fori_loop(0, 2, enter, 0)

        load(branch, l).start()

        @pl.when(step > 0)
        def _():
            load(xs, l).start()
            vec_start(l + 1)

        whole = lambda ref: ref[...].reshape(4 * block, ref.shape[2])
        grads[down][...] = mm_tn(act_ref[...], whole(gf_ref)).astype(BF16).reshape(grads[down].shape)
        y_copy(l, down).start()
        grads[upw][...] = mm_tn(whole(loaded[mlp]), whole(gup_ref)).astype(BF16).reshape(grads[upw].shape)
        y_copy(l, upw).start()

        load(attn, l).start()

        @pl.when(step > 0)
        def _():
            z_start(l + 1, outw)
            z_start(l + 1, qkvw)

        @pl.when(l > 0)
        def _():
            for i in (wd, up, wu):
                load(i, l - 1).start()

        @pl.when(l == 0)
        def _():
            for q in range(6 * layers):
                ada_load(q).start()

        for i in (mid, branch, wo, tok, qh):
            load(i, l).wait()
        dk_acc[...] = jnp.zeros_like(dk_acc)
        dv_acc[...] = jnp.zeros_like(dv_acc)

        def pair(c):
            src = act_ref.at[pl.ds(0, width), pl.ds(c * half, half)]
            return rcopy(src, orecv.at[l], o_s.at[0], o_r.at[l], {"seq": partner})

        def inner(i, carry):
            over(0, i).wait_recv()
            over(0, i).wait_send()
            g_min = chip_sum[i] + xrecv[i].astype(F32)
            normed, inverse = normalize(loaded[mid][i])
            g_mid = gx_ref[i] + norm_back(g_min * (1.0 + row(4)), normed, inverse)
            gmid_ref[i] = g_mid
            g_branch = (row(2) * g_mid).astype(BF16)
            gb_ref[2 * i + core] = g_branch
            share(gb_ref, i, t_s, t_r).start()

            @pl.when(i == side)
            def _():
                vec_ref[l, 4:5, :] = sums(g_min * normed)
                vec_ref[l, 3:4, :] = sums(g_min)
                vec_ref[l, 2:3, :] = sums(g_mid * loaded[branch][...])
                vec_ref[l, 6:7, :] = sums(g_branch.astype(F32))

            @pl.when((step > 0) & (i == 1))
            def _():
                z_finish(l + 1, down)
                z_finish(l + 1, upw)

            @pl.when(i == 1)
            def _():
                tokens_out = jnp.concatenate([loaded[tok][t] for t in range(4)], axis=1)
                for c in range(2):
                    act_ref[:width, c * half: (c + 1) * half] = mm_tn(
                        tokens_out, gb_ref[s, :, c * half: (c + 1) * half]
                    ).astype(BF16)
                for c in range(2):
                    @pl.when(core != c)
                    def _():
                        pair(c).start()

            def tile(w, carry):
                @pl.when(w == 1)
                def _():
                    shared(gb_ref, i, t_s, t_r)

                t = 2 * i + (core + w) % 2
                at = pl.ds(pl.multiple_of(t * block, block), block)
                lines = hc // rows
                g_o = sum(
                    mm_nt(
                        gb_ref[t, :, c * half: (c + 1) * half],
                        loaded[wo][c, pl.ds(s * lines, lines)].reshape(hc, half),
                    )
                    for c in range(2)
                ).astype(BF16)
                for h in range(heads):
                    q = loaded[qh][h, at, :]
                    k = loaded[qh][heads + h]
                    g_out = g_o[:, h * HEAD_DIM: (h + 1) * HEAD_DIM]
                    e = jnp.exp2(mm_nt(k, q) * EXP2_SCALE)
                    prob = e * (1.0 / jnp.sum(e, axis=0, keepdims=True))
                    dv_acc[h] = dv_acc[h] + mm(prob.astype(BF16), g_out)
                    dp = mm_nt(loaded[qh][2 * heads + h], g_out)
                    inner_sum = jnp.sum(prob * dp, axis=0, keepdims=True)
                    ds = (prob * (dp - inner_sum)).astype(BF16)
                    gqkv_ref[t, :, h * HEAD_DIM: (h + 1) * HEAD_DIM] = (mm_tn(ds, k) * SCORE_SCALE).astype(BF16)
                    dk_acc[h] = dk_acc[h] + mm(ds, q)
                return carry

            lax.fori_loop(0, 2, tile, 0)

            return carry

        lax.fori_loop(0, 2, inner, 0)
        pair(0).wait_recv()
        for c in range(2):
            @pl.when(core == c)
            def _():
                out_sum = act_ref[:width, c * half: (c + 1) * half].astype(F32) + orecv[l].astype(F32)
                grads[outw][...] = out_sum.astype(BF16).reshape(grads[outw].shape)
        y_copy(l, outw).start()
        pair(0).wait_send()

        z_start(l, down)
        for h in range(heads):
            for j, acc, scale in ((1, dk_acc, SCORE_SCALE), (2, dv_acc, 1.0)):
                lo = (j * heads + h) * HEAD_DIM
                value = (acc[h] * scale).astype(BF16)
                for t in range(4):
                    gqkv_ref[t, :, lo: lo + HEAD_DIM] = value[t * block: (t + 1) * block]

        @pl.when(l > 0)
        def _():
            for i in (feed, mid, wo, tok, qh):
                load(i, l - 1).start()

        load(wq, l).wait()

        flip = (1 - side) * ((step + 1) // layers)

        def back(turn, carry):
            i = (turn + flip) % 2

            def both(w, carry):
                place(1 - w, i, mm_nt(gqkv_ref[2 * i + (core + 1 - w) % 2], matrix(wq)))
                return carry

            lax.fori_loop(0, 2, both, 0)
            exchange(1, i, (l > 0) | (i != side))
            return carry

        lax.fori_loop(0, 2, back, 0)
        load(attn, l).wait()
        grads[qkvw][...] = mm_tn(whole(loaded[attn]), whole(gqkv_ref)).astype(BF16).reshape(grads[qkvw].shape)
        y_copy(l, qkvw).start()
        cat_ref[l, 1:2, : 3 * hc] = sums(whole(gqkv_ref).astype(F32))

        @pl.when(l > 0)
        def _():
            for i in (wq, mlp):
                load(i, l - 1).start()

        for i in range(2):
            share(gf_ref, i, g_s, g_r).wait_send()
            share(gb_ref, i, t_s, t_r).wait_send()
        z_start(l, upw)

        @pl.when(step > 0)
        def _():
            z_finish(l + 1, outw)
            z_finish(l + 1, qkvw)
            vec_spread(l + 1)

        return carry

    lax.fori_loop(0, layers, layer, 0)
    load(xs, 0).wait()
    z_start(0, outw)
    over(1, side).wait_recv()
    g_ref[...] = leave(0, side)
    vec_start(0)
    z_start(0, qkvw)
    vec_spread(0)
    over(1, 1 - side).wait_send()
    cot_over.wait_send()
    z_finish(0, down)
    z_finish(0, upw)
    z_finish(0, outw)
    for l in range(1, layers):
        for p in (down, upw, outw, qkvw):
            fin_arrived(l, p, 1)
            fin_copy(l, p, 2).start()
    for l in range(layers):
        vec_arrived(l)
        cat_all[l, s] = jnp.sum(cat_in[l], axis=0)
    for j in range(3):
        ref = cat_all.at[:, s]
        rcopy(ref, ref, h_s.at[j], h_r.at[j], {"seq": relative(s, j)}).start()
    for q in range(6 * layers):
        ada_load(q).wait()
    g_cond = jnp.zeros((n, rows), F32)
    for l in range(layers):
        for r in range(6):
            d = vec_all[l, :, r, :]
            high = d.astype(BF16)
            low = (d - high.astype(F32)).astype(BF16)
            q = 6 * l + r
            w = loaded[(wd, wu)[q // n]][q % n]
            g_cond = g_cond + mm_nt(high, w) + mm_nt(low, w)
    for i in range(n):
        gc_send[i, 0:1, :rows] = g_cond[i: i + 1, :]

    def cond_copy(k):
        to = (f + k) % n
        return rcopy(gc_send.at[to], gc_recv.at[f], i_s.at[k], i_r.at[k], {"fsdp": to})

    gc_recv[f] = gc_send[f]
    for k in range(1, n):
        cond_copy(k).start()
    z_finish(0, qkvw)
    for p in (down, upw, outw, qkvw):
        fin_arrived(0, p, 1)
        fin_copy(0, p, 2).start()
    for k in range(1, n):
        at = (f - k + n) % n
        rcopy(gc_send.at[at], gc_recv.at[at], i_s.at[k], i_r.at[k], {"fsdp": at}).wait_recv()
    gcond_ref[...] = jnp.concatenate([gc_recv[i, 0:1, :rows] for i in range(n)], axis=1)
    for j in range(3):
        ref = cat_all.at[:, relative(s, j)]
        rcopy(ref, ref, h_s.at[j], h_r.at[j], {"seq": relative(s, j)}).wait_recv()
    for l in range(layers):
        for p in range(4):
            fin_arrived(l, p, 0)
            fin_arrived(l, p, 2)
            for i in range(3):
                fin_copy(l, p, i).wait_send()
    for k in range(1, n):
        cond_copy(k).wait_send()
        to = {"fsdp": (f + k) % n}
        for l in range(layers):
            rcopy(vec_sum.at[l], vec_all.at[l, f], u_s.at[l, k], u_r.at[l, k], to).wait_send()
            rcopy(cat_ref.at[l], cat_in.at[l, f], k_s.at[l, k], k_r.at[l, k], to).wait_send()
    for j in range(3):
        ref = cat_all.at[:, s]
        rcopy(ref, ref, h_s.at[j], h_r.at[j], {"seq": relative(s, j)}).wait_send()
        for l in range(layers):
            vec_copy(l, j).wait_send()


def backward(n, cot, mod, ada, stored):
    layers = mod.shape[0]
    block, width = cot.shape
    rows = width // n
    slow = n // FAST
    qc = stored[0].shape[3]
    uc = stored[2].shape[3]
    hc = qc // 3
    nh = qc // HEAD_DIM
    sds = jax.ShapeDtypeStruct
    dma = pltpu.SemaphoreType.DMA
    columns = (width, uc, width // 2, qc)
    outs = [
        sds((block, width), F32),
        sds((layers, n, 8, width), F32),
        sds((layers, 4, 2, uc), F32),
        sds((1, width), F32),
    ] + [sds((layers, 4, rows, c), BF16) for c in columns]
    scratch = (
        [pltpu.VMEM(x.shape[1:], x.dtype) for i, x in enumerate(stored) if i not in (5, 8)]
        + [pltpu.VMEM((slow, FAST, rows, c), BF16) for c in columns]
        + [pltpu.VMEM((layers, slow, rows, c), BF16) for c in columns]
        + [pltpu.VMEM((slow, rows, c), BF16) for c in columns]
        + [pltpu.VMEM((layers, slow - 1, rows, c), BF16) for c in columns]
        + [pltpu.VMEM((rows, c), F32) for c in columns]
        + [
            pltpu.VMEM((4, block, width), BF16),
            pltpu.VMEM((4, block, width), BF16),
            pltpu.VMEM((4 * block, uc), BF16),
            pltpu.VMEM((4, block, uc), BF16),
            pltpu.VMEM((4, block, qc), BF16),
            pltpu.VMEM((1, block, width), F32),
            pltpu.VMEM((2, block, width), F32),
            pltpu.VMEM((2, block, width), F32),
            pltpu.VMEM((2, block, width), BF16),
            pltpu.VMEM((4, block, width), BF16),
            pltpu.VMEM((2, block, width), F32),
            pltpu.VMEM((2, block, width), F32),
            pltpu.VMEM((nh // 3, 4 * block, HEAD_DIM), F32),
            pltpu.VMEM((nh // 3, 4 * block, HEAD_DIM), F32),
            pltpu.VMEM((layers, width, width // 2), BF16),
            pltpu.VMEM((layers, 8, width), F32),
            pltpu.VMEM((layers, 2, uc), F32),
            pltpu.VMEM((layers, 4, 8, width), F32),
            pltpu.VMEM((layers, 8, width), F32),
            pltpu.VMEM((layers, n, 2, uc), F32),
            pltpu.VMEM((n, 8, rows + -rows % 128), F32),
            pltpu.VMEM((n, 8, rows + -rows % 128), F32),
            dma((layers, 3)), dma((layers, 3)),
            dma((layers, n)), dma((layers, n)), dma((layers, n)), dma((layers, n)),
            dma((3,)), dma((3,)), dma((n,)), dma((n,)),
            dma((13,)), dma((1,)), dma((layers,)),
            dma((4,)), dma((layers, 4)),
            dma((4, slow)), dma((layers, 4, slow)),
            dma((layers, 4, 3)), dma((layers, 4, 3)),
        ]
        + [dma((2,))] * 6 + [dma((4,))] * 2 + [dma((1,))] * 2 + [dma((6 * layers,))]
    )
    return pl.pallas_call(
        functools.partial(backward_kernel, n),
        out_shape=tuple(outs),
        in_specs=vmem_specs(2) + [pl.BlockSpec(memory_space=pl.ANY)] * 14,
        out_specs=tuple(vmem_specs(len(outs))),
        scratch_shapes=scratch,
        compiler_params=pltpu.CompilerParams(
            collective_id=2, has_side_effects=True, vmem_limit_bytes=VMEM_LIMIT
        ),
    )(cot, mod, ada, *stored)


def assemble_kernel(n, vec_ref, cat_ref, rows_ref, gcond_ref, cond_ref, fd_ref, fu_ref, fo_ref, fq_ref,
                    gcondition, g_adab, g_qvb, g_ob, g_ub, g_db, g_ada, g_qkv, g_out, g_up, g_down,
                    ada_buf, qkv_buf, out_buf, up_buf, down_buf, sem):
    f = lax.axis_index("fsdp")
    layers, rows = fd_ref.shape[0], fd_ref.shape[2]
    width = rows * n
    hc = fq_ref.shape[3] // 3
    fc = fu_ref.shape[3] // n
    ac = g_adab.shape[1]
    copies = []

    def write(i, l, buf, out):
        copies.append(pltpu.make_async_copy(buf.at[l], out.at[l], sem.at[i, l]))
        copies[-1].start()

    for l in range(layers):
        for t in range(4):
            down_buf[l, t * rows: (t + 1) * rows, :] = fd_ref[l, t].astype(F32)
        write(0, l, down_buf, g_down)
    for l in range(layers):
        for j in range(n):
            up_buf[l, :, 4 * j * fc: 4 * (j + 1) * fc] = jnp.concatenate(
                [fu_ref[l, t, :, j * fc: (j + 1) * fc].astype(F32) for t in range(4)], axis=1
            )
        write(1, l, up_buf, g_up)
    cond_rows = rows_ref[:, :rows].astype(BF16)
    for l in range(layers):
        for r in range(6):
            d = vec_ref[l, :, r, :]
            high = d.astype(BF16)
            low = (d - high.astype(F32)).astype(BF16)
            ada_buf[l, :, r * width: (r + 1) * width] = mm_tn(cond_rows, high) + mm_tn(cond_rows, low)
        write(2, l, ada_buf, g_ada)
    for l in range(layers):
        for j in range(3):
            qkv_buf[l, :, j * width: (j + 1) * width] = jnp.concatenate(
                [fq_ref[l, t, :, j * hc: (j + 1) * hc].astype(F32) for t in range(4)], axis=1
            )
        write(3, l, qkv_buf, g_qkv)
    for l in range(layers):
        for c in range(2):
            out_buf[l, :, c * (width // 2): (c + 1) * (width // 2)] = (
                fo_ref[l, c].astype(F32) + fo_ref[l, 2 + c].astype(F32)
            )
        write(4, l, out_buf, g_out)
    cond = cond_ref[...].astype(F32)
    gate = 1.0 / (1.0 + jnp.exp(-cond))
    gcondition[...] = gcond_ref[...] * (gate * (1.0 + cond * (1.0 - gate)))
    total = [jnp.sum(vec_ref[l], axis=0) for l in range(layers)]
    for i in range(n):
        @pl.when(f == i)
        def _():
            for l in range(layers):
                at = slice(l, l + 1)
                flat = jnp.concatenate([total[l][r: r + 1, :] for r in range(6)], axis=1)
                g_adab[at, :] = flat[:, i * ac: (i + 1) * ac]
                g_ob[at, :] = total[l][6:7, i * rows: (i + 1) * rows]
                g_db[at, :] = total[l][7:8, i * rows: (i + 1) * rows]
                g_ub[at, :] = jnp.concatenate(
                    [cat_ref[l, t, 0:1, i * fc: (i + 1) * fc] for t in range(4)], axis=1
                )
                lo = (i // 4) * 2 * hc
                g_qvb[at, :] = cat_ref[l, i % 4, 1:2, lo: lo + hc]
    for copy in copies:
        copy.wait()


def assemble(n, vec_all, cat_all, cond_rows, g_cond, cond, fins):
    layers, _, rows, width = fins[0].shape
    uc, qc = fins[1].shape[3], fins[3].shape[3]
    sds = jax.ShapeDtypeStruct
    big = [(layers, rows, 6 * width), (layers, rows, 4 * qc), (layers, rows, width),
           (layers, rows, 4 * uc), (layers, 4 * rows, width)]
    small = [(1, width), (layers, 6 * width // n), (layers, 2 * width // n), (layers, rows),
             (layers, 4 * uc // n), (layers, rows)]
    return pl.pallas_call(
        functools.partial(assemble_kernel, n),
        out_shape=tuple(sds(x, F32) for x in small + big),
        in_specs=vmem_specs(9),
        out_specs=tuple(vmem_specs(6) + [pl.BlockSpec(memory_space=pl.ANY)] * 5),
        scratch_shapes=[pltpu.VMEM(x, F32) for x in big] + [pltpu.SemaphoreType.DMA((5, layers))],
        compiler_params=pltpu.CompilerParams(vmem_limit_bytes=VMEM_LIMIT),
    )(vec_all, cat_all, cond_rows, g_cond, cond, *fins)


def fused_device(
    tokens, condition, ada_weight, ada_bias, qkv_weight, qv_bias, out_weight, out_bias,
    up_weight, up_bias, down_weight, down_bias, cotangent,
):
    n = lax.axis_size("fsdp")
    block_out, mod, cond_rows, *stored = forward(
        n, tokens[0], condition,
        (ada_weight, ada_bias, qkv_weight, qv_bias, out_weight, out_bias, up_weight, up_bias, down_weight, down_bias))
    g, vec_all, cat_all, g_cond, *fins = backward(n, cotangent[0], mod, ada_weight, stored)
    (g_condition, g_adab, g_qvb, g_ob, g_ub, g_db, g_ada, g_qkv, g_out, g_up, g_down) = assemble(
        n, vec_all, cat_all, cond_rows, g_cond, condition, fins)
    return (
        block_out[None], g[None], g_condition, g_ada, g_adab, g_qkv, g_qvb, g_out, g_ob, g_up, g_ub, g_down, g_db,
    )


def solution(mesh):
    token = P("fsdp", "seq", None)
    matrix = P(None, "fsdp", None)
    vector = P(None, "fsdp")

    def per_device(*args):
        rows = args[2].shape[1]
        fits = rows % 32 == 0 and mesh.shape["seq"] == 4 and mesh.shape["fsdp"] == 8 and args[0].shape[0] == 1
        return (fused_device if fits else plain_device)(*args)

    return jax.shard_map(
        per_device,
        mesh=mesh,
        in_specs=(token, P("fsdp", None)) + (matrix, vector) * 5 + (token,),
        out_specs=(token, token, P("fsdp", None)) + (matrix, vector) * 5,
        check_vma=False,
    )
```

```python
import functools

import jax
import jax.numpy as jnp
from jax import lax
from jax.experimental import pallas as pl
from jax.experimental.pallas import tpu as pltpu
from jax.sharding import PartitionSpec as P

HEAD_DIM = 64
SCORE_SCALE = HEAD_DIM ** (-0.5)
EPSILON = 1e-06
HIGHEST = lax.Precision.HIGHEST
F32 = jnp.float32
BF16 = jnp.bfloat16


def normalize(values):
    centred = values - jnp.mean(values, axis=-1, keepdims=True)
    inverse = lax.rsqrt(jnp.mean(centred * centred, axis=-1, keepdims=True) + EPSILON)
    return centred * inverse, inverse


def norm_back(gradient, normed, inverse):
    return inverse * (
        gradient
        - jnp.mean(gradient, axis=-1, keepdims=True)
        - normed * jnp.mean(gradient * normed, axis=-1, keepdims=True)
    )


def mm(a, b):
    return lax.dot_general(a, b, (((1,), (0,)), ((), ())), preferred_element_type=F32)


def mm_nt(a, b):
    return lax.dot_general(a, b, (((1,), (1,)), ((), ())), preferred_element_type=F32)


def mm_tn(a, b):
    return lax.dot_general(a, b, (((0,), (0,)), ((), ())), preferred_element_type=F32)


def split_heads(rows):
    return rows.reshape(rows.shape[0], -1, HEAD_DIM).transpose(1, 0, 2)


def join_heads(heads):
    return heads.transpose(1, 0, 2).reshape(heads.shape[1], -1)


def attend(q, k, v):
    q, k, v = split_heads(q), split_heads(k), split_heads(v)
    scores = jnp.einsum("hqd,hkd->hqk", q, k, preferred_element_type=F32) * SCORE_SCALE
    logsum = jnp.log(jnp.sum(jnp.exp(scores), axis=-1, keepdims=True))
    prob = jnp.exp(scores - logsum).astype(BF16)
    out = jnp.einsum("hqk,hkd->hqd", prob, v, preferred_element_type=F32)
    return join_heads(out).astype(BF16), logsum


def attend_back(q, k, v, logsum, out_grad):
    q, k, v, out_grad = split_heads(q), split_heads(k), split_heads(v), split_heads(out_grad)
    scores = jnp.einsum("hqd,hkd->hqk", q, k, preferred_element_type=F32) * SCORE_SCALE
    prob = jnp.exp(scores - logsum)
    dv = jnp.einsum("hqk,hqd->hkd", prob.astype(BF16), out_grad, preferred_element_type=F32)
    dp = jnp.einsum("hqd,hkd->hqk", out_grad, v, preferred_element_type=F32)
    inner = jnp.sum(prob * dp, axis=-1, keepdims=True)
    ds = (prob * (dp - inner)).astype(BF16)
    dq = jnp.einsum("hqk,hkd->hqd", ds, k, preferred_element_type=F32) * SCORE_SCALE
    dk = jnp.einsum("hqk,hqd->hkd", ds, q, preferred_element_type=F32) * SCORE_SCALE
    return [join_heads(t).astype(BF16) for t in (dq, dk, dv)]


def gelu_parts(u):
    c = 0.7978845608028654
    inner = c * (u + 0.044715 * (u * u * u))
    t = jnp.tanh(inner)
    value = 0.5 * u * (1.0 + t)
    slope = 0.5 * (1.0 + t) + 0.5 * u * (1.0 - t * t) * (c * (1.0 + 3.0 * 0.044715 * u * u))
    return value, slope


def plain_device(
    tokens, condition, ada_weight, ada_bias, qkv_weight, qv_bias, out_weight, out_bias,
    up_weight, up_bias, down_weight, down_bias, cotangent,
):
    n = lax.axis_size("fsdp")
    ns = lax.axis_size("seq")
    f = lax.axis_index("fsdp")
    s = lax.axis_index("seq")
    layers, rows, width6 = ada_weight.shape
    width = rows * n
    ff = up_weight.shape[2]
    hc = width // ns
    fc = ff // (ns * n)

    def take(x, axis):
        return lax.dynamic_index_in_dim(x, s, axis, keepdims=False)

    def own(x, axis, size):
        return lax.dynamic_slice_in_dim(x, f * size, size, axis)

    w_qkv, w_rest = [], []
    for l in range(layers):
        q_part = take(qkv_weight[l].reshape(rows, 3, ns, hc), 2).reshape(rows, 3 * hc)
        u_part = take(up_weight[l].reshape(rows, n, ns, fc), 2).reshape(rows, n * fc)
        d_part = take(down_weight[l].reshape(ns, fc, width), 0)
        w_qkv.append(lax.all_gather(q_part, "fsdp", axis=0, tiled=True))
        rest = jnp.concatenate([u_part, d_part, out_weight[l]], axis=1)
        w_rest.append(lax.all_gather(rest, "fsdp", axis=0, tiled=True))
    fw = n * fc

    cond_float = condition.astype(F32)
    cond_act = jax.nn.silu(cond_float).astype(BF16)
    small = jnp.concatenate(
        [ada_bias.reshape(-1), qv_bias.reshape(-1), out_bias.reshape(-1), up_bias.reshape(-1),
         down_bias.reshape(-1), cond_act.reshape(-1)]
    )
    small = lax.all_gather(small, "fsdp", axis=0, tiled=False)
    pos = 0

    def unpack(per_layer):
        nonlocal pos
        part = small[:, pos: pos + layers * per_layer].reshape(n, layers, per_layer)
        pos += layers * per_layer
        return part.transpose(1, 0, 2).reshape(layers, n * per_layer)

    ada_b = unpack(ada_bias.shape[1]).astype(F32)
    qv_b = unpack(qv_bias.shape[1]).astype(F32)
    out_b = unpack(out_bias.shape[1]).astype(F32)
    up_b = unpack(up_bias.shape[1]).astype(F32)
    down_b = unpack(down_bias.shape[1]).astype(F32)
    cond_all = small[:, pos:]
    cond_rows = own(cond_all, 1, rows)
    q_b = take(qv_b[:, :width].reshape(layers, ns, hc), 1)
    v_b = take(qv_b[:, width:].reshape(layers, ns, hc), 1)
    qkv_b = jnp.concatenate([q_b, jnp.zeros_like(q_b), v_b], axis=1)
    up_bs = take(up_b.reshape(layers, n, ns, fc), 2).reshape(layers, fw)

    mod_partial = jnp.stack([mm(cond_rows, ada_weight[l]) for l in range(layers)], axis=1)
    mod = lax.psum_scatter(mod_partial, "fsdp", scatter_dimension=0, tiled=True)[0] + ada_b

    hidden = tokens[0].astype(F32)
    saved = []
    for l in range(layers):
        shift_a, scale_a, gate_a, shift_m, scale_m, gate_m = jnp.split(mod[l], 6)
        n_a, r_a = normalize(hidden)
        attn_in = (n_a * (1.0 + scale_a) + shift_a).astype(BF16)
        attn_all = lax.all_gather(attn_in, "seq", axis=0, tiled=True)
        qkv = (mm(attn_all, w_qkv[l]) + qkv_b[l]).astype(BF16)
        q, k, v = qkv[:, :hc], qkv[:, hc: 2 * hc], qkv[:, 2 * hc:]
        head_out, logsum = attend(q, k, v)
        tok_out = lax.all_to_all(head_out, "seq", split_axis=0, concat_axis=1, tiled=True)
        branch = mm(tok_out, w_rest[l][:, fw + width:]) + out_b[l]
        middle = hidden + gate_a * branch
        n_m, r_m = normalize(middle)
        mlp_in = (n_m * (1.0 + scale_m) + shift_m).astype(BF16)
        mlp_all = lax.all_gather(mlp_in, "seq", axis=0, tiled=True)
        up = mm(mlp_all, w_rest[l][:, :fw]) + up_bs[l]
        act = gelu_parts(up)[0].astype(BF16)
        feed = mm(act, w_rest[l][:, fw: fw + width])
        feed = lax.psum_scatter(feed, "seq", scatter_dimension=0, tiled=True) + down_b[l]
        saved.append((n_a, r_a, attn_all, q, k, v, logsum, tok_out, branch, n_m, r_m, mlp_all, up, act, feed))
        hidden = middle + gate_m * feed
    block_out = hidden.astype(BF16)

    g = cotangent[0].astype(F32)
    d_mods = [None] * layers
    reduced = [None] * layers
    bias_grads = [None] * layers
    for l in reversed(range(layers)):
        shift_a, scale_a, gate_a, shift_m, scale_m, gate_m = jnp.split(mod[l], 6)
        n_a, r_a, attn_all, q, k, v, logsum, tok_out, branch, n_m, r_m, mlp_all, up, act, feed = saved[l]
        g_feed = (gate_m * g).astype(BF16)
        d_gate_m = jnp.sum(g * feed, axis=0)
        g_feed_all = lax.all_gather(g_feed, "seq", axis=0, tiled=True)
        grad_down = mm_tn(act, g_feed_all)
        g_up = (mm_nt(g_feed_all, w_rest[l][:, fw: fw + width]) * gelu_parts(up)[1]).astype(BF16)
        grad_up = mm_tn(mlp_all, g_up)
        g_min = lax.psum_scatter(mm_nt(g_up, w_rest[l][:, :fw]), "seq", scatter_dimension=0, tiled=True)
        d_scale_m = jnp.sum(g_min * n_m, axis=0)
        d_shift_m = jnp.sum(g_min, axis=0)
        g_mid = g + norm_back(g_min * (1.0 + scale_m), n_m, r_m)
        g_branch = (gate_a * g_mid).astype(BF16)
        d_gate_a = jnp.sum(g_mid * branch, axis=0)
        grad_out = mm_tn(tok_out, g_branch)
        g_o = mm_nt(g_branch, w_rest[l][:, fw + width:]).astype(BF16)
        g_o_heads = lax.all_to_all(g_o, "seq", split_axis=1, concat_axis=0, tiled=True)
        dq, dk, dv = attend_back(q, k, v, logsum, g_o_heads)
        g_qkv = jnp.concatenate([dq, dk, dv], axis=1)
        grad_qkv = mm_tn(attn_all, g_qkv)
        g_ain = lax.psum_scatter(mm_nt(g_qkv, w_qkv[l]), "seq", scatter_dimension=0, tiled=True)
        d_scale_a = jnp.sum(g_ain * n_a, axis=0)
        d_shift_a = jnp.sum(g_ain, axis=0)
        g = g_mid + norm_back(g_ain * (1.0 + scale_a), n_a, r_a)
        d_mods[l] = jnp.concatenate([d_shift_a, d_scale_a, d_gate_a, d_shift_m, d_scale_m, d_gate_m])
        packed = jnp.concatenate([grad_up, grad_down, grad_out, grad_qkv], axis=1).astype(BF16)
        reduced[l] = lax.psum_scatter(packed, "fsdp", scatter_dimension=0, tiled=True)

        def place(x, axis):
            zeros = jnp.zeros(x.shape[:axis] + (ns,) + x.shape[axis + 1:], F32)
            return lax.dynamic_update_slice_in_dim(zeros, x, s, axis)

        qv_g = place(jnp.stack([jnp.sum(dq.astype(F32), axis=0), jnp.sum(dv.astype(F32), axis=0)])[:, None, :], 1)
        up_g = place(jnp.sum(g_up.astype(F32), axis=0).reshape(n, 1, fc), 1)
        bias_grads[l] = jnp.concatenate([
            qv_g.reshape(n, -1), jnp.sum(g_branch.astype(F32), axis=0).reshape(n, -1),
            up_g.reshape(n, -1), jnp.sum(g_feed.astype(F32), axis=0).reshape(n, -1)], axis=1)

    red = jnp.stack(reduced)
    shared = jnp.concatenate([red[:, :, : fw + width], red[:, :, fw + 2 * width:]], axis=2)
    shared = lax.all_gather(shared, "seq", axis=0, tiled=False).astype(F32)
    grad_up = shared[..., :fw].reshape(ns, layers, rows, n, fc).transpose(1, 2, 3, 0, 4).reshape(layers, rows, ff)
    grad_down = shared[..., fw: fw + width].transpose(1, 0, 2, 3).reshape(layers, ns * fc, width)
    grad_qkv = shared[..., fw + width:].reshape(ns, layers, rows, 3, hc).transpose(1, 2, 3, 0, 4)
    grad_qkv = grad_qkv.reshape(layers, rows, 3 * width)
    grad_out = lax.psum(red[:, :, fw + width: fw + 2 * width], "seq").astype(F32)

    bias = lax.psum(jnp.stack(bias_grads), ("fsdp", "seq"))
    bias = lax.dynamic_index_in_dim(bias, f, 1, keepdims=False)
    cuts = [qv_bias.shape[1], out_bias.shape[1], up_bias.shape[1], down_bias.shape[1]]
    grad_bias, at = [], 0
    for size in cuts:
        grad_bias.append(bias[:, at: at + size])
        at += size

    d_mod = lax.psum(jnp.stack(d_mods), "seq")
    d_mod_all = lax.all_gather(d_mod, "fsdp", axis=0, tiled=False)
    cond_rows32 = cond_rows.astype(F32)
    grad_ada = jnp.stack([
        lax.dot_general(cond_rows32, d_mod_all[:, l], (((0,), (0,)), ((), ())), precision=HIGHEST,
                        preferred_element_type=F32) for l in range(layers)])
    grad_ada_bias = own(jnp.sum(d_mod_all, axis=0), 1, width6 // n)
    g_cond = sum(
        lax.dot_general(d_mod_all[:, l], ada_weight[l].astype(F32), (((1,), (1,)), ((), ())),
                        precision=HIGHEST, preferred_element_type=F32) for l in range(layers))
    g_cond = lax.all_to_all(g_cond, "fsdp", split_axis=0, concat_axis=1, tiled=True)
    _, silu_back = jax.vjp(jax.nn.silu, cond_float)
    grad_condition = silu_back(g_cond)[0]
    return (
        block_out[None], g[None], grad_condition, grad_ada, grad_ada_bias, grad_qkv, grad_bias[0],
        grad_out, grad_bias[1], grad_up, grad_bias[2], grad_down, grad_bias[3],
    )


MESH = pl.DeviceIdType.MESH
FAST = 2
VMEM_LIMIT = 67_043_328
EXP2_SCALE = SCORE_SCALE * 1.4426950408889634


def rcopy(src, dst, send, recv, device):
    return pltpu.make_async_remote_copy(
        src_ref=src, dst_ref=dst, send_sem=send, recv_sem=recv, device_id=device, device_id_type=MESH
    )


def vmem_specs(count):
    return [pl.BlockSpec(memory_space=pltpu.VMEM)] * count


def entry_barrier(devices):
    barrier = pltpu.get_barrier_semaphore()
    for device in devices:
        pl.semaphore_signal(barrier, inc=1, device_id=device, device_id_type=MESH)
    pl.semaphore_wait(barrier, len(devices))


def relative(s, j):
    half = j // 2
    return ((s // 2 + 1 - half) % 2) * 2 + (s % 2 + half + j) % 2


def forward_kernel(n, *refs):
    (x_ref, cond_ref, ada_in, adab_ref, qkvw_ref, qvb_ref, outw_in, outb_ref, upw_in, upb_ref,
     downw_in, downb_ref,
     out_ref, mod_ref, rows_ref), refs = refs[:15], refs[15:]
    stored, held, refs = refs[:13], refs[13:26], refs[26:]
    wq_ref, wo_ref, wu_ref, wd_ref, xs_ref, attn_ref, qh_ref, tok_ref, branch_ref, mid_ref, mlp_ref, up_ref, feed_ref = held
    (osend, psend, precv, chip_sum, xsend, xrecv, xin,
     sq_ref, so_ref, su_ref, bq_ref, bo_ref, bu_ref, bd_ref, cblock, crecv, bsend, brecv, msend, mrecv, mgath,
     c_s, c_r, b_s, b_r, m_s, m_r, w_s, w_r, z_s, z_r, y_s, y_r, a_s, a_r, t_s, t_r, g_s, g_r, r_s, r_r, e_s, e_r, n_s, n_r, q_s, q_r, o_s,
     upw_ref, outw_ref, ada_ref, downw_ref, i_s) = refs
    loads = [
        pltpu.make_async_copy(src, dst, i_s.at[i])
        for i, (src, dst) in enumerate(
            ((upw_in, upw_ref), (outw_in, outw_ref), (ada_in, ada_ref), (downw_in, downw_ref))
        )
    ]
    for load in loads:
        load.start()
    f = lax.axis_index("fsdp")
    s = lax.axis_index("seq")
    slow = n // FAST
    a, b = f // FAST, f % FAST
    layers, rows = qkvw_ref.shape[0], qkvw_ref.shape[1]
    block = x_ref.shape[0]
    width = x_ref.shape[1]
    hc = sq_ref.shape[2] // 3
    heads = hc // HEAD_DIM
    fc = su_ref.shape[2] // n
    chunk = downw_ref.shape[1] // 4
    core = s % 2
    across, diagonal, partner = relative(s, 0), relative(s, 1), relative(s, 2)
    y_dev = {"fsdp": a * FAST + (1 - b)}

    def place(l, p, at):
        if p == 1:
            return wo_ref.at[l, core, at]
        return (wq_ref, None, wu_ref, wd_ref)[p].at[l, at]

    peers = [{"fsdp": (f + k) % n} for k in range(1, n)] + [{"seq": across}, {"seq": diagonal}, {"seq": partner}]
    barrier = pltpu.get_barrier_semaphore()
    for device in peers:
        pl.semaphore_signal(barrier, inc=1, device_id=device, device_id_type=MESH)

    def cut_qkv(l, i):
        sq_ref[l] = jnp.concatenate(
            [qkvw_ref[l, :, j * width + i * hc: j * width + (i + 1) * hc] for j in range(3)], axis=1
        )

    def cut_rest(l, i):
        so_ref[l] = outw_ref[l, :, (i % 2) * (width // 2): (i % 2 + 1) * (width // 2)]
        su_ref[l] = jnp.concatenate(
            [upw_ref[l, :, (4 * j + i) * fc: (4 * j + i + 1) * fc] for j in range(n)], axis=1
        )

    def by_member(work):
        for i in range(4):
            @pl.when(s == i)
            def _():
                work(i)

    by_member(lambda i: cut_qkv(0, i))
    cond = cond_ref[...].astype(F32)
    act = cond / (1.0 + jnp.exp(-cond))
    act = act.astype(BF16).astype(F32)
    cblock[...] = jnp.zeros_like(cblock)
    for i in range(n):
        cblock[i, 0:1, :rows] = act[:, i * rows: (i + 1) * rows]
    crecv[f] = cblock[f]
    for l in range(layers):
        bsend[l: l + 1, :] = jnp.concatenate(
            [r[l: l + 1, :].astype(F32) for r in (adab_ref, outb_ref, downb_ref)], axis=1
        )
        bsend[layers + l: layers + l + 1, : hc + 4 * fc] = jnp.concatenate(
            [r[l: l + 1, :].astype(F32) for r in (qvb_ref, upb_ref)], axis=1
        )
    brecv[f] = bsend[...]
    tokens_over = rcopy(x_ref, xin, n_s.at[0], n_r.at[0], {"seq": across})

    def shard(l, p):
        if p == 3:
            return downw_ref.at[l, pl.ds(pl.multiple_of(s * chunk, chunk), chunk)]
        return (sq_ref, so_ref, su_ref)[p].at[l]

    pl.semaphore_wait(barrier, len(peers))
    for k in range(1, n):
        to = (f + k) % n
        rcopy(cblock.at[to], crecv.at[f], c_s.at[k], c_r.at[k], {"fsdp": to}).start()

    def z_copy(l, p, k, to):
        return rcopy(shard(l, p), place(l, p, f), z_s.at[l, p, k], z_r.at[l, p, k], {"fsdp": to})

    def y_copy(l, p, k):
        at = ((a - k + slow) % slow) * FAST + b
        src = shard(l, p) if k == 0 else place(l, p, at)
        return rcopy(src, place(l, p, at), y_s.at[l, p, k], y_r.at[l, p, k], y_dev)

    def launch(l, p):
        y_copy(l, p, 0).start()
        for k in range(1, slow):
            z_copy(l, p, k, ((a + k) % slow) * FAST + b).start()

    launch(0, 0)
    tokens_over.start()
    for k in range(1, n):
        to = (f + k) % n
        rcopy(bsend, brecv.at[f], b_s.at[k], b_r.at[k], {"fsdp": to}).start()

    loads[0].wait()
    loads[1].wait()
    by_member(lambda i: cut_rest(0, i))
    loads[2].wait()
    loads[3].wait()
    for k in range(1, n):
        at = (f - k + n) % n
        rcopy(cblock.at[at], crecv.at[at], c_s.at[k], c_r.at[k], {"fsdp": at}).wait_recv()
    cond_rows = jnp.sum(crecv[...], axis=1)
    rows_ref[...] = cond_rows
    cond_rows = cond_rows[:, :rows].astype(BF16)
    for l in range(layers):
        quarter = msend.shape[2]
        part = mm(cond_rows, ada_ref[l, :, pl.ds(pl.multiple_of(s * quarter, quarter), quarter)])
        for i in range(n):
            msend[i, l: l + 1, :] = part[i: i + 1, :]
    mrecv[f] = msend[f]
    for k in range(1, n):
        to = (f + k) % n
        rcopy(msend.at[to], mrecv.at[f], m_s.at[k], m_r.at[k], {"fsdp": to}).start()
    for p in range(1, 4):
        launch(0, p)
    for l in range(1, layers):
        by_member(lambda i: cut_qkv(l, i))
        by_member(lambda i: cut_rest(l, i))
        for p in range(4):
            launch(l, p)

    def forward_weights(l, p):
        for k in range(1, slow):
            at = ((a - k + slow) % slow) * FAST + b
            rcopy(shard(l, p), place(l, p, at), z_s.at[l, p, k], z_r.at[l, p, k], {"fsdp": at}).wait_recv()
            y_copy(l, p, k).start()

    def ready(l, p):
        for k in range(slow):
            at = ((a - k + slow) % slow) * FAST + 1 - b
            rcopy(shard(l, p), place(l, p, at), y_s.at[l, p, k], y_r.at[l, p, k], y_dev).wait_recv()

    for k in range(1, n):
        at = (f - k + n) % n
        rcopy(bsend, brecv.at[at], b_s.at[k], b_r.at[k], {"fsdp": at}).wait_recv()
    ac = adab_ref.shape[1]
    for l in range(layers):
        gathered = lambda lo, size, r=l: jnp.concatenate([brecv[i, r: r + 1, lo: lo + size] for i in range(n)], axis=1)
        bo_ref[l] = gathered(ac, rows)
        bd_ref[l] = gathered(ac + rows, rows)
        q_b, v_b = brecv[s, layers + l: layers + l + 1, :hc], brecv[4 + s, layers + l: layers + l + 1, :hc]
        bq_ref[l] = jnp.concatenate([q_b, jnp.zeros_like(q_b), v_b], axis=1)
    for i in range(4):
        @pl.when(s == i)
        def _():
            for l in range(layers):
                lo = hc + i * fc
                bu_ref[l] = jnp.concatenate(
                    [brecv[j, layers + l: layers + l + 1, lo: lo + fc] for j in range(n)], axis=1
                )
    for k in range(1, n):
        at = (f - k + n) % n
        rcopy(msend.at[at], mrecv.at[at], m_s.at[k], m_r.at[k], {"fsdp": at}).wait_recv()
    mgath[s] = jnp.sum(mrecv[...], axis=0)
    for j in range(3):
        rcopy(mgath.at[s], mgath.at[s], q_s.at[j], q_r.at[j], {"seq": relative(s, j)}).start()
    for j in range(3):
        ref = mgath.at[relative(s, j)]
        rcopy(ref, ref, q_s.at[j], q_r.at[j], {"seq": relative(s, j)}).wait_recv()
    for l in range(layers):
        full = jnp.concatenate([mgath[i, l: l + 1, :] for i in range(4)], axis=1) + jnp.concatenate([brecv[i, l: l + 1, :ac] for i in range(n)], axis=1)
        for r in range(6):
            mod_ref[l, r: r + 1, :] = full[:, r * width: (r + 1) * width]
    for l in range(layers):
        for p in range(4):
            place(l, p, f)[...] = shard(l, p)[...]

    core, side = s % 2, s // 2
    xs_ref[0, side] = x_ref[...].astype(F32)
    tokens_over.wait_recv()
    xs_ref[0, 1 - side] = xin[...].astype(F32)

    def save(l, *members):
        for i in members:
            save_copy(l, i).start()

    def save_copy(l, i):
        src = held[i].at[l, side] if i in (7, 8) else held[i].at[l]
        return pltpu.make_async_copy(src, stored[i].at[l], o_s.at[l, i])

    def matrix(ref, l):
        return ref[l].reshape(n * rows, ref.shape[3])

    def half_copy(l):
        ref = wo_ref.at[l, core]
        return rcopy(ref, ref, w_s.at[l], w_r.at[l], {"seq": partner})

    def half_arrived(l):
        ref = wo_ref.at[l, 1 - core]
        rcopy(ref, ref, w_s.at[l], w_r.at[l], {"seq": partner}).wait_recv()

    def share(buf, l, i, send, recv):
        ref = buf.at[l, 2 * i + core]
        return rcopy(ref, ref, send.at[i], recv.at[i], {"seq": partner})

    def shared(buf, l, i, send, recv):
        ref = buf.at[l, 2 * i + 1 - core]
        rcopy(ref, ref, send.at[i], recv.at[i], {"seq": partner}).wait_recv()

    def part_copy(i):
        return rcopy(psend.at[i], precv.at[i], r_s.at[i], r_r.at[i], {"seq": partner})

    def over(i):
        return rcopy(xsend.at[i], xrecv.at[i], e_s.at[i], e_r.at[i], {"seq": across})

    def out_copy(l, j, i, t):
        return rcopy(osend.at[t], tok_ref.at[l, i, s], t_s.at[j, i], t_r.at[j, i], {"seq": relative(s, j)})

    def layer(l, carry):
        row = lambda i: mod_ref[l, i: i + 1, :]

        def qkv_block(t):
            val = (mm(attn_ref[l, t], matrix(wq_ref, l)) + bq_ref[l]).astype(BF16)
            for h in range(3 * heads):
                qh_ref[l, h, pl.ds(pl.multiple_of(t * block, block), block), :] = (
                    val[:, h * HEAD_DIM: (h + 1) * HEAD_DIM]
                )

        def enter(i, carry):
            @pl.when((l > 0) & (i == 1))
            def _():
                forward_weights(l, 2)

            @pl.when(l > 0)
            def _():
                over(i).wait_recv()
                feed = chip_sum[i] + xrecv[i].astype(F32) + bd_ref[l - 1]
                xs_ref[l, i] = mid_ref[l - 1, i] + mod_ref[l - 1, 5:6, :] * feed

                @pl.when(i == side)
                def _():
                    feed_ref[l - 1] = feed

                over(i).wait_send()

            normed, _ = normalize(xs_ref[l, i])
            attn_ref[l, 2 * i + core] = (normed * (1.0 + row(1)) + row(0)).astype(BF16)
            share(attn_ref, l, i, a_s, a_r).start()

            @pl.when((l == 0) & (i == 0))
            def _():
                forward_weights(0, 0)

            @pl.when(i == 0)
            def _():
                ready(l, 0)

            def both(w, carry):
                @pl.when(w == 1)
                def _():
                    shared(attn_ref, l, i, a_s, a_r)

                qkv_block(2 * i + (core + w) % 2)
                return carry

            lax.fori_loop(0, 2, both, 0)
            return carry

        lax.fori_loop(0, 2, enter, 0)

        @pl.when(l > 0)
        def _():
            save(l - 1, 12)

        def attend_block(t, carry):
            outs = []
            for h in range(heads):
                q = qh_ref[l, h, pl.ds(pl.multiple_of(t * block, block), block), :]
                e = jnp.exp2(mm_nt(q, qh_ref[l, heads + h]) * EXP2_SCALE)
                inverse = 1.0 / jnp.sum(e, axis=-1, keepdims=True)
                prob = (e * inverse).astype(BF16)
                outs.append(mm(prob, qh_ref[l, 2 * heads + h]))
            val = jnp.concatenate(outs, axis=1).astype(BF16)
            osend[t] = val
            i = t // 2

            @pl.when(t % 2 == core)
            def _():
                tok_ref[l, i, s] = val
                out_copy(l, 0, i, t).start()

            @pl.when(t % 2 != core)
            def _():
                out_copy(l, 1, i, t).start()
                out_copy(l, 2, i, t).start()

            @pl.when((t == 2) & (l == 0))
            def _():
                forward_weights(0, 1)

            @pl.when((t == 3) & (l > 0))
            def _():
                forward_weights(l, 3)

            return carry

        lax.fori_loop(0, 4, attend_block, 0)
        save(l, 0, 4, 5, 6)
        ready(l, 1)
        half_copy(l).start()

        half_arrived(l)

        def exchange(i):
            part_copy(i).wait_recv()
            chip_sum[i] = chip_sum[i] + precv[i]

            @pl.when((l + 1 < layers) | (i != side))
            def _():
                xsend[i] = chip_sum[i].astype(BF16)
                over(i).start()

        flip = (1 - side) * ((l + 1) // layers)

        def mlp(turn, carry):
            i = (turn + flip) % 2
            for j in range(3):
                ref = tok_ref.at[l, i, relative(s, j)]
                rcopy(ref, ref, t_s.at[j, i], t_r.at[j, i], {"seq": relative(s, j)}).wait_recv()
            tokens_out = jnp.concatenate([tok_ref[l, i, t] for t in range(4)], axis=1)
            branch = jnp.concatenate(
                [mm(tokens_out, wo_ref[l, c].reshape(n * rows, width // 2)) for c in range(2)], axis=1
            ) + bo_ref[l]
            branch_ref[l, i] = branch
            middle = xs_ref[l, i] + row(2) * branch
            mid_ref[l, i] = middle
            normed, _ = normalize(middle)
            mlp_ref[l, 2 * i + core] = (normed * (1.0 + row(4)) + row(3)).astype(BF16)
            share(mlp_ref, l, i, g_s, g_r).start()

            @pl.when((turn == 0) & (l == 0))
            def _():
                forward_weights(0, 2)

            @pl.when(turn == 0)
            def _():
                ready(l, 2)

            def both(w, carry):
                @pl.when(w == 1)
                def _():
                    shared(mlp_ref, l, i, g_s, g_r)

                t = 2 * i + (core + w) % 2
                up = mm(mlp_ref[l, t], matrix(wu_ref, l)) + bu_ref[l]
                up_ref[l, t] = up
                act = gelu_parts(up)[0].astype(BF16)

                @pl.when((turn == 0) & (w == 0) & (l == 0))
                def _():
                    forward_weights(0, 3)

                @pl.when((turn == 0) & (w == 0))
                def _():
                    ready(l, 3)

                part = mm(act, matrix(wd_ref, l))

                @pl.when(w == 0)
                def _():
                    chip_sum[i] = part

                @pl.when(w == 1)
                def _():
                    psend[i] = part
                    part_copy(i).start()

                @pl.when((w == 0) & (turn == 1))
                def _():
                    exchange(1 - i)

                @pl.when((w == 0) & (turn == 1) & (l + 1 < layers))
                def _():
                    forward_weights(1, 0)

                return carry

            lax.fori_loop(0, 2, both, 0)
            return carry

        lax.fori_loop(0, 2, mlp, 0)
        exchange((1 + flip) % 2)
        save(l, 1, 2, 3, 7, 8, 9, 10, 11)

        @pl.when(l + 1 < layers)
        def _():
            forward_weights(1, 1)

        half_copy(l).wait_send()
        for i in range(2):
            share(attn_ref, l, i, a_s, a_r).wait_send()
            share(mlp_ref, l, i, g_s, g_r).wait_send()
            part_copy(i).wait_send()
            for j in range(3):
                out_copy(l, j, i, 2 * i).wait_send()
        return carry

    lax.fori_loop(0, layers, layer, 0)
    last = layers - 1
    over(side).wait_recv()
    feed = chip_sum[side] + xrecv[side].astype(F32) + bd_ref[last]
    feed_ref[last] = feed
    save(last, 12)
    out_ref[...] = (mid_ref[last, side] + mod_ref[last, 5:6, :] * feed).astype(BF16)
    over(1 - side).wait_send()
    tokens_over.wait_send()
    for j in range(3):
        rcopy(mgath.at[s], mgath.at[s], q_s.at[j], q_r.at[j], {"seq": relative(s, j)}).wait_send()
    for l in range(layers):
        for i in range(13):
            save_copy(l, i).wait()
    for l in range(layers):
        for p in range(4):
            y_copy(l, p, 0).wait_send()
            for k in range(1, slow):
                z_copy(l, p, k, ((a + k) % slow) * FAST + b).wait_send()
                y_copy(l, p, k).wait_send()
    for k in range(1, n):
        to = (f + k) % n
        rcopy(cblock.at[to], crecv.at[f], c_s.at[k], c_r.at[k], {"fsdp": to}).wait_send()
        rcopy(bsend, brecv.at[f], b_s.at[k], b_r.at[k], {"fsdp": to}).wait_send()
        rcopy(msend.at[to], mrecv.at[f], m_s.at[k], m_r.at[k], {"fsdp": to}).wait_send()


def forward(n, x, cond, weights):
    layers, rows, width6 = weights[0].shape
    block, width = x.shape
    qc = weights[2].shape[2] // 4
    hc = qc // 3
    nh = qc // HEAD_DIM
    uc = weights[6].shape[2] // 4
    total = 4 * block
    lanes = rows + -rows % 128
    sds = jax.ShapeDtypeStruct
    outs = (
        sds((block, width), BF16),
        sds((layers, 6, width), F32),
        sds((n, lanes), F32),
        sds((layers, n, rows, qc), BF16),
        sds((layers, 2, n, rows, width // 2), BF16),
        sds((layers, n, rows, uc), BF16),
        sds((layers, n, rows, width), BF16),
        sds((layers, 2, block, width), F32),
        sds((layers, 4, block, width), BF16),
        sds((layers, nh, total, HEAD_DIM), BF16),
        sds((layers, 4, block, hc), BF16),
        sds((layers, block, width), F32),
        sds((layers, 2, block, width), F32),
        sds((layers, 4, block, width), BF16),
        sds((layers, 4, block, uc), F32),
        sds((layers, block, width), F32),
    )
    slow = n // FAST
    dma = pltpu.SemaphoreType.DMA
    kept = [list(x.shape) for x in outs[3:]]
    for i in (7, 8):
        kept[i].insert(1, 2)
    scratch = [pltpu.VMEM(tuple(shape), x.dtype) for shape, x in zip(kept, outs[3:])] + [
        pltpu.VMEM((4, block, hc), BF16),
        pltpu.VMEM((2, block, width), F32),
        pltpu.VMEM((2, block, width), F32),
        pltpu.VMEM((2, block, width), F32),
        pltpu.VMEM((2, block, width), BF16),
        pltpu.VMEM((2, block, width), BF16),
        pltpu.VMEM((block, width), BF16),
        pltpu.VMEM((layers, rows, qc), BF16),
        pltpu.VMEM((layers, rows, width // 2), BF16),
        pltpu.VMEM((layers, rows, uc), BF16),
        pltpu.VMEM((layers, 1, qc), F32),
        pltpu.VMEM((layers, 1, width), F32),
        pltpu.VMEM((layers, 1, uc), F32),
        pltpu.VMEM((layers, 1, width), F32),
        pltpu.VMEM((n, 8, lanes), F32),
        pltpu.VMEM((n, 8, lanes), F32),
        pltpu.VMEM((2 * layers, width), F32),
        pltpu.VMEM((n, 2 * layers, width), F32),
        pltpu.VMEM((n, layers, width6 // 4), F32),
        pltpu.VMEM((n, layers, width6 // 4), F32),
        pltpu.VMEM((4, layers, width6 // 4), F32),
    ] + [dma((n,))] * 6 + [dma((layers,))] * 2 + [dma((layers, 4, slow))] * 4 + [dma((2,))] * 2 + [dma((3, 2))] * 2 + [dma((2,))] * 6 + [dma((1,))] * 2 + [dma((3,))] * 2 + [dma((layers, 13))] + [
        pltpu.VMEM(weights[i].shape, BF16) for i in (6, 4, 0, 8)
    ] + [dma((4,))]
    return pl.pallas_call(
        functools.partial(forward_kernel, n),
        out_shape=outs,
        in_specs=[
            pl.BlockSpec(memory_space=pl.ANY if i in (2, 6, 8, 10) else pltpu.VMEM) for i in range(12)
        ],
        out_specs=tuple(vmem_specs(3) + [pl.BlockSpec(memory_space=pl.ANY)] * 13),
        scratch_shapes=scratch,
        compiler_params=pltpu.CompilerParams(
            collective_id=1, has_side_effects=True, vmem_limit_bytes=VMEM_LIMIT
        ),
    )(x, cond, *weights)


def backward_kernel(n, *refs):
    (cot_ref, mod_ref, ada_ref), rest = refs[:3], refs[3:]
    stored, rest = rest[:13], rest[13:]
    (g_ref, vec_all, cat_all, gcond_ref), rest = rest[:4], rest[4:]
    fin, rest = rest[:4], rest[4:]
    loaded, rest = list(rest[:11]), rest[11:]
    loaded.insert(5, loaded[8])
    loaded.insert(8, loaded[11])
    grads, rest = rest[:4], rest[4:]
    y_in, rest = rest[:4], rest[4:]
    z_out, rest = rest[:4], rest[4:]
    z_in, rest = rest[:4], rest[4:]
    kept, rest = rest[:4], rest[4:]
    (gf_ref, gb_ref, act_ref, gup_ref, gqkv_ref, psend, precv, chip_sum, xsend, xrecv,
     gx_ref, gmid_ref, dk_acc, dv_acc, orecv,
     vec_ref, cat_ref, vec_in, vec_sum, cat_in, gc_send, gc_recv, v_s, v_r, u_s, u_r, k_s, k_r, h_s, h_r, i_s, i_r,
     l_s, o_s, o_r, y_s, y_r, z_s, z_r, f_s, f_r, g_s, g_r, t_s, t_r, r_s, r_r, e_s, e_r, n_s, n_r, ada_s) = rest
    wq, wo, wu, wd, xs, attn, qh, tok, branch, mid, mlp, up, feed = range(13)
    down, upw, outw, qkvw = range(4)
    f = lax.axis_index("fsdp")
    s = lax.axis_index("seq")
    slow = n // FAST
    a, b = f // FAST, f % FAST
    layers = mod_ref.shape[0]
    block, width = cot_ref.shape
    rows = width // n
    hc = gqkv_ref.shape[2] // 3
    half = width // 2
    core, side = s % 2, s // 2
    heads = hc // HEAD_DIM
    across, diagonal, partner = relative(s, 0), relative(s, 1), relative(s, 2)
    y_dev = {"fsdp": a * FAST + (1 - b)}

    def load(i, l):
        return pltpu.make_async_copy(stored[i].at[l], loaded[i], l_s.at[i])

    for i in (feed, wd, up, wu, mlp, mid, wo, tok, qh, wq, xs):
        load(i, layers - 1).start()

    entry_barrier(
        [{"fsdp": (f + k) % n} for k in range(1, n)]
        + [{"seq": across}, {"seq": diagonal}, {"seq": partner}]
    )

    def y_copy(l, p):
        return rcopy(grads[p].at[:, 1 - b], y_in[p].at[l], y_s.at[p], y_r.at[l, p], y_dev)

    def z_copy(l, p, k):
        to = (a + k) % slow
        return rcopy(z_out[p].at[to], z_in[p].at[l, k - 1], z_s.at[p, k], z_r.at[l, p, k], {"fsdp": to * FAST + b})

    def z_start(l, p):
        y_copy(l, p).wait_recv()
        for i in range(slow):
            z_out[p][i] = (grads[p][i, b].astype(F32) + y_in[p][l, i].astype(F32)).astype(BF16)
        kept[p][...] = grads[p][a, b].astype(F32) + y_in[p][l, a].astype(F32)
        for k in range(1, slow):
            z_copy(l, p, k).start()
        y_copy(l, p).wait_send()

    def fin_copy(l, p, i):
        mine, theirs = fin[p].at[l, s], fin[p].at[l, across]
        ref = theirs if i == 2 else mine
        return rcopy(ref, ref, f_s.at[l, p, i], f_r.at[l, p, i], {"seq": across if i == 1 else partner})

    def z_finish(l, p):
        total = kept[p][...]
        for k in range(1, slow):
            z_copy(l, p, k).wait_recv()
            total = total + z_in[p][l, k - 1].astype(F32)
        fin[p][l, s] = total.astype(BF16)
        fin_copy(l, p, 1).start()
        fin_copy(l, p, 0).start()
        for k in range(1, slow):
            z_copy(l, p, k).wait_send()

    def fin_arrived(l, p, i):
        ref = fin[p].at[l, (partner, across, diagonal)[i]]
        rcopy(ref, ref, f_s.at[l, p, i], f_r.at[l, p, i], {"seq": partner}).wait_recv()

    def ada_load(q):
        l, r = q // 6, q % 6
        dst = loaded[(wd, wu)[q // n]].at[q % n]
        return pltpu.make_async_copy(ada_ref.at[l, :, pl.ds(r * width, width)], dst, ada_s.at[q])

    def matrix(i):
        return loaded[i][...].reshape(width, loaded[i].shape[2])

    def part_copy(i):
        return rcopy(psend.at[0], precv.at[i], r_s.at[i], r_r.at[i], {"seq": partner})

    def over(kind, i):
        at = 2 * kind + i
        return rcopy(xsend.at[i], xrecv.at[at], e_s.at[at], e_r.at[at], {"seq": across})

    def share(buf, i, send, recv):
        ref = buf.at[2 * i + core]
        return rcopy(ref, ref, send.at[i], recv.at[i], {"seq": partner})

    def shared(buf, i, send, recv):
        ref = buf.at[2 * i + 1 - core]
        rcopy(ref, ref, send.at[i], recv.at[i], {"seq": partner}).wait_recv()

    def place(w, i, part):
        @pl.when(w == 0)
        def _():
            chip_sum[i] = part

        @pl.when(w == 1)
        def _():
            psend[0] = part
            part_copy(i).start()

    def exchange(kind, i, wanted):
        part_copy(i).wait_recv()
        chip_sum[i] = chip_sum[i] + precv[i]

        @pl.when(wanted)
        def _():
            xsend[i] = chip_sum[i].astype(BF16)
            over(kind, i).start()

        part_copy(i).wait_send()

    def vec_copy(l, j):
        return rcopy(vec_ref.at[l], vec_in.at[l, s], v_s.at[l, j], v_r.at[l, j], {"seq": relative(s, j)})

    def vec_start(l):
        vec_in[l, s] = vec_ref[l]
        for j in range(3):
            vec_copy(l, j).start()

    def vec_spread(l):
        for j in range(3):
            ref = vec_in.at[l, relative(s, j)]
            rcopy(ref, ref, v_s.at[l, j], v_r.at[l, j], {"seq": relative(s, j)}).wait_recv()
        vec_sum[l] = jnp.sum(vec_in[l], axis=0)
        vec_all[l, f] = vec_sum[l]
        cat_in[l, f] = cat_ref[l]
        for k in range(1, n):
            to = {"fsdp": (f + k) % n}
            rcopy(vec_sum.at[l], vec_all.at[l, f], u_s.at[l, k], u_r.at[l, k], to).start()
            rcopy(cat_ref.at[l], cat_in.at[l, f], k_s.at[l, k], k_r.at[l, k], to).start()

    def vec_arrived(l):
        for k in range(1, n):
            at = (f - k + n) % n
            rcopy(vec_sum.at[l], vec_all.at[l, at], u_s.at[l, k], u_r.at[l, k], {"fsdp": at}).wait_recv()
            rcopy(cat_ref.at[l], cat_in.at[l, at], k_s.at[l, k], k_r.at[l, k], {"fsdp": at}).wait_recv()

    def sums(value):
        return jnp.sum(value, axis=0, keepdims=True)

    def leave(l, i):
        g_ain = chip_sum[i] + xrecv[2 + i].astype(F32)
        normed, inverse = normalize(loaded[xs][i])

        @pl.when(i == side)
        def _():
            vec_ref[l, 1:2, :] = sums(g_ain * normed)
            vec_ref[l, 0:1, :] = sums(g_ain)

        return gmid_ref[i] + norm_back(g_ain * (1.0 + mod_ref[l, 1:2, :]), normed, inverse)

    cot_over = rcopy(cot_ref, xrecv.at[2 + side], n_s.at[0], n_r.at[0], {"seq": across})
    cot_over.start()
    gx_ref[side] = cot_ref[...].astype(F32)

    def layer(step, carry):
        l = layers - 1 - step
        row = lambda i: mod_ref[l, i: i + 1, :]
        cat_ref[l] = jnp.zeros_like(cat_ref[l])
        for i in (feed, wd, up, wu, mlp):
            load(i, l).wait()

        @pl.when(step > 0)
        def _():
            load(xs, l + 1).wait()

        def enter(turn, carry):
            i = (turn + side * (1 - (step + layers - 1) // layers)) % 2

            @pl.when((step == 0) & (turn == 1))
            def _():
                theirs = xrecv.at[3 - side]
                rcopy(cot_ref, theirs, n_s.at[0], n_r.at[0], {"seq": across}).wait_recv()
                gx_ref[1 - side] = theirs[...].astype(F32)

            @pl.when(step > 0)
            def _():
                over(1, i).wait_recv()
                over(1, i).wait_send()
                gx_ref[i] = leave(l + 1, i)

            g = gx_ref[i]
            g_feed = (row(5) * g).astype(BF16)
            gf_ref[2 * i + core] = g_feed
            share(gf_ref, i, g_s, g_r).start()

            @pl.when(i == side)
            def _():
                vec_ref[l, 5:6, :] = sums(g * loaded[feed][...])
                vec_ref[l, 7:8, :] = sums(g_feed.astype(F32))

            def both(w, carry):
                @pl.when(w == 1)
                def _():
                    shared(gf_ref, i, g_s, g_r)

                t = 2 * i + (core + w) % 2
                value, slope = gelu_parts(loaded[up][t])
                act_ref[pl.ds(pl.multiple_of(t * block, block), block), :] = value.astype(BF16)
                g_up = (mm_nt(gf_ref[t], matrix(wd)) * slope).astype(BF16)
                gup_ref[t] = g_up
                cat_ref[l, 0:1, :] = cat_ref[l, 0:1, :] + sums(g_up.astype(F32))
                place(w, i, mm_nt(g_up, matrix(wu)))
                return carry

            lax.fori_loop(0, 2, both, 0)
            exchange(0, i, l >= 0)
            return carry

        lax.fori_loop(0, 2, enter, 0)

        load(branch, l).start()

        @pl.when(step > 0)
        def _():
            load(xs, l).start()
            vec_start(l + 1)
            z_start(l + 1, outw)
            z_start(l + 1, qkvw)

        whole = lambda ref: ref[...].reshape(4 * block, ref.shape[2])
        grads[down][...] = mm_tn(act_ref[...], whole(gf_ref)).astype(BF16).reshape(grads[down].shape)
        y_copy(l, down).start()
        grads[upw][...] = mm_tn(whole(loaded[mlp]), whole(gup_ref)).astype(BF16).reshape(grads[upw].shape)
        y_copy(l, upw).start()

        load(attn, l).start()

        @pl.when(l > 0)
        def _():
            for i in (wd, up, wu):
                load(i, l - 1).start()

        @pl.when(l == 0)
        def _():
            for q in range(6 * layers):
                ada_load(q).start()

        for i in (mid, branch, wo, tok, qh):
            load(i, l).wait()
        dk_acc[...] = jnp.zeros_like(dk_acc)
        dv_acc[...] = jnp.zeros_like(dv_acc)

        def pair(c):
            src = act_ref.at[pl.ds(0, width), pl.ds(c * half, half)]
            return rcopy(src, orecv.at[l], o_s.at[0], o_r.at[l], {"seq": partner})

        def inner(i, carry):
            over(0, i).wait_recv()
            over(0, i).wait_send()
            g_min = chip_sum[i] + xrecv[i].astype(F32)
            normed, inverse = normalize(loaded[mid][i])
            g_mid = gx_ref[i] + norm_back(g_min * (1.0 + row(4)), normed, inverse)
            gmid_ref[i] = g_mid
            g_branch = (row(2) * g_mid).astype(BF16)
            gb_ref[2 * i + core] = g_branch
            share(gb_ref, i, t_s, t_r).start()

            @pl.when(i == side)
            def _():
                vec_ref[l, 4:5, :] = sums(g_min * normed)
                vec_ref[l, 3:4, :] = sums(g_min)
                vec_ref[l, 2:3, :] = sums(g_mid * loaded[branch][...])
                vec_ref[l, 6:7, :] = sums(g_branch.astype(F32))

            @pl.when((step > 0) & (i == 1))
            def _():
                z_finish(l + 1, down)
                z_finish(l + 1, upw)
                vec_spread(l + 1)

            @pl.when(i == 1)
            def _():
                tokens_out = jnp.concatenate([loaded[tok][t] for t in range(4)], axis=1)
                for c in range(2):
                    act_ref[:width, c * half: (c + 1) * half] = mm_tn(
                        tokens_out, gb_ref[s, :, c * half: (c + 1) * half]
                    ).astype(BF16)
                for c in range(2):
                    @pl.when(core != c)
                    def _():
                        pair(c).start()

            def tile(w, carry):
                @pl.when(w == 1)
                def _():
                    shared(gb_ref, i, t_s, t_r)

                t = 2 * i + (core + w) % 2
                at = pl.ds(pl.multiple_of(t * block, block), block)
                lines = hc // rows
                g_o = sum(
                    mm_nt(
                        gb_ref[t, :, c * half: (c + 1) * half],
                        loaded[wo][c, pl.ds(s * lines, lines)].reshape(hc, half),
                    )
                    for c in range(2)
                ).astype(BF16)
                for h in range(heads):
                    q = loaded[qh][h, at, :]
                    k = loaded[qh][heads + h]
                    g_out = g_o[:, h * HEAD_DIM: (h + 1) * HEAD_DIM]
                    e = jnp.exp2(mm_nt(k, q) * EXP2_SCALE)
                    prob = e * (1.0 / jnp.sum(e, axis=0, keepdims=True))
                    dv_acc[h] = dv_acc[h] + mm(prob.astype(BF16), g_out)
                    dp = mm_nt(loaded[qh][2 * heads + h], g_out)
                    inner_sum = jnp.sum(prob * dp, axis=0, keepdims=True)
                    ds = (prob * (dp - inner_sum)).astype(BF16)
                    gqkv_ref[t, :, h * HEAD_DIM: (h + 1) * HEAD_DIM] = (mm_tn(ds, k) * SCORE_SCALE).astype(BF16)
                    dk_acc[h] = dk_acc[h] + mm(ds, q)
                return carry

            lax.fori_loop(0, 2, tile, 0)

            return carry

        lax.fori_loop(0, 2, inner, 0)
        pair(0).wait_recv()
        for c in range(2):
            @pl.when(core == c)
            def _():
                out_sum = act_ref[:width, c * half: (c + 1) * half].astype(F32) + orecv[l].astype(F32)
                grads[outw][...] = out_sum.astype(BF16).reshape(grads[outw].shape)
        y_copy(l, outw).start()
        pair(0).wait_send()

        z_start(l, down)
        for h in range(heads):
            for j, acc, scale in ((1, dk_acc, SCORE_SCALE), (2, dv_acc, 1.0)):
                lo = (j * heads + h) * HEAD_DIM
                value = (acc[h] * scale).astype(BF16)
                for t in range(4):
                    gqkv_ref[t, :, lo: lo + HEAD_DIM] = value[t * block: (t + 1) * block]

        @pl.when(l > 0)
        def _():
            for i in (feed, mid, wo, tok, qh):
                load(i, l - 1).start()

        load(wq, l).wait()

        flip = (1 - side) * ((step + 1) // layers)

        def back(turn, carry):
            i = (turn + flip) % 2

            def both(w, carry):
                place(1 - w, i, mm_nt(gqkv_ref[2 * i + (core + 1 - w) % 2], matrix(wq)))
                return carry

            lax.fori_loop(0, 2, both, 0)
            exchange(1, i, (l > 0) | (i != side))
            return carry

        lax.fori_loop(0, 2, back, 0)
        load(attn, l).wait()
        grads[qkvw][...] = mm_tn(whole(loaded[attn]), whole(gqkv_ref)).astype(BF16).reshape(grads[qkvw].shape)
        y_copy(l, qkvw).start()
        cat_ref[l, 1:2, : 3 * hc] = sums(whole(gqkv_ref).astype(F32))

        @pl.when(l > 0)
        def _():
            for i in (wq, mlp):
                load(i, l - 1).start()

        for i in range(2):
            share(gf_ref, i, g_s, g_r).wait_send()
            share(gb_ref, i, t_s, t_r).wait_send()
        z_start(l, upw)

        @pl.when(step > 0)
        def _():
            z_finish(l + 1, outw)
            z_finish(l + 1, qkvw)

        return carry

    lax.fori_loop(0, layers, layer, 0)
    load(xs, 0).wait()
    z_start(0, outw)
    over(1, side).wait_recv()
    g_ref[...] = leave(0, side)
    vec_start(0)
    z_start(0, qkvw)
    vec_spread(0)
    over(1, 1 - side).wait_send()
    cot_over.wait_send()
    z_finish(0, down)
    z_finish(0, upw)
    z_finish(0, outw)
    for l in range(1, layers):
        for p in (down, upw, outw, qkvw):
            fin_arrived(l, p, 1)
            fin_copy(l, p, 2).start()
    for l in range(layers):
        vec_arrived(l)
        cat_all[l, s] = jnp.sum(cat_in[l], axis=0)
    for j in range(3):
        ref = cat_all.at[:, s]
        rcopy(ref, ref, h_s.at[j], h_r.at[j], {"seq": relative(s, j)}).start()
    for q in range(6 * layers):
        ada_load(q).wait()
    g_cond = jnp.zeros((n, rows), F32)
    for l in range(layers):
        for r in range(6):
            d = vec_all[l, :, r, :]
            high = d.astype(BF16)
            low = (d - high.astype(F32)).astype(BF16)
            q = 6 * l + r
            w = loaded[(wd, wu)[q // n]][q % n]
            g_cond = g_cond + mm_nt(high, w) + mm_nt(low, w)
    for i in range(n):
        gc_send[i, 0:1, :rows] = g_cond[i: i + 1, :]

    def cond_copy(k):
        to = (f + k) % n
        return rcopy(gc_send.at[to], gc_recv.at[f], i_s.at[k], i_r.at[k], {"fsdp": to})

    gc_recv[f] = gc_send[f]
    for k in range(1, n):
        cond_copy(k).start()
    z_finish(0, qkvw)
    for p in (down, upw, outw, qkvw):
        fin_arrived(0, p, 1)
        fin_copy(0, p, 2).start()
    for k in range(1, n):
        at = (f - k + n) % n
        rcopy(gc_send.at[at], gc_recv.at[at], i_s.at[k], i_r.at[k], {"fsdp": at}).wait_recv()
    gcond_ref[...] = jnp.concatenate([gc_recv[i, 0:1, :rows] for i in range(n)], axis=1)
    for j in range(3):
        ref = cat_all.at[:, relative(s, j)]
        rcopy(ref, ref, h_s.at[j], h_r.at[j], {"seq": relative(s, j)}).wait_recv()
    for l in range(layers):
        for p in range(4):
            fin_arrived(l, p, 0)
            fin_arrived(l, p, 2)
            for i in range(3):
                fin_copy(l, p, i).wait_send()
    for k in range(1, n):
        cond_copy(k).wait_send()
        to = {"fsdp": (f + k) % n}
        for l in range(layers):
            rcopy(vec_sum.at[l], vec_all.at[l, f], u_s.at[l, k], u_r.at[l, k], to).wait_send()
            rcopy(cat_ref.at[l], cat_in.at[l, f], k_s.at[l, k], k_r.at[l, k], to).wait_send()
    for j in range(3):
        ref = cat_all.at[:, s]
        rcopy(ref, ref, h_s.at[j], h_r.at[j], {"seq": relative(s, j)}).wait_send()
        for l in range(layers):
            vec_copy(l, j).wait_send()


def backward(n, cot, mod, ada, stored):
    layers = mod.shape[0]
    block, width = cot.shape
    rows = width // n
    slow = n // FAST
    qc = stored[0].shape[3]
    uc = stored[2].shape[3]
    hc = qc // 3
    nh = qc // HEAD_DIM
    sds = jax.ShapeDtypeStruct
    dma = pltpu.SemaphoreType.DMA
    columns = (width, uc, width // 2, qc)
    outs = [
        sds((block, width), F32),
        sds((layers, n, 8, width), F32),
        sds((layers, 4, 2, uc), F32),
        sds((1, width), F32),
    ] + [sds((layers, 4, rows, c), BF16) for c in columns]
    scratch = (
        [pltpu.VMEM(x.shape[1:], x.dtype) for i, x in enumerate(stored) if i not in (5, 8)]
        + [pltpu.VMEM((slow, FAST, rows, c), BF16) for c in columns]
        + [pltpu.VMEM((layers, slow, rows, c), BF16) for c in columns]
        + [pltpu.VMEM((slow, rows, c), BF16) for c in columns]
        + [pltpu.VMEM((layers, slow - 1, rows, c), BF16) for c in columns]
        + [pltpu.VMEM((rows, c), F32) for c in columns]
        + [
            pltpu.VMEM((4, block, width), BF16),
            pltpu.VMEM((4, block, width), BF16),
            pltpu.VMEM((4 * block, uc), BF16),
            pltpu.VMEM((4, block, uc), BF16),
            pltpu.VMEM((4, block, qc), BF16),
            pltpu.VMEM((1, block, width), F32),
            pltpu.VMEM((2, block, width), F32),
            pltpu.VMEM((2, block, width), F32),
            pltpu.VMEM((2, block, width), BF16),
            pltpu.VMEM((4, block, width), BF16),
            pltpu.VMEM((2, block, width), F32),
            pltpu.VMEM((2, block, width), F32),
            pltpu.VMEM((nh // 3, 4 * block, HEAD_DIM), F32),
            pltpu.VMEM((nh // 3, 4 * block, HEAD_DIM), F32),
            pltpu.VMEM((layers, width, width // 2), BF16),
            pltpu.VMEM((layers, 8, width), F32),
            pltpu.VMEM((layers, 2, uc), F32),
            pltpu.VMEM((layers, 4, 8, width), F32),
            pltpu.VMEM((layers, 8, width), F32),
            pltpu.VMEM((layers, n, 2, uc), F32),
            pltpu.VMEM((n, 8, rows + -rows % 128), F32),
            pltpu.VMEM((n, 8, rows + -rows % 128), F32),
            dma((layers, 3)), dma((layers, 3)),
            dma((layers, n)), dma((layers, n)), dma((layers, n)), dma((layers, n)),
            dma((3,)), dma((3,)), dma((n,)), dma((n,)),
            dma((13,)), dma((1,)), dma((layers,)),
            dma((4,)), dma((layers, 4)),
            dma((4, slow)), dma((layers, 4, slow)),
            dma((layers, 4, 3)), dma((layers, 4, 3)),
        ]
        + [dma((2,))] * 6 + [dma((4,))] * 2 + [dma((1,))] * 2 + [dma((6 * layers,))]
    )
    return pl.pallas_call(
        functools.partial(backward_kernel, n),
        out_shape=tuple(outs),
        in_specs=vmem_specs(2) + [pl.BlockSpec(memory_space=pl.ANY)] * 14,
        out_specs=tuple(vmem_specs(len(outs))),
        scratch_shapes=scratch,
        compiler_params=pltpu.CompilerParams(
            collective_id=2, has_side_effects=True, vmem_limit_bytes=VMEM_LIMIT
        ),
    )(cot, mod, ada, *stored)


def assemble_kernel(n, vec_ref, cat_ref, rows_ref, gcond_ref, cond_ref, fd_ref, fu_ref, fo_ref, fq_ref,
                    gcondition, g_adab, g_qvb, g_ob, g_ub, g_db, g_ada, g_qkv, g_out, g_up, g_down,
                    ada_buf, qkv_buf, out_buf, up_buf, down_buf, sem):
    f = lax.axis_index("fsdp")
    layers, rows = fd_ref.shape[0], fd_ref.shape[2]
    width = rows * n
    hc = fq_ref.shape[3] // 3
    fc = fu_ref.shape[3] // n
    ac = g_adab.shape[1]
    copies = []

    def write(i, l, buf, out):
        copies.append(pltpu.make_async_copy(buf.at[l], out.at[l], sem.at[i, l]))
        copies[-1].start()

    for l in range(layers):
        for t in range(4):
            down_buf[l, t * rows: (t + 1) * rows, :] = fd_ref[l, t].astype(F32)
        write(0, l, down_buf, g_down)
    for l in range(layers):
        for j in range(n):
            up_buf[l, :, 4 * j * fc: 4 * (j + 1) * fc] = jnp.concatenate(
                [fu_ref[l, t, :, j * fc: (j + 1) * fc].astype(F32) for t in range(4)], axis=1
            )
        write(1, l, up_buf, g_up)
    cond_rows = rows_ref[:, :rows].astype(BF16)
    for l in range(layers):
        for r in range(6):
            d = vec_ref[l, :, r, :]
            high = d.astype(BF16)
            low = (d - high.astype(F32)).astype(BF16)
            ada_buf[l, :, r * width: (r + 1) * width] = mm_tn(cond_rows, high) + mm_tn(cond_rows, low)
        write(2, l, ada_buf, g_ada)
    for l in range(layers):
        for j in range(3):
            qkv_buf[l, :, j * width: (j + 1) * width] = jnp.concatenate(
                [fq_ref[l, t, :, j * hc: (j + 1) * hc].astype(F32) for t in range(4)], axis=1
            )
        write(3, l, qkv_buf, g_qkv)
    for l in range(layers):
        for c in range(2):
            out_buf[l, :, c * (width // 2): (c + 1) * (width // 2)] = (
                fo_ref[l, c].astype(F32) + fo_ref[l, 2 + c].astype(F32)
            )
        write(4, l, out_buf, g_out)
    cond = cond_ref[...].astype(F32)
    gate = 1.0 / (1.0 + jnp.exp(-cond))
    gcondition[...] = gcond_ref[...] * (gate * (1.0 + cond * (1.0 - gate)))
    total = [jnp.sum(vec_ref[l], axis=0) for l in range(layers)]
    for i in range(n):
        @pl.when(f == i)
        def _():
            for l in range(layers):
                at = slice(l, l + 1)
                flat = jnp.concatenate([total[l][r: r + 1, :] for r in range(6)], axis=1)
                g_adab[at, :] = flat[:, i * ac: (i + 1) * ac]
                g_ob[at, :] = total[l][6:7, i * rows: (i + 1) * rows]
                g_db[at, :] = total[l][7:8, i * rows: (i + 1) * rows]
                g_ub[at, :] = jnp.concatenate(
                    [cat_ref[l, t, 0:1, i * fc: (i + 1) * fc] for t in range(4)], axis=1
                )
                lo = (i // 4) * 2 * hc
                g_qvb[at, :] = cat_ref[l, i % 4, 1:2, lo: lo + hc]
    for copy in copies:
        copy.wait()


def assemble(n, vec_all, cat_all, cond_rows, g_cond, cond, fins):
    layers, _, rows, width = fins[0].shape
    uc, qc = fins[1].shape[3], fins[3].shape[3]
    sds = jax.ShapeDtypeStruct
    big = [(layers, rows, 6 * width), (layers, rows, 4 * qc), (layers, rows, width),
           (layers, rows, 4 * uc), (layers, 4 * rows, width)]
    small = [(1, width), (layers, 6 * width // n), (layers, 2 * width // n), (layers, rows),
             (layers, 4 * uc // n), (layers, rows)]
    return pl.pallas_call(
        functools.partial(assemble_kernel, n),
        out_shape=tuple(sds(x, F32) for x in small + big),
        in_specs=vmem_specs(9),
        out_specs=tuple(vmem_specs(6) + [pl.BlockSpec(memory_space=pl.ANY)] * 5),
        scratch_shapes=[pltpu.VMEM(x, F32) for x in big] + [pltpu.SemaphoreType.DMA((5, layers))],
        compiler_params=pltpu.CompilerParams(vmem_limit_bytes=VMEM_LIMIT),
    )(vec_all, cat_all, cond_rows, g_cond, cond, *fins)


def fused_device(
    tokens, condition, ada_weight, ada_bias, qkv_weight, qv_bias, out_weight, out_bias,
    up_weight, up_bias, down_weight, down_bias, cotangent,
):
    n = lax.axis_size("fsdp")
    block_out, mod, cond_rows, *stored = forward(
        n, tokens[0], condition,
        (ada_weight, ada_bias, qkv_weight, qv_bias, out_weight, out_bias, up_weight, up_bias, down_weight, down_bias))
    g, vec_all, cat_all, g_cond, *fins = backward(n, cotangent[0], mod, ada_weight, stored)
    (g_condition, g_adab, g_qvb, g_ob, g_ub, g_db, g_ada, g_qkv, g_out, g_up, g_down) = assemble(
        n, vec_all, cat_all, cond_rows, g_cond, condition, fins)
    return (
        block_out[None], g[None], g_condition, g_ada, g_adab, g_qkv, g_qvb, g_out, g_ob, g_up, g_ub, g_down, g_db,
    )


def solution(mesh):
    token = P("fsdp", "seq", None)
    matrix = P(None, "fsdp", None)
    vector = P(None, "fsdp")

    def per_device(*args):
        rows = args[2].shape[1]
        fits = rows % 32 == 0 and mesh.shape["seq"] == 4 and mesh.shape["fsdp"] == 8 and args[0].shape[0] == 1
        return (fused_device if fits else plain_device)(*args)

    return jax.shard_map(
        per_device,
        mesh=mesh,
        in_specs=(token, P("fsdp", None)) + (matrix, vector) * 5 + (token,),
        out_specs=(token, token, P("fsdp", None)) + (matrix, vector) * 5,
        check_vma=False,
    )
```
